32 devices in a mesh: fsdp: 4 (over z), context: 8 (over y, x, core).
Axes of the slice: x: 2, y: 2, z: 4, core: 2. Of those that a mesh axis runs over, the one named last changes fastest.
Arguments:
- block_input: bfloat16 [4, 1024, 1536], P('fsdp', 'context'), may hold values from -15 to 15
- cotangent: bfloat16 [4, 1024, 1536], P('fsdp', 'context'), may hold values from -6 to 6
- documents: int32 [4, 1024], P('fsdp', 'context'), may hold values from 0 to 7, as said below
- attn_weights: float32 [4608, 1536], P(('fsdp', 'context')), may hold values from -1.5 to 1.5
- ffn_weights: float32 [12288, 1536], P(('fsdp', 'context')), may hold values from -0.36 to 0.36
- norm_gains: float32 [2, 1536], replicated, may hold values from -0.5 to 0.5
- attn_moments: float32 [2, 4608, 1536], P(None, ('fsdp', 'context')), may hold values from -0.8 to 0.8, as said below
- ffn_moments: float32 [2, 12288, 1536], P(None, ('fsdp', 'context')), may hold values from -0.8 to 0.8, as said below
- gain_moments: float32 [2, 2, 1536], P(None, None, ('fsdp', 'context')), may hold values from -0.8 to 0.8, as said below
Outputs:
- block_output: float32 [4, 1024, 1536], P('fsdp', 'context')
- input_grad: float32 [4, 1024, 1536], P('fsdp', 'context')
- attn_grad: float32 [4608, 1536], P(('fsdp', 'context'))
- ffn_grad: float32 [12288, 1536], P(('fsdp', 'context'))
- gain_grad: float32 [2, 1536], P(None, ('fsdp', 'context'))
- new_attn_weights: float32 [4608, 1536], P(('fsdp', 'context'))
- new_ffn_weights: float32 [12288, 1536], P(('fsdp', 'context'))
- new_norm_gains: float32 [2, 1536], P(None, ('fsdp', 'context'))
- new_attn_moments: float32 [2, 4608, 1536], P(None, ('fsdp', 'context'))
- new_ffn_moments: float32 [2, 12288, 1536], P(None, ('fsdp', 'context'))
- new_gain_moments: float32 [2, 2, 1536], P(None, None, ('fsdp', 'context'))
The draws below stay inside these ranges and needn't reach their ends.
Inputs may be any that keep to these rules, and one draw needn't show every extreme that they name: Segment numbers never fall along a sequence and start at 0; each sequence holds 8 documents of 50 to 640 tokens, one of exactly 640. `attn_moments`: entry 1 along the first dimension is positive. `ffn_moments`: entry 1 along the first dimension is positive. `gain_moments`: entry 1 along the first dimension is positive.
All inputs are finite; a program needn't handle non-finite values.
Results may differ from the reference program's by a relative error of at most 0.015.
Values may be sent and summed in bfloat16 or wider, within the bound.
A program may use at most 448 MiB of HBM per device.

```python
import math
import jax
import jax.numpy as jnp
from jax import lax

D = 1536
FF = 4096
QUERY_HEADS = 16
KEY_VALUE_HEADS = 8
HEAD_SIZE = 96
STEP = 3
DOCS = 8
SEQUENCE_TOKENS = 1024
SEQS = 4
TOKENS = 4096
DOC_MOST = 640
DOC_LEAST = 50
ATT_ROWS = 4608
FFN_ROWS = 12288


def draw_block_input(key, part):
    key_values, key_scales = jax.random.split(key, 2)
    spread = jnp.exp(jax.random.uniform(key_scales, (SEQS, SEQUENCE_TOKENS, 1), jnp.float32, 0.0, math.log(10.0))) * 0.3
    noise = jax.random.truncated_normal(key_values, -5.0, 5.0, (SEQS, SEQUENCE_TOKENS, D), jnp.float32)
    return (noise * spread).astype(jnp.bfloat16)


def one_sequence_docs(key):
    key_cuts, key_place = jax.random.split(key)
    spare = SEQUENCE_TOKENS - DOC_MOST - (DOCS - 1) * DOC_LEAST
    cuts = jnp.sort(jax.random.randint(key_cuts, (DOCS - 2,), 0, spare + 1)).astype(jnp.int32)
    edges = jnp.concatenate([jnp.zeros((1,), jnp.int32), cuts, jnp.full((1,), spare, jnp.int32)])
    shorter = edges[1:] - edges[:-1] + DOC_LEAST
    place = jax.random.randint(key_place, (), 0, DOCS).astype(jnp.int32)
    slot = jnp.arange(DOCS, dtype=jnp.int32)
    before = shorter[jnp.clip(slot, 0, DOCS - 2)]
    after = shorter[jnp.clip(slot - 1, 0, DOCS - 2)]
    lengths = jnp.where(slot < place, before, jnp.where(slot == place, DOC_MOST, after)).astype(jnp.int32)
    ends = jnp.cumsum(lengths).astype(jnp.int32)
    token = jnp.arange(SEQUENCE_TOKENS, dtype=jnp.int32)
    return jnp.sum((token[:, None] >= ends[None, :-1]).astype(jnp.int32), axis=1).astype(jnp.int32)


def draw_documents(key, part):
    keys = jax.random.split(jax.random.fold_in(key, 11), SEQS)
    return jax.vmap(one_sequence_docs)(keys)


def draw_attn_weights(key, part):
    row_index = jnp.arange(ATT_ROWS)[:, None]
    deviation = jnp.where(row_index < ATT_ROWS - QUERY_HEADS * HEAD_SIZE, D ** (-0.5), (D // 16) ** (-0.5))
    return jax.random.truncated_normal(jax.random.fold_in(key, 3), -4.0, 4.0, (ATT_ROWS, D), jnp.float32) * deviation


def draw_ffn_weights(key, part):
    row_index = jnp.arange(FFN_ROWS)[:, None]
    deviation = jnp.where(row_index < 2 * FF, D ** (-0.5), FF ** (-0.5))
    return jax.random.truncated_normal(jax.random.fold_in(key, 5), -4.0, 4.0, (FFN_ROWS, D), jnp.float32) * deviation


def moment_pair(key, shape_rows, salt):
    key_first, key_second = jax.random.split(jax.random.fold_in(key, salt))
    first_moment = 0.15 * jax.random.truncated_normal(key_first, -4.0, 4.0, shape_rows, jnp.float32)
    second_moment = jnp.exp(jax.random.uniform(key_second, shape_rows, jnp.float32, math.log(0.05), math.log(0.2)))
    return jnp.stack([first_moment, second_moment])


def draw_attn_moments(key, part):
    return moment_pair(key, (ATT_ROWS, D), 7)


def draw_ffn_moments(key, part):
    return moment_pair(key, (FFN_ROWS, D), 13)


def draw_gain_moments(key, part):
    return moment_pair(key, (2, D), 19)


def block_levels(key, extent, shards, least, largest):
    loudness = 1.0
    for position, blocks in shards:
        draws = jax.random.uniform(jax.random.fold_in(jax.random.fold_in(key, 6), position), (blocks,), jnp.float32, least / len(shards), largest / len(shards))
        loudness = loudness * jnp.repeat(jnp.exp(draws), extent[position] // blocks).reshape((-1,) + (1,) * (len(extent) - 1 - position))
    return loudness


def scatter_about(rng, shape, scale, bound, cuts=(), held_as=jnp.bfloat16):
    entries = jax.random.normal(rng, shape, jnp.float32) * scale
    if len(cuts) > 0:
        entries = block_levels(rng, shape, cuts, -0.22, 0.18) * entries
    return jnp.clip(entries, min=-bound, max=bound).astype(held_as)


def setup_inputs(seed: int = 0) -> dict:
    key_list = jax.random.split(jax.random.key(seed), 10)
    return {
        "block_input": draw_block_input(jax.random.fold_in(key_list[9], 71), 0),
        "cotangent": scatter_about(key_list[1], (SEQS, SEQUENCE_TOKENS, D), 1.0, 6.0, ((0, 4), (1, 8))),
        "documents": draw_documents(jax.random.fold_in(key_list[9], 71), 0),
        "attn_weights": draw_attn_weights(jax.random.fold_in(key_list[9], 71), 0),
        "ffn_weights": draw_ffn_weights(jax.random.fold_in(key_list[9], 71), 0),
        "norm_gains": scatter_about(key_list[5], (2, D), 0.1, 0.5, (), jnp.float32),
        "attn_moments": draw_attn_moments(jax.random.fold_in(key_list[9], 71), 0),
        "ffn_moments": draw_ffn_moments(jax.random.fold_in(key_list[9], 71), 0),
        "gain_moments": draw_gain_moments(jax.random.fold_in(key_list[9], 71), 0),
    }


NORM_EPS = 1e-05
ROPE_THETA = 100000.0
BETA_ONE = 0.9
BETA_TWO = 0.95
ADAM_EPS = 1e-08
LEARN_RATE = 0.02
WEIGHT_DECAY = 0.1

def rounded(tensor_in):
    return lax.optimization_barrier(tensor_in.astype(jnp.bfloat16)).astype(jnp.float32)

def product_transposed(left_matrix, right_matrix):
    return lax.dot_general(left_matrix, right_matrix, (((1,), (1,)), ((), ())), preferred_element_type=jnp.float32)

def transposed_times(left_matrix, right_matrix):
    return lax.dot_general(left_matrix, right_matrix, (((0,), (0,)), ((), ())), preferred_element_type=jnp.float32)

def plain_times(left_matrix, right_matrix):
    return jnp.dot(left_matrix, right_matrix, preferred_element_type=jnp.float32)

def rms_scale(tensor_in):
    return lax.rsqrt(lax.optimization_barrier(jnp.mean(tensor_in * tensor_in, axis=-1, keepdims=True)) + NORM_EPS)

def norm_backward(grad_in, normed, norm_scale, gain_row):
    scaled = grad_in * (1.0 + gain_row)
    return norm_scale * (scaled - normed * lax.optimization_barrier(jnp.mean(scaled * normed, axis=-1, keepdims=True)))

def rope_tables(positions):
    half_width = HEAD_SIZE // 2
    frequency = ROPE_THETA ** (-2.0 * jnp.arange(half_width, dtype=jnp.float32) / HEAD_SIZE)
    angles = positions.astype(jnp.float32)[:, None] * frequency[None, :]
    return (jnp.cos(angles), jnp.sin(angles))

def rotary_heads(tensor_in, cosine_lookup, sine_lookup, direction):
    half_width = HEAD_SIZE // 2
    first_half = tensor_in[..., :half_width]
    second_half = tensor_in[..., half_width:]
    cos_rows = cosine_lookup[:, None, :]
    sin_rows = sine_lookup[:, None, :] * direction
    return jnp.concatenate([first_half * cos_rows - second_half * sin_rows, second_half * cos_rows + first_half * sin_rows], axis=-1)

def doc_positions(doc_ids):
    index_row = jnp.arange(doc_ids.shape[0], dtype=jnp.int32)
    earlier = (doc_ids[None, :] < doc_ids[:, None]).astype(jnp.int32)
    starts = lax.optimization_barrier(jnp.sum(earlier, axis=1)).astype(jnp.int32)
    return (index_row - starts).astype(jnp.int32)

def attention_forward(query_matrix, keys_bfloat, values_bfloat, doc_ids):
    block_row_span = math.gcd(SEQUENCE_TOKENS, 512)
    heads_per_group = QUERY_HEADS // KEY_VALUE_HEADS
    keys_wide = keys_bfloat.astype(jnp.float32)
    values_wide = values_bfloat.astype(jnp.float32)
    key_index = jnp.arange(SEQUENCE_TOKENS, dtype=jnp.int32)

    def one_block(block_first_row):
        query_row_block = lax.dynamic_slice_in_dim(query_matrix, block_first_row, block_row_span, 0).astype(jnp.float32).reshape(block_row_span, KEY_VALUE_HEADS, heads_per_group, HEAD_SIZE)
        query_docs = lax.dynamic_slice_in_dim(doc_ids, block_first_row, block_row_span, 0)
        query_index = block_first_row + jnp.arange(block_row_span, dtype=jnp.int32)
        allowed = (key_index[None, :] <= query_index[:, None]) & (doc_ids[None, :] == query_docs[:, None])
        scores = jnp.einsum('qhgd,khd->hgqk', query_row_block, keys_wide) * HEAD_SIZE ** (-0.5)
        exponent = jnp.where(allowed[None, None], jnp.exp(scores), jnp.zeros_like(scores))
        totals = lax.optimization_barrier(jnp.sum(exponent, axis=-1))
        summed = jnp.einsum('hgqk,khd->hgqd', rounded(exponent), values_wide)
        output = (summed / totals[..., None]).transpose(2, 0, 1, 3).reshape(block_row_span, QUERY_HEADS * HEAD_SIZE)
        return (output.astype(jnp.bfloat16), jnp.log(totals))
    block_starts = jnp.arange(SEQUENCE_TOKENS // block_row_span, dtype=jnp.int32) * block_row_span
    outputs, log_blocks = lax.map(one_block, block_starts)
    return (outputs.reshape(SEQUENCE_TOKENS, QUERY_HEADS * HEAD_SIZE), log_blocks)

def attention_backward(query_matrix, keys_bfloat, values_bfloat, doc_ids, attended_rows, attended_gradient, log_blocks):
    block_row_span = math.gcd(SEQUENCE_TOKENS, 512)
    heads_per_group = QUERY_HEADS // KEY_VALUE_HEADS
    keys_wide = keys_bfloat.astype(jnp.float32)
    values_wide = values_bfloat.astype(jnp.float32)
    key_index = jnp.arange(SEQUENCE_TOKENS, dtype=jnp.int32)

    def one_block(acc_pair, block_items):
        key_acc, value_acc = acc_pair
        block_first_row, log_rows = block_items
        query_row_block = lax.dynamic_slice_in_dim(query_matrix, block_first_row, block_row_span, 0).astype(jnp.float32).reshape(block_row_span, KEY_VALUE_HEADS, heads_per_group, HEAD_SIZE)
        output_rows = lax.dynamic_slice_in_dim(attended_rows, block_first_row, block_row_span, 0).astype(jnp.float32).reshape(block_row_span, KEY_VALUE_HEADS, heads_per_group, HEAD_SIZE)
        gradient_rows = lax.dynamic_slice_in_dim(attended_gradient, block_first_row, block_row_span, 0).astype(jnp.float32).reshape(block_row_span, KEY_VALUE_HEADS, heads_per_group, HEAD_SIZE)
        query_docs = lax.dynamic_slice_in_dim(doc_ids, block_first_row, block_row_span, 0)
        query_index = block_first_row + jnp.arange(block_row_span, dtype=jnp.int32)
        allowed = (key_index[None, :] <= query_index[:, None]) & (doc_ids[None, :] == query_docs[:, None])
        scores = jnp.einsum('qhgd,khd->hgqk', query_row_block, keys_wide) * HEAD_SIZE ** (-0.5)
        row_delta = lax.optimization_barrier(jnp.sum(gradient_rows * output_rows, axis=-1)).transpose(1, 2, 0)
        probabilities = jnp.where(allowed[None, None], jnp.exp(scores - log_rows[..., None]), jnp.zeros_like(scores))
        grad_probs = jnp.einsum('qhgd,khd->hgqk', gradient_rows, values_wide)
        grad_scores = rounded(probabilities * (grad_probs - row_delta[..., None]) * HEAD_SIZE ** (-0.5))
        grad_query = jnp.einsum('hgqk,khd->qhgd', grad_scores, keys_wide).reshape(block_row_span, QUERY_HEADS, HEAD_SIZE)
        key_acc = key_acc + jnp.einsum('hgqk,qhgd->khd', grad_scores, query_row_block)
        value_acc = value_acc + jnp.einsum('hgqk,qhgd->khd', rounded(probabilities), gradient_rows)
        return ((key_acc, value_acc), grad_query)
    block_starts = jnp.arange(SEQUENCE_TOKENS // block_row_span, dtype=jnp.int32) * block_row_span
    zero_key_value = jnp.zeros_like(keys_wide)
    (key_gradient_rows, grad_values), grad_queries = lax.scan(one_block, (zero_key_value, zero_key_value), (block_starts, log_blocks))
    return (grad_queries.reshape(SEQUENCE_TOKENS, QUERY_HEADS, HEAD_SIZE), key_gradient_rows, grad_values)

def layer_sequence(seq_input, seq_cotangent, doc_ids, attn_bf, ffn_bf, norm_gains):
    query_width = QUERY_HEADS * HEAD_SIZE
    key_value_width = KEY_VALUE_HEADS * HEAD_SIZE
    w_query = attn_bf[:query_width]
    key_weight = attn_bf[query_width:query_width + key_value_width]
    value_weight = attn_bf[query_width + key_value_width:query_width + 2 * key_value_width]
    w_out = attn_bf[query_width + 2 * key_value_width:]
    w_gate = ffn_bf[:FF]
    w_up = ffn_bf[FF:2 * FF]
    w_down = ffn_bf[2 * FF:]
    residual = seq_input.astype(jnp.float32)
    scale_one = rms_scale(residual)
    normed_one = residual * scale_one
    first_hidden = (normed_one * (1.0 + norm_gains[0])).astype(jnp.bfloat16)
    cosine_lookup, sine_lookup = rope_tables(doc_positions(doc_ids))
    query_matrix = rotary_heads(product_transposed(first_hidden, w_query).reshape(SEQUENCE_TOKENS, QUERY_HEADS, HEAD_SIZE), cosine_lookup, sine_lookup, 1.0).astype(jnp.bfloat16)
    keys_bfloat = rotary_heads(product_transposed(first_hidden, key_weight).reshape(SEQUENCE_TOKENS, KEY_VALUE_HEADS, HEAD_SIZE), cosine_lookup, sine_lookup, 1.0).astype(jnp.bfloat16)
    values_bfloat = product_transposed(first_hidden, value_weight).astype(jnp.bfloat16).reshape(SEQUENCE_TOKENS, KEY_VALUE_HEADS, HEAD_SIZE)
    attended_rows, log_blocks = attention_forward(query_matrix, keys_bfloat, values_bfloat, doc_ids)
    middle = residual + plain_times(attended_rows, w_out)
    scale_two = rms_scale(middle)
    normed_two = middle * scale_two
    hidden_two = (normed_two * (1.0 + norm_gains[1])).astype(jnp.bfloat16)
    gate_pre = product_transposed(hidden_two, w_gate)
    up_pre = product_transposed(hidden_two, w_up)
    sigmoid_gate = jax.nn.sigmoid(gate_pre)
    activated = (gate_pre * sigmoid_gate * up_pre).astype(jnp.bfloat16)
    block_out = middle + plain_times(activated, w_down)
    grad_w_down = transposed_times(activated, seq_cotangent)
    grad_act = product_transposed(seq_cotangent, w_down)
    grad_gate = (grad_act * up_pre * sigmoid_gate * (1.0 + gate_pre * (1.0 - sigmoid_gate))).astype(jnp.bfloat16)
    grad_up = (grad_act * gate_pre * sigmoid_gate).astype(jnp.bfloat16)
    grad_w_gate = transposed_times(grad_gate, hidden_two)
    grad_w_up = transposed_times(grad_up, hidden_two)
    grad_hidden_two = plain_times(grad_gate, w_gate) + plain_times(grad_up, w_up)
    gain_two = lax.optimization_barrier(jnp.sum(grad_hidden_two * normed_two, axis=0))
    grad_middle = seq_cotangent.astype(jnp.float32) + norm_backward(grad_hidden_two, normed_two, scale_two, norm_gains[1])
    grad_middle_bf = grad_middle.astype(jnp.bfloat16)
    grad_w_out = transposed_times(attended_rows, grad_middle_bf)
    attended_gradient = product_transposed(grad_middle_bf, w_out).astype(jnp.bfloat16)
    grad_queries, key_gradient_rows, grad_values = attention_backward(query_matrix, keys_bfloat, values_bfloat, doc_ids, attended_rows, attended_gradient, log_blocks)
    grad_q_bf = rotary_heads(grad_queries, cosine_lookup, sine_lookup, -1.0).reshape(SEQUENCE_TOKENS, query_width).astype(jnp.bfloat16)
    grad_k_bf = rotary_heads(key_gradient_rows, cosine_lookup, sine_lookup, -1.0).reshape(SEQUENCE_TOKENS, key_value_width).astype(jnp.bfloat16)
    grad_v_bf = grad_values.reshape(SEQUENCE_TOKENS, key_value_width).astype(jnp.bfloat16)
    grad_attn = jnp.concatenate([transposed_times(grad_q_bf, first_hidden), transposed_times(grad_k_bf, first_hidden), transposed_times(grad_v_bf, first_hidden), grad_w_out], axis=0)
    grad_ffn = jnp.concatenate([grad_w_gate, grad_w_up, grad_w_down], axis=0)
    grad_hidden_one = plain_times(grad_q_bf, w_query) + plain_times(grad_k_bf, key_weight) + plain_times(grad_v_bf, value_weight)
    gain_one = lax.optimization_barrier(jnp.sum(grad_hidden_one * normed_one, axis=0))
    grad_input = grad_middle + norm_backward(grad_hidden_one, normed_one, scale_one, norm_gains[0])
    return (block_out, grad_input, grad_attn, grad_ffn, jnp.stack([gain_one, gain_two]))

def adamw_update(parameter, gradient, moments, decay_rate):
    first_moment = BETA_ONE * moments[0] + (1.0 - BETA_ONE) * gradient
    second_moment = BETA_TWO * moments[1] + (1.0 - BETA_TWO) * gradient * gradient
    first_hat = first_moment / (1.0 - BETA_ONE ** STEP)
    second_hat = second_moment / (1.0 - BETA_TWO ** STEP)
    updated = parameter - LEARN_RATE * (first_hat / (jnp.sqrt(second_hat) + ADAM_EPS) + decay_rate * parameter)
    return (updated, jnp.stack([first_moment, second_moment]))

def reference(block_input, cotangent, documents, attn_weights, ffn_weights, norm_gains, attn_moments, ffn_moments, gain_moments):
    attn_bf = attn_weights.astype(jnp.bfloat16)
    ffn_bf = ffn_weights.astype(jnp.bfloat16)
    grad_factor = float(TOKENS) ** (-0.5)

    def per_sequence(totals_carry, sequence_items):
        seq_input, seq_cotangent, seq_docs = sequence_items
        block_out, grad_input, grad_attn, grad_ffn, grad_gains = layer_sequence(seq_input, seq_cotangent, seq_docs, attn_bf, ffn_bf, norm_gains)
        return ((totals_carry[0] + grad_attn * grad_factor, totals_carry[1] + grad_ffn * grad_factor, totals_carry[2] + grad_gains * grad_factor), (block_out, grad_input))
    start_totals = (jnp.zeros_like(attn_weights), jnp.zeros_like(ffn_weights), jnp.zeros_like(norm_gains))
    (attn_grad, ffn_grad, gain_grad), (block_output, input_grad) = lax.scan(per_sequence, start_totals, (block_input, cotangent, documents))
    new_attn, new_attn_moments = adamw_update(attn_weights, attn_grad, attn_moments, WEIGHT_DECAY)
    new_ffn, new_ffn_moments = adamw_update(ffn_weights, ffn_grad, ffn_moments, WEIGHT_DECAY)
    new_gains, new_gain_moments = adamw_update(norm_gains, gain_grad, gain_moments, 0.0)
    return (block_output, input_grad, attn_grad, ffn_grad, gain_grad, new_attn, new_ffn, new_gains, new_attn_moments, new_ffn_moments, new_gain_moments)
```

```python
import functools

import jax
import jax.numpy as jnp
import numpy as np
from jax import lax
from jax.experimental import pallas as pl
from jax.experimental.pallas import tpu as pltpu
from jax.sharding import PartitionSpec as P

QUERY_HEADS = 16
KEY_VALUE_HEADS = 8
HEAD_SIZE = 96
STEP = 3

NORM_EPS = 1e-05
ROPE_THETA = 100000.0
BETA_ONE = 0.9
BETA_TWO = 0.95
ADAM_EPS = 1e-08
LEARN_RATE = 0.02
WEIGHT_DECAY = 0.1

LANES = 128
TILE = 256
CHUNK = 16
VMEM_LIMIT = 62 * 1024 * 1024
EVERY = ("fsdp", "context")
BF = jnp.bfloat16
F32 = jnp.float32
ID_TYPE = pl.DeviceIdType.MESH


def product_transposed(left_matrix, right_matrix):
    return lax.dot_general(
        left_matrix, right_matrix, (((1,), (1,)), ((), ())), preferred_element_type=F32
    )


def transposed_times(left_matrix, right_matrix):
    return lax.dot_general(
        left_matrix, right_matrix, (((0,), (0,)), ((), ())), preferred_element_type=F32
    )


def plain_times(left_matrix, right_matrix):
    return jnp.dot(left_matrix, right_matrix, preferred_element_type=F32)


def rms_scale(tensor_in):
    return lax.rsqrt(jnp.mean(tensor_in * tensor_in, axis=-1, keepdims=True) + NORM_EPS)


def norm_backward(grad_in, normed, norm_scale, gain_row):
    scaled = grad_in * (1.0 + gain_row)
    return norm_scale * (scaled - normed * jnp.mean(scaled * normed, axis=-1, keepdims=True))


def adamw_update(parameter, gradient, moments, decay_rate):
    first_moment = BETA_ONE * moments[0] + (1.0 - BETA_ONE) * gradient
    second_moment = BETA_TWO * moments[1] + (1.0 - BETA_TWO) * gradient * gradient
    first_hat = first_moment / (1.0 - BETA_ONE**STEP)
    second_hat = second_moment / (1.0 - BETA_TWO**STEP)
    updated = parameter - LEARN_RATE * (
        first_hat / (jnp.sqrt(second_hat) + ADAM_EPS) + decay_rate * parameter
    )
    return (updated, jnp.stack([first_moment, second_moment]))


class UnitPlan:
    def __init__(self, homes, devices):
        waiting = [[] for _ in range(devices)]
        for unit, (device, place) in enumerate(homes):
            waiting[unit // 3].append((unit % 3, device, place))
        self.rounds = []
        for _ in range(3):
            taken = [None] * devices

            def settle(source, seen):
                for piece, device, place in waiting[source]:
                    if device in seen:
                        continue
                    seen.add(device)
                    if taken[device] is None or settle(taken[device][0], seen):
                        taken[device] = (source, piece, place)
                        return True
                return False

            for source in range(devices):
                if not settle(source, set()):
                    raise ValueError("no matching")
            pairs, pieces, places = [], [0] * devices, [0] * devices
            for device, (source, piece, place) in enumerate(taken):
                pairs.append((source, device))
                pieces[source] = piece
                places[device] = place
                waiting[source].remove((piece, device, place))
            self.rounds.append((pairs, np.array(pieces), np.array(places)))

    def _reorder(self, got, columns):
        order = np.argsort(np.stack(columns, axis=1), axis=1).astype(np.int32)
        mine = jnp.asarray(order)[lax.axis_index(EVERY)]
        stacked = jnp.stack(got)
        return jnp.concatenate(
            [lax.dynamic_index_in_dim(stacked, mine[k], 0, keepdims=False) for k in range(3)]
        )

    def spread(self, rows):
        pieces = rows.reshape(3, rows.shape[0] // 3, rows.shape[1])
        me = lax.axis_index(EVERY)
        got = []
        for pairs, piece, _ in self.rounds:
            unit = lax.dynamic_index_in_dim(
                pieces, jnp.asarray(piece, jnp.int32)[me], 0, keepdims=False
            )
            got.append(lax.ppermute(unit, EVERY, pairs))
        return self._reorder(got, [place for _, _, place in self.rounds])

    def collect(self, rows):
        places_of = rows.reshape(3, rows.shape[0] // 3, rows.shape[1])
        me = lax.axis_index(EVERY)
        got = []
        for pairs, _, place in self.rounds:
            unit = lax.dynamic_index_in_dim(
                places_of, jnp.asarray(place, jnp.int32)[me], 0, keepdims=False
            )
            got.append(lax.ppermute(unit, EVERY, [(b, a) for a, b in pairs]))
        return self._reorder(got, [piece for _, piece, _ in self.rounds])


def unit_plans(layers, columns, attn_rows, ffn_rows):
    devices = layers * columns

    def home(column, position):
        return ((position // 3) * columns + column, position % 3)

    homes = []
    for unit in range(3 * devices):
        matrix, rest = divmod(unit, devices)
        stretch, column = divmod(rest, columns)
        homes.append(home(column, matrix * layers + stretch))
    ffn_plan = UnitPlan(homes, devices)
    unit_rows = attn_rows // (3 * devices)
    query_units = QUERY_HEADS * HEAD_SIZE // columns // unit_rows
    share_units = KEY_VALUE_HEADS * HEAD_SIZE // columns // unit_rows
    homes = []
    position = 0
    for count in (query_units, share_units, share_units, query_units):
        for column in range(columns):
            for k in range(count):
                homes.append(home(column, position + k))
        position += count
    return UnitPlan(homes, devices), ffn_plan


def partner(me, step, chips):
    return lax.rem(me // 2 + step, chips) * 2 + lax.rem(me, 2)


def sibling_of(me):
    return me + 1 - 2 * lax.rem(me, 2)


def rows_at(index, rows):
    return pl.ds(pl.multiple_of(index * rows, rows), rows)


def greet(columns, layers=1):
    barrier = pltpu.get_barrier_semaphore()
    me = lax.axis_index("context")
    for step in range(1, columns):
        pl.semaphore_signal(
            barrier, inc=1, device_id={"context": lax.rem(me + step, columns)}, device_id_type=ID_TYPE
        )
    if layers > 1:
        layer = lax.axis_index("fsdp")
        for step in range(1, layers):
            pl.semaphore_signal(
                barrier, inc=1, device_id={"fsdp": lax.rem(layer + step, layers)}, device_id_type=ID_TYPE
            )
    pl.semaphore_wait(barrier, columns - 1 + layers - 1)


def send(source, target, send_sem, recv_sem, device):
    copy = pltpu.make_async_remote_copy(
        src_ref=source,
        dst_ref=target,
        send_sem=send_sem,
        recv_sem=recv_sem,
        device_id=device,
        device_id_type=ID_TYPE,
    )
    copy.start()
    return copy


class Gather:
    @staticmethod
    def scratch(chips):
        return [
            pltpu.SemaphoreType.DMA((chips,)),
            pltpu.SemaphoreType.DMA((chips,)),
            pltpu.SemaphoreType.DMA((chips,)),
            pltpu.SemaphoreType.DMA((chips,)),
            pltpu.SemaphoreType.DMA,
        ]

    def __init__(self, block, full, chips, sems):
        own_send, own_recv, self.on_send, self.on_recv, local_sem = sems
        me = lax.axis_index("context")
        rows = block.shape[0]
        self.block, self.full, self.chips, self.me, self.rows = block, full, chips, me, rows
        mine = full.at[rows_at(me, rows), :]
        self.own = [
            send(block, mine, own_send.at[step], own_recv.at[step], {"context": partner(me, step, chips)})
            for step in range(1, chips)
        ]
        self.own.append(
            send(block, mine, own_send.at[0], own_recv.at[0], {"context": sibling_of(me)})
        )
        self.local = pltpu.make_async_copy(block, mine, local_sem)
        self.local.start()

    def finish(self):
        passed = []
        for step in range(1, self.chips):
            self.own[step - 1].wait_recv()
            source = partner(self.me, self.chips - step, self.chips)
            there = self.full.at[rows_at(source, self.rows), :]
            passed.append(
                send(there, there, self.on_send.at[step], self.on_recv.at[step], {"context": sibling_of(self.me)})
            )
        self.own[-1].wait_recv()
        for copy in passed:
            copy.wait_recv()
        for copy in self.own + passed:
            copy.wait_send()
        self.local.wait()


class Reduce:
    @staticmethod
    def scratch(chips, rows, width):
        return [
            pltpu.VMEM((chips, rows, width), BF),
            pltpu.VMEM((chips, rows, width), BF),
            pltpu.VMEM((chips, rows, width), BF),
            pltpu.SemaphoreType.DMA((chips,)),
            pltpu.SemaphoreType.DMA((chips,)),
            pltpu.SemaphoreType.DMA((chips,)),
            pltpu.SemaphoreType.DMA((chips,)),
        ]

    def __init__(self, part, chips, rows, scratch):
        self.near, self.summed, self.far, near_send, near_recv, self.far_send, self.far_recv = scratch
        me = lax.axis_index("context")
        self.part, self.chips, self.rows, self.me = part, chips, rows, me
        self.near_copies = {}
        for step in [*range(1, chips), 0]:
            block = partner(sibling_of(me), step, chips)
            self.near_copies[step] = send(
                part.at[rows_at(block, rows), :],
                self.near.at[step],
                near_send.at[step],
                near_recv.at[step],
                {"context": sibling_of(me)},
            )
        self.far_copies = []

    def exchange(self):
        for step in range(1, self.chips):
            self.near_copies[step].wait_recv()
            target = partner(self.me, step, self.chips)
            first = pl.multiple_of(target * self.rows, self.rows)

            @pl.loop(0, self.rows // CHUNK)
            def add(k):
                at = pl.ds(pl.multiple_of(k * CHUNK, CHUNK), CHUNK)
                from_part = pl.ds(pl.multiple_of(first + k * CHUNK, CHUNK), CHUNK)
                self.summed[step, at, :] = (
                    self.part[from_part, :].astype(F32) + self.near[step, at, :].astype(F32)
                ).astype(BF)

            self.far_copies.append(
                send(
                    self.summed.at[step],
                    self.far.at[step],
                    self.far_send.at[step],
                    self.far_recv.at[step],
                    {"context": target},
                )
            )

    def arrive(self):
        self.near_copies[0].wait_recv()
        for copy in self.far_copies:
            copy.wait_recv()

    def total(self, k):
        at = pl.ds(pl.multiple_of(k * CHUNK, CHUNK), CHUNK)
        first = pl.multiple_of(self.me * self.rows, self.rows)
        value = self.part[pl.ds(pl.multiple_of(first + k * CHUNK, CHUNK), CHUNK), :].astype(F32)
        value = value + self.near[0, at, :].astype(F32)
        for step in range(1, self.chips):
            value = value + self.far[step, at, :].astype(F32)
        return value

    def drain(self):
        for copy in list(self.near_copies.values()) + self.far_copies:
            copy.wait_send()


def chunk_rows(k):
    return pl.ds(pl.multiple_of(k * CHUNK, CHUNK), CHUNK)


def vmem_specs(count):
    return [pl.BlockSpec(memory_space=pltpu.VMEM)] * count


def comm_params(collective_id):
    return pltpu.CompilerParams(
        collective_id=collective_id, has_side_effects=True, vmem_limit_bytes=VMEM_LIMIT
    )


def gather_kernel(columns, block, docs, full, docs_full, *scratch):
    chips = columns // 2
    docs_send, docs_recv, docs_local = scratch[-3:]
    greet(columns)
    gather = Gather(block, full, chips, scratch[:-3])
    me = lax.axis_index("context")
    mine = docs_full.at[pl.ds(me, 1), :]
    copies = [
        send(docs, mine, docs_send.at[step], docs_recv.at[step], {"context": lax.rem(me + step, columns)})
        for step in range(1, columns)
    ]
    local = pltpu.make_async_copy(docs, mine, docs_local)
    local.start()
    gather.finish()
    for copy in copies:
        copy.wait_recv()
    for copy in copies:
        copy.wait_send()
    local.wait()


def gather_first(block, docs, columns):
    rows, width = block.shape
    return pl.pallas_call(
        functools.partial(gather_kernel, columns),
        out_shape=(
            jax.ShapeDtypeStruct((columns * rows, width), BF),
            jax.ShapeDtypeStruct((columns, docs.shape[1]), jnp.int32),
        ),
        in_specs=vmem_specs(2),
        out_specs=(pl.BlockSpec(memory_space=pl.ANY), pl.BlockSpec(memory_space=pl.ANY)),
        scratch_shapes=[
            *Gather.scratch(columns // 2),
            pltpu.SemaphoreType.DMA((columns,)),
            pltpu.SemaphoreType.DMA((columns,)),
            pltpu.SemaphoreType.DMA,
        ],
        compiler_params=comm_params(1),
        name="gather_first",
        cost_estimate=pl.CostEstimate(flops=0, bytes_accessed=60_000_000, transcendentals=0),
    )(block, docs)


def gather_plain_kernel(columns, block, full, *scratch):
    greet(columns)
    gather = Gather(block, full, columns // 2, scratch)
    gather.finish()


def gather_plain(block, columns):
    rows, width = block.shape
    return pl.pallas_call(
        functools.partial(gather_plain_kernel, columns),
        out_shape=jax.ShapeDtypeStruct((columns * rows, width), BF),
        in_specs=vmem_specs(1),
        out_specs=pl.BlockSpec(memory_space=pl.ANY),
        scratch_shapes=Gather.scratch(columns // 2),
        compiler_params=comm_params(2),
        name="gather_plain",
        cost_estimate=pl.CostEstimate(flops=0, bytes_accessed=60_000_000, transcendentals=0),
    )(block)


def middle_kernel(columns, part, x_ref, gain_ref, middle_ref, full, hidden, *scratch):
    chips = columns // 2
    rows = x_ref.shape[0]
    greet(columns)
    reduce = Reduce(part, chips, rows, scratch[:7])
    reduce.exchange()
    reduce.arrive()

    @pl.loop(0, rows // CHUNK)
    def finish(k):
        at = chunk_rows(k)
        middle = x_ref[at, :].astype(F32) + reduce.total(k)
        middle_ref[at, :] = middle
        hidden[at, :] = (middle * rms_scale(middle) * (1.0 + gain_ref[...])).astype(BF)

    gather = Gather(hidden, full, chips, scratch[7:])
    gather.finish()
    reduce.drain()


def middle_step(part, x_own, gain_row, columns):
    rows, width = x_own.shape
    chips = columns // 2
    return pl.pallas_call(
        functools.partial(middle_kernel, columns),
        out_shape=(
            jax.ShapeDtypeStruct((rows, width), F32),
            jax.ShapeDtypeStruct((columns * rows, width), BF),
        ),
        in_specs=vmem_specs(3),
        out_specs=(pl.BlockSpec(memory_space=pltpu.VMEM), pl.BlockSpec(memory_space=pl.ANY)),
        scratch_shapes=[
            pltpu.VMEM((rows, width), BF),
            *Reduce.scratch(chips, rows, width),
            *Gather.scratch(chips),
        ],
        compiler_params=comm_params(3),
        name="middle_step",
        cost_estimate=pl.CostEstimate(flops=0, bytes_accessed=150_000_000, transcendentals=0),
    )(part, x_own, gain_row)


def turn_kernel(columns, part, middle_ref, dy_ref, gain_ref, grad_ref, sums_ref, full, grad_bf, *scratch):
    chips = columns // 2
    rows = middle_ref.shape[0]
    greet(columns)
    reduce = Reduce(part, chips, rows, scratch[:7])
    sums_ref[...] = jnp.zeros_like(sums_ref)
    reduce.exchange()
    reduce.arrive()

    @pl.loop(0, rows // CHUNK)
    def finish(k):
        at = chunk_rows(k)
        grad_hidden = reduce.total(k)
        middle = middle_ref[at, :]
        scale = rms_scale(middle)
        normed = middle * scale
        sums_ref[0:1, :] += jnp.sum(grad_hidden * normed, axis=0, keepdims=True)
        grad = dy_ref[at, :].astype(F32) + norm_backward(grad_hidden, normed, scale, gain_ref[...])
        grad_ref[at, :] = grad
        grad_bf[at, :] = grad.astype(BF)

    gather = Gather(grad_bf, full, chips, scratch[7:])
    gather.finish()
    reduce.drain()


def turn_step(part, middle, dy_own, gain_row, columns):
    rows, width = middle.shape
    chips = columns // 2
    return pl.pallas_call(
        functools.partial(turn_kernel, columns),
        out_shape=(
            jax.ShapeDtypeStruct((rows, width), F32),
            jax.ShapeDtypeStruct((8, width), F32),
            jax.ShapeDtypeStruct((columns * rows, width), BF),
        ),
        in_specs=vmem_specs(4),
        out_specs=(*vmem_specs(2), pl.BlockSpec(memory_space=pl.ANY)),
        scratch_shapes=[
            pltpu.VMEM((rows, width), BF),
            *Reduce.scratch(chips, rows, width),
            *Gather.scratch(chips),
        ],
        compiler_params=comm_params(4),
        name="turn_step",
        cost_estimate=pl.CostEstimate(flops=0, bytes_accessed=150_000_000, transcendentals=0),
    )(part, middle, dy_own, gain_row)


def last_kernel(
    columns,
    layers,
    part_in,
    part_out,
    x_ref,
    middle_ref,
    grad_ref,
    gain_ref,
    sums_ref,
    input_grad_ref,
    block_out_ref,
    gains_ref,
    own_sums,
    plane_slots,
    plane_sums,
    line_slots,
    plane_send,
    plane_recv,
    line_send,
    line_recv,
    *scratch,
):
    chips = columns // 2
    rows = x_ref.shape[0]
    greet(columns, layers)
    first = Reduce(part_in, chips, rows, scratch[:7])
    second = Reduce(part_out, chips, rows, scratch[7:])
    first.exchange()
    second.exchange()
    own_sums[...] = jnp.zeros_like(own_sums)
    own_sums[1:2, :] = sums_ref[0:1, :]
    first.arrive()

    @pl.loop(0, rows // CHUNK)
    def finish(k):
        at = chunk_rows(k)
        grad_hidden = first.total(k)
        residual = x_ref[at, :].astype(F32)
        scale = rms_scale(residual)
        normed = residual * scale
        own_sums[0:1, :] += jnp.sum(grad_hidden * normed, axis=0, keepdims=True)
        input_grad_ref[at, :] = grad_ref[at, :] + norm_backward(
            grad_hidden, normed, scale, gain_ref[...]
        )

    me = lax.axis_index("context")
    layer = lax.axis_index("fsdp")
    in_plane = [
        send(
            own_sums,
            plane_slots.at[step],
            plane_send.at[step],
            plane_recv.at[step],
            {"context": lax.rem(me + step, columns)},
        )
        for step in range(1, columns)
    ]
    second.arrive()

    @pl.loop(0, rows // CHUNK)
    def finish_out(k):
        at = chunk_rows(k)
        block_out_ref[at, :] = middle_ref[at, :] + second.total(k)

    total = own_sums[...]
    for step, copy in enumerate(in_plane):
        copy.wait_recv()
        total = total + plane_slots[step + 1]
    plane_sums[...] = total
    in_line = [
        send(
            plane_sums,
            line_slots.at[step],
            line_send.at[step],
            line_recv.at[step],
            {"fsdp": lax.rem(layer + step, layers)},
        )
        for step in range(1, layers)
    ]
    for step, copy in enumerate(in_line):
        copy.wait_recv()
        total = total + line_slots[step + 1]
    gains_ref[...] = total
    for copy in in_plane + in_line:
        copy.wait_send()
    first.drain()
    second.drain()


def last_step(part_in, part_out, x_own, middle, grad_middle, gain_row, sums, columns, layers):
    rows, width = x_own.shape
    chips = columns // 2
    return pl.pallas_call(
        functools.partial(last_kernel, columns, layers),
        out_shape=(
            jax.ShapeDtypeStruct((rows, width), F32),
            jax.ShapeDtypeStruct((rows, width), F32),
            jax.ShapeDtypeStruct((8, width), F32),
        ),
        in_specs=vmem_specs(7),
        out_specs=tuple(vmem_specs(3)),
        scratch_shapes=[
            pltpu.VMEM((8, width), F32),
            pltpu.VMEM((columns, 8, width), F32),
            pltpu.VMEM((8, width), F32),
            pltpu.VMEM((layers, 8, width), F32),
            pltpu.SemaphoreType.DMA((columns,)),
            pltpu.SemaphoreType.DMA((columns,)),
            pltpu.SemaphoreType.DMA((layers,)),
            pltpu.SemaphoreType.DMA((layers,)),
            *Reduce.scratch(chips, rows, width),
            *Reduce.scratch(chips, rows, width),
        ],
        compiler_params=comm_params(5),
        name="last_step",
        cost_estimate=pl.CostEstimate(flops=0, bytes_accessed=150_000_000, transcendentals=0),
    )(part_in, part_out, x_own, middle, grad_middle, gain_row, sums)


def turned(heads, low):
    return jnp.where(low, pltpu.roll(heads, LANES - HEAD_SIZE // 2, 1), pltpu.roll(heads, HEAD_SIZE // 2, 1))


def allowed_tile(start_ref, row_first, col_first):
    rows = row_first + lax.broadcasted_iota(jnp.int32, (TILE, TILE), 0)
    cols = col_first + lax.broadcasted_iota(jnp.int32, (TILE, TILE), 1)
    starts = jnp.broadcast_to(start_ref[row_first : row_first + TILE, 0:1], (TILE, TILE))
    return (cols <= rows) & (cols >= starts)


def attend_kernel(
    heads, h_ref, w_ref, cos_ref, sin_ref, start_ref, q_ref, k_ref, v_ref, att_ref, log_ref, part_ref, pad_ref
):
    seq = h_ref.shape[0]
    scale = HEAD_SIZE**-0.5
    for slot in range(2 * heads + 2):
        pad_ref[slot * LANES : slot * LANES + HEAD_SIZE, :] = w_ref[
            slot * HEAD_SIZE : (slot + 1) * HEAD_SIZE, :
        ]
        pad_ref[slot * LANES + HEAD_SIZE : (slot + 1) * LANES, :] = jnp.zeros(
            (LANES - HEAD_SIZE, w_ref.shape[1]), BF
        )
    width = (heads + 2) * LANES

    @pl.loop(0, seq // TILE)
    def project(i):
        at = pl.ds(pl.multiple_of(i * TILE, TILE), TILE)
        low = lax.broadcasted_iota(jnp.int32, (TILE, LANES), 1) < HEAD_SIZE // 2
        projected = product_transposed(h_ref[at, :], pad_ref[0:width, :])
        cosine, sine = cos_ref[at, :], sin_ref[at, :]
        for head in range(heads + 1):
            u = projected[:, head * LANES : (head + 1) * LANES]
            r = (u * cosine + turned(u, low) * sine).astype(BF)
            if head < heads:
                q_ref[at, head * LANES : (head + 1) * LANES] = r
            else:
                k_ref[at, :] = r
        v_ref[at, :] = projected[:, (heads + 1) * LANES :].astype(BF)

    for i in range(seq // TILE):
        rows = slice(i * TILE, (i + 1) * TILE)
        for head in range(heads):
            lanes = slice(head * LANES, (head + 1) * LANES)
            q = q_ref[rows, lanes]
            out = jnp.zeros((TILE, LANES), F32)
            total = jnp.zeros((TILE, 1), F32)
            for j in range(i + 1):
                keys = slice(j * TILE, (j + 1) * TILE)
                s = product_transposed(q, k_ref[keys, :]) * scale
                e = jnp.where(allowed_tile(start_ref, i * TILE, j * TILE), jnp.exp(s), 0.0)
                total = total + jnp.sum(e, axis=1, keepdims=True)
                out = out + plain_times(e.astype(BF), v_ref[keys, :])
            att_ref[rows, lanes] = (out / total).astype(BF)
            log_ref[rows, lanes] = jnp.broadcast_to(jnp.log(total), (TILE, LANES))

    @pl.loop(0, seq // TILE)
    def project_out(i):
        at = pl.ds(pl.multiple_of(i * TILE, TILE), TILE)
        part_ref[at, :] = plain_times(att_ref[at, :], pad_ref[width:, :]).astype(BF)


def attend(h_full, w_col, cosine, sine, starts, heads):
    seq, width = h_full.shape
    return pl.pallas_call(
        functools.partial(attend_kernel, heads),
        out_shape=(
            jax.ShapeDtypeStruct((seq, heads * LANES), BF),
            jax.ShapeDtypeStruct((seq, LANES), BF),
            jax.ShapeDtypeStruct((seq, LANES), BF),
            jax.ShapeDtypeStruct((seq, heads * LANES), BF),
            jax.ShapeDtypeStruct((seq, heads * LANES), F32),
            jax.ShapeDtypeStruct((seq, width), BF),
            jax.ShapeDtypeStruct(((2 * heads + 2) * LANES, width), BF),
        ),
        in_specs=vmem_specs(5),
        out_specs=tuple(vmem_specs(7)),
        compiler_params=pltpu.CompilerParams(vmem_limit_bytes=VMEM_LIMIT),
        name="attend",
        cost_estimate=pl.CostEstimate(flops=6_000_000_000, bytes_accessed=20_000_000, transcendentals=2_000_000),
    )(h_full, w_col, cosine, sine, starts)


def attend_back_kernel(
    heads,
    grad_ref,
    pad_ref,
    cos_ref,
    sin_ref,
    start_ref,
    q_ref,
    k_ref,
    v_ref,
    att_ref,
    log_ref,
    out_ref,
    ga_ref,
    dk_ref,
    dv_ref,
):
    seq = grad_ref.shape[0]
    scale = HEAD_SIZE**-0.5
    width = (heads + 2) * LANES

    @pl.loop(0, seq // TILE)
    def attended_gradient(i):
        at = pl.ds(pl.multiple_of(i * TILE, TILE), TILE)
        ga_ref[at, :] = product_transposed(grad_ref[at, :], pad_ref[width:, :]).astype(BF)

    dk_ref[...] = jnp.zeros_like(dk_ref)
    dv_ref[...] = jnp.zeros_like(dv_ref)
    low = lax.broadcasted_iota(jnp.int32, (TILE, LANES), 1) < HEAD_SIZE // 2

    def turn_back(u, rows):
        return (u * cos_ref[rows, :] - turned(u, low) * sin_ref[rows, :]).astype(BF)

    for i in range(seq // TILE):
        rows = slice(i * TILE, (i + 1) * TILE)
        for head in range(heads):
            lanes = slice(head * LANES, (head + 1) * LANES)
            q = q_ref[rows, lanes]
            ga = ga_ref[rows, lanes]
            delta = jnp.sum(ga.astype(F32) * att_ref[rows, lanes].astype(F32), axis=1, keepdims=True)
            logs = log_ref[rows, head * LANES : head * LANES + 1]
            dq = jnp.zeros((TILE, LANES), F32)
            for j in range(i + 1):
                keys = slice(j * TILE, (j + 1) * TILE)
                s = product_transposed(q, k_ref[keys, :]) * scale
                p = jnp.where(allowed_tile(start_ref, i * TILE, j * TILE), jnp.exp(s - logs), 0.0)
                dp = product_transposed(ga, v_ref[keys, :])
                ds = (p * (dp - delta) * scale).astype(BF)
                dq = dq + plain_times(ds, k_ref[keys, :])
                dk_ref[keys, :] += transposed_times(ds, q)
                dv_ref[keys, :] += transposed_times(p.astype(BF), ga)
            out_ref[rows, lanes] = turn_back(dq, rows)
    for i in range(seq // TILE):
        rows = slice(i * TILE, (i + 1) * TILE)
        out_ref[rows, heads * LANES : (heads + 1) * LANES] = turn_back(dk_ref[rows, :], rows)
        out_ref[rows, (heads + 1) * LANES :] = dv_ref[rows, :].astype(BF)


def attend_back(grad_full, padded, cosine, sine, starts, saved, heads):
    seq = grad_full.shape[0]
    return pl.pallas_call(
        functools.partial(attend_back_kernel, heads),
        out_shape=jax.ShapeDtypeStruct((seq, (heads + 2) * LANES), BF),
        in_specs=vmem_specs(10),
        out_specs=pl.BlockSpec(memory_space=pltpu.VMEM),
        scratch_shapes=[
            pltpu.VMEM((seq, heads * LANES), BF),
            pltpu.VMEM((seq, LANES), F32),
            pltpu.VMEM((seq, LANES), F32),
        ],
        compiler_params=pltpu.CompilerParams(vmem_limit_bytes=VMEM_LIMIT),
        name="attend_back",
        cost_estimate=pl.CostEstimate(flops=8_000_000_000, bytes_accessed=20_000_000, transcendentals=2_000_000),
    )(grad_full, padded, cosine, sine, starts, *saved)


def rope_tables(positions):
    half_width = HEAD_SIZE // 2
    frequency = ROPE_THETA ** (-2.0 * jnp.arange(half_width, dtype=F32) / HEAD_SIZE)
    angles = positions.astype(F32)[:, None] * frequency[None, :]
    cosine, sine = jnp.cos(angles), jnp.sin(angles)
    blank = jnp.zeros((positions.shape[0], LANES - HEAD_SIZE), F32)
    return (
        jnp.concatenate([cosine, cosine, blank], axis=1),
        jnp.concatenate([-sine, sine, blank], axis=1),
    )


def unpadded(rows, count):
    return jnp.concatenate([rows[k * LANES : k * LANES + HEAD_SIZE] for k in range(count)])


def on_device(
    block_input,
    cotangent,
    documents,
    attn_weights,
    ffn_weights,
    norm_gains,
    attn_moments,
    ffn_moments,
    gain_moments,
):
    layers, columns = lax.axis_size("fsdp"), lax.axis_size("context")
    rows, width = block_input.shape[1:]
    seq = rows * columns
    heads = QUERY_HEADS // columns
    sharers = max(1, columns // KEY_VALUE_HEADS)
    share = KEY_VALUE_HEADS * HEAD_SIZE // columns
    hidden = ffn_weights.shape[0] * layers // 3
    grad_factor = float(rows * layers * columns) ** (-0.5)
    attn_plan, ffn_plan = unit_plans(
        layers, columns, attn_weights.shape[0] * layers * columns, ffn_weights.shape[0] * layers * columns
    )
    core = lax.rem(lax.axis_index("context"), 2)
    swap = [(c, c + 1 - 2 * (c % 2)) for c in range(columns)]

    attn_col = lax.all_gather(
        attn_plan.spread(attn_weights.astype(BF)), "fsdp", axis=0, tiled=True
    )
    ffn_col = lax.all_gather(ffn_plan.spread(ffn_weights.astype(BF)), "fsdp", axis=0, tiled=True)
    query_rows = heads * HEAD_SIZE
    if sharers > 1:
        own_part = attn_col[query_rows : query_rows + 2 * share]
        other = lax.ppermute(own_part, "context", swap)

        def whole_head(first):
            mine, theirs = own_part[first : first + share], other[first : first + share]
            return jnp.where(
                core == 0, jnp.concatenate([mine, theirs]), jnp.concatenate([theirs, mine])
            )

        attn_col = jnp.concatenate(
            [
                attn_col[:query_rows],
                whole_head(0),
                whole_head(share),
                attn_col[query_rows + 2 * share :],
            ]
        )
    w_gate, w_up, w_down = ffn_col[:hidden], ffn_col[hidden : 2 * hidden], ffn_col[2 * hidden :]

    x_own = block_input[0]
    residual = x_own.astype(F32)
    first_hidden = (residual * rms_scale(residual) * (1.0 + norm_gains[0])).astype(BF)
    h_full, docs_full = gather_first(first_hidden, documents, columns)
    all_docs = docs_full.reshape(seq)
    starts = jnp.sum((all_docs[None, :] < all_docs[:, None]).astype(jnp.int32), axis=1)
    cosine, sine = rope_tables(jnp.arange(seq, dtype=jnp.int32) - starts)
    start_lanes = jnp.broadcast_to(starts[:, None], (seq, LANES))
    q_all, k_all, v_all, attended, logs, part, padded = attend(
        h_full, attn_col, cosine, sine, start_lanes, heads
    )
    middle, h2_full = middle_step(part, x_own, norm_gains[1:2], columns)
    dy_full = gather_plain(cotangent[0], columns)

    gate_pre = product_transposed(h2_full, w_gate)
    up_pre = product_transposed(h2_full, w_up)
    sigmoid_gate = jax.nn.sigmoid(gate_pre)
    activated = (gate_pre * sigmoid_gate * up_pre).astype(BF)
    grad_act = product_transposed(dy_full, w_down)
    grad_gate = (grad_act * up_pre * sigmoid_gate * (1.0 + gate_pre * (1.0 - sigmoid_gate))).astype(BF)
    grad_up = (grad_act * gate_pre * sigmoid_gate).astype(BF)
    ffn_term = jnp.concatenate(
        [
            (transposed_times(grad_gate, h2_full) * grad_factor).astype(BF),
            (transposed_times(grad_up, h2_full) * grad_factor).astype(BF),
            (transposed_times(activated, dy_full) * grad_factor).astype(BF),
        ]
    )
    ffn_sum = lax.psum_scatter(ffn_term, "fsdp", scatter_dimension=0, tiled=True)
    out_part = plain_times(activated, w_down).astype(BF)
    back_part = (plain_times(grad_gate, w_gate) + plain_times(grad_up, w_up)).astype(BF)
    grad_middle, sums, gm_full = turn_step(back_part, middle, cotangent[0], norm_gains[1:2], columns)

    grads = attend_back(
        gm_full, padded, cosine, sine, start_lanes, (q_all, k_all, v_all, attended, logs), heads
    )
    if sharers > 1:
        shared = grads[:, heads * LANES :]
        shared = (shared.astype(F32) + lax.ppermute(shared, "context", swap).astype(F32)).astype(BF)
        lane = jnp.arange(2 * LANES, dtype=jnp.int32) % LANES // share
        grads = jnp.concatenate(
            [grads[:, : heads * LANES], jnp.where(lane == core, shared, jnp.zeros_like(shared))], axis=1
        )
    term_in = (transposed_times(grads, h_full) * grad_factor).astype(BF)
    term_out = (transposed_times(attended, gm_full) * grad_factor).astype(BF)
    if sharers > 1:
        own_rows = [
            lax.dynamic_slice_in_dim(term_in, (heads + k) * LANES + core * share, share, 0)
            for k in range(2)
        ]
        attn_term = jnp.concatenate(
            [unpadded(term_in, heads), *own_rows, unpadded(term_out, heads)]
        )
    else:
        attn_term = jnp.concatenate([unpadded(term_in, heads + 2), unpadded(term_out, heads)])
    attn_sum = lax.psum_scatter(attn_term, "fsdp", scatter_dimension=0, tiled=True)
    in_part = plain_times(grads, padded[: (heads + 2) * LANES]).astype(BF)
    grad_input, block_out, gain_sums = last_step(
        in_part, out_part, x_own, middle, grad_middle, norm_gains[0:1], sums, columns, layers
    )

    ffn_shard = ffn_plan.collect(ffn_sum).astype(F32)
    attn_shard = attn_plan.collect(attn_sum).astype(F32)
    column_count = width // (layers * columns)
    first_column = lax.axis_index(EVERY) * column_count
    gain_shard = lax.dynamic_slice_in_dim(gain_sums[:2], first_column, column_count, 1) * grad_factor
    own_gains = lax.dynamic_slice_in_dim(norm_gains, first_column, column_count, 1)
    new_ffn, ffn_states = adamw_update(ffn_weights, ffn_shard, ffn_moments, WEIGHT_DECAY)
    new_attn, attn_states = adamw_update(attn_weights, attn_shard, attn_moments, WEIGHT_DECAY)
    new_gains, gain_states = adamw_update(own_gains, gain_shard, gain_moments, 0.0)
    return (
        block_out[None],
        grad_input[None],
        attn_shard,
        ffn_shard,
        gain_shard,
        new_attn,
        new_ffn,
        new_gains,
        attn_states,
        ffn_states,
        gain_states,
    )


def solution(mesh):
    placed = (
        P("fsdp", "context", None),
        P("fsdp", "context", None),
        P("fsdp", "context"),
        P(EVERY, None),
        P(EVERY, None),
        P(),
        P(None, EVERY, None),
        P(None, EVERY, None),
        P(None, None, EVERY),
    )
    return jax.shard_map(
        on_device,
        mesh=mesh,
        in_specs=placed,
        out_specs=(
            P("fsdp", "context", None),
            P("fsdp", "context", None),
            P(EVERY, None),
            P(EVERY, None),
            P(None, EVERY),
            P(EVERY, None),
            P(EVERY, None),
            P(None, EVERY),
            P(None, EVERY, None),
            P(None, EVERY, None),
            P(None, None, EVERY),
        ),
        check_vma=False,
    )
```

```python
import functools

import jax
import jax.numpy as jnp
import numpy as np
from jax import lax
from jax.experimental import pallas as pl
from jax.experimental.pallas import tpu as pltpu
from jax.sharding import PartitionSpec as P

QUERY_HEADS = 16
KEY_VALUE_HEADS = 8
HEAD_SIZE = 96
STEP = 3

NORM_EPS = 1e-05
ROPE_THETA = 100000.0
BETA_ONE = 0.9
BETA_TWO = 0.95
ADAM_EPS = 1e-08
LEARN_RATE = 0.02
WEIGHT_DECAY = 0.1

LANES = 128
TILE = 256
CHUNK = 16
VMEM_LIMIT = 62 * 1024 * 1024
EVERY = ("fsdp", "context")
BF = jnp.bfloat16
F32 = jnp.float32
ID_TYPE = pl.DeviceIdType.MESH


def product_transposed(left_matrix, right_matrix):
    return lax.dot_general(
        left_matrix, right_matrix, (((1,), (1,)), ((), ())), preferred_element_type=F32
    )


def transposed_times(left_matrix, right_matrix):
    return lax.dot_general(
        left_matrix, right_matrix, (((0,), (0,)), ((), ())), preferred_element_type=F32
    )


def plain_times(left_matrix, right_matrix):
    return jnp.dot(left_matrix, right_matrix, preferred_element_type=F32)


def rms_scale(tensor_in):
    return lax.rsqrt(jnp.mean(tensor_in * tensor_in, axis=-1, keepdims=True) + NORM_EPS)


def norm_backward(grad_in, normed, norm_scale, gain_row):
    scaled = grad_in * (1.0 + gain_row)
    return norm_scale * (scaled - normed * jnp.mean(scaled * normed, axis=-1, keepdims=True))


def adamw_update(parameter, gradient, moments, decay_rate):
    first_moment = BETA_ONE * moments[0] + (1.0 - BETA_ONE) * gradient
    second_moment = BETA_TWO * moments[1] + (1.0 - BETA_TWO) * gradient * gradient
    first_hat = first_moment / (1.0 - BETA_ONE**STEP)
    second_hat = second_moment / (1.0 - BETA_TWO**STEP)
    updated = parameter - LEARN_RATE * (
        first_hat / (jnp.sqrt(second_hat) + ADAM_EPS) + decay_rate * parameter
    )
    return (updated, jnp.stack([first_moment, second_moment]))


class UnitPlan:
    def __init__(self, homes, devices):
        waiting = [[] for _ in range(devices)]
        for unit, (device, place) in enumerate(homes):
            waiting[unit // 3].append((unit % 3, device, place))
        self.rounds = []
        for _ in range(3):
            taken = [None] * devices

            def settle(source, seen):
                for piece, device, place in waiting[source]:
                    if device in seen:
                        continue
                    seen.add(device)
                    if taken[device] is None or settle(taken[device][0], seen):
                        taken[device] = (source, piece, place)
                        return True
                return False

            for source in range(devices):
                if not settle(source, set()):
                    raise ValueError("no matching")
            pairs, pieces, places = [], [0] * devices, [0] * devices
            for device, (source, piece, place) in enumerate(taken):
                pairs.append((source, device))
                pieces[source] = piece
                places[device] = place
                waiting[source].remove((piece, device, place))
            self.rounds.append((pairs, np.array(pieces), np.array(places)))

    def _reorder(self, got, columns):
        order = np.argsort(np.stack(columns, axis=1), axis=1).astype(np.int32)
        mine = jnp.asarray(order)[lax.axis_index(EVERY)]
        stacked = jnp.stack(got)
        return jnp.concatenate(
            [lax.dynamic_index_in_dim(stacked, mine[k], 0, keepdims=False) for k in range(3)]
        )

    def spread(self, rows):
        pieces = rows.reshape(3, rows.shape[0] // 3, rows.shape[1])
        me = lax.axis_index(EVERY)
        got = []
        for pairs, piece, _ in self.rounds:
            unit = lax.dynamic_index_in_dim(
                pieces, jnp.asarray(piece, jnp.int32)[me], 0, keepdims=False
            )
            got.append(lax.ppermute(unit, EVERY, pairs))
        return self._reorder(got, [place for _, _, place in self.rounds])

    def collect(self, rows):
        places_of = rows.reshape(3, rows.shape[0] // 3, rows.shape[1])
        me = lax.axis_index(EVERY)
        got = []
        for pairs, _, place in self.rounds:
            unit = lax.dynamic_index_in_dim(
                places_of, jnp.asarray(place, jnp.int32)[me], 0, keepdims=False
            )
            got.append(lax.ppermute(unit, EVERY, [(b, a) for a, b in pairs]))
        return self._reorder(got, [piece for _, piece, _ in self.rounds])


def unit_plans(layers, columns, attn_rows):
    devices = layers * columns

    def home(column, position):
        return ((position // 3) * columns + column, position % 3)

    homes = []
    for unit in range(3 * devices):
        matrix, rest = divmod(unit, devices)
        stretch, column = divmod(rest, columns)
        homes.append(home(column, matrix * layers + stretch))
    ffn_plan = UnitPlan(homes, devices)
    unit_rows = attn_rows // (3 * devices)
    query_units = QUERY_HEADS * HEAD_SIZE // columns // unit_rows
    share_units = KEY_VALUE_HEADS * HEAD_SIZE // columns // unit_rows
    homes = []
    position = 0
    for count in (query_units, share_units, share_units, query_units):
        for column in range(columns):
            for k in range(count):
                homes.append(home(column, position + k))
        position += count
    return UnitPlan(homes, devices), ffn_plan


class Homes:
    def __init__(self, layers, columns, attn_rows):
        devices = layers * columns
        unit_rows = attn_rows // (3 * devices)
        self.layers, self.columns = layers, columns
        self.counts = [
            QUERY_HEADS * HEAD_SIZE // columns // unit_rows,
            KEY_VALUE_HEADS * HEAD_SIZE // columns // unit_rows,
        ]
        query, share = self.counts
        self.first = [0, query, query + share, query + 2 * share]
        self.sizes = [query, share, share, query]

    def _spot(self, column, position):
        return position // 3, column, position % 3

    def attn_targets(self):
        device = lax.axis_index("fsdp") * self.columns + lax.axis_index("context")
        found = []
        for piece in range(3):
            unit = device * 3 + piece
            column, position = 0, 0
            for first, size in zip(self.first, self.sizes):
                inside = unit - first * self.columns
                begun = inside >= 0
                column = jnp.where(begun, inside // size, column)
                position = jnp.where(begun, first + inside % size, position)
            found.append(self._spot(column, position))
        return found

    def attn_owners(self):
        column = lax.axis_index("context")
        found = []
        for place in range(3):
            position = lax.axis_index("fsdp") * 3 + place
            unit = 0
            for first, size in zip(self.first, self.sizes):
                inside = position - first
                unit = jnp.where(inside >= 0, first * self.columns + column * size + inside, unit)
            device = unit // 3
            found.append((device // self.columns, device % self.columns, unit % 3))
        return found

    def ffn_targets(self):
        layer, column = lax.axis_index("fsdp"), lax.axis_index("context")
        return [
            (layer, (3 * column + piece) % self.columns, (3 * column + piece) // self.columns)
            for piece in range(3)
        ]

    def ffn_owners(self):
        layer, column = lax.axis_index("fsdp"), lax.axis_index("context")
        return [
            (layer, (place * self.columns + column) // 3, (place * self.columns + column) % 3)
            for place in range(3)
        ]


def partner(me, step, chips):
    return lax.rem(me // 2 + step, chips) * 2 + lax.rem(me, 2)


def sibling_of(me):
    return me + 1 - 2 * lax.rem(me, 2)


def rows_at(index, rows):
    return pl.ds(pl.multiple_of(index * rows, rows), rows)


def greet(columns, layers=1, others=()):
    barrier = pltpu.get_barrier_semaphore()
    me = lax.axis_index("context")
    awaited = columns - 1 + layers - 1
    for layer, column in others:
        apart = (layer != lax.axis_index("fsdp")) | (column != me)
        awaited = awaited + jnp.where(apart, 1, 0)

        @pl.when(apart)
        def there():
            pl.semaphore_signal(
                barrier, inc=1, device_id={"fsdp": layer, "context": column}, device_id_type=ID_TYPE
            )

    for step in range(1, columns):
        pl.semaphore_signal(
            barrier, inc=1, device_id={"context": lax.rem(me + step, columns)}, device_id_type=ID_TYPE
        )
    if layers > 1:
        layer = lax.axis_index("fsdp")
        for step in range(1, layers):
            pl.semaphore_signal(
                barrier, inc=1, device_id={"fsdp": lax.rem(layer + step, layers)}, device_id_type=ID_TYPE
            )
    pl.semaphore_wait(barrier, awaited)


def send(source, target, send_sem, recv_sem, device):
    copy = pltpu.make_async_remote_copy(
        src_ref=source,
        dst_ref=target,
        send_sem=send_sem,
        recv_sem=recv_sem,
        device_id=device,
        device_id_type=ID_TYPE,
    )
    copy.start()
    return copy


def remote(source, target, send_sem, recv_sem, device):
    return pltpu.make_async_remote_copy(
        src_ref=source,
        dst_ref=target,
        send_sem=send_sem,
        recv_sem=recv_sem,
        device_id=device,
        device_id_type=ID_TYPE,
    )


class Exchange:
    @staticmethod
    def scratch():
        return [pltpu.SemaphoreType.DMA((3,)), pltpu.SemaphoreType.DMA((3,))]

    def __init__(self, sources, targets, homes, sems):
        send_sem, recv_sem = sems
        self.parts = []
        for i, (layer, column, place) in enumerate(homes):
            itself = (layer == lax.axis_index("fsdp")) & (column == lax.axis_index("context"))
            target = targets(layer, place)
            copy = functools.partial(
                remote,
                sources[i],
                target,
                send_sem.at[i],
                recv_sem.at[place],
                {"fsdp": layer, "context": column},
            )
            stay = functools.partial(pltpu.make_async_copy, sources[i], target, recv_sem.at[place])

            @pl.when(itself)
            def here():
                stay().start()

            @pl.when(jnp.logical_not(itself))
            def there():
                copy().start()

            self.parts.append((itself, copy))
        self.landing = [
            functools.partial(pltpu.make_async_copy, sources[k], sources[k], recv_sem.at[k])
            for k in range(3)
        ]

    def arrive(self):
        for landed in self.landing:
            landed().wait()

    def drain(self):
        for itself, copy in self.parts:

            @pl.when(jnp.logical_not(itself))
            def sent():
                copy().wait_send()


class LineGather:
    @staticmethod
    def scratch(layers):
        return [pltpu.SemaphoreType.DMA((layers - 1,))] * 4

    def __init__(self, full, rows, layers, sems, own):
        self.full, self.rows, self.layers, self.sems, self.own = full, rows, layers, sems, own

    def _moves(self, k):
        layer = lax.axis_index("fsdp")
        up_send, up_recv, down_send, down_recv = self.sems
        top = self.layers - 1
        for first, last, other, shard, send_sem, recv_sem in (
            (layer - k >= 0, layer < top, layer + 1, layer - k, up_send, up_recv),
            (layer + k <= top, layer > 0, layer - 1, layer + k, down_send, down_recv),
        ):
            block = self.full.at[rows_at(shard, self.rows), :]
            yield first & last, functools.partial(
                remote, self.own if k == 0 else block, block, send_sem.at[k], recv_sem.at[k], {"fsdp": other}
            )

    def _landed(self, k):
        layer = lax.axis_index("fsdp")
        _, up_recv, _, down_recv = self.sems
        for there, shard, recv_sem in (
            (layer - 1 - k >= 0, layer - 1 - k, up_recv),
            (layer + 1 + k <= self.layers - 1, layer + 1 + k, down_recv),
        ):
            block = self.full.at[rows_at(shard, self.rows), :]
            yield there, functools.partial(pltpu.make_async_copy, block, block, recv_sem.at[k])

    def step(self, k):
        if k > 0:
            for there, copy in self._landed(k - 1):

                @pl.when(there)
                def landed():
                    copy().wait()

        if k < self.layers - 1:
            for go, copy in self._moves(k):

                @pl.when(go)
                def start():
                    copy().start()

    def drain(self):
        for k in range(self.layers - 1):
            for go, copy in self._moves(k):

                @pl.when(go)
                def sent():
                    copy().wait_send()


class LineReduce:
    @staticmethod
    def scratch(layers, rows, width):
        return [
            pltpu.VMEM((layers - 1, rows, width), BF),
            pltpu.VMEM((layers - 1, rows, width), BF),
            *[pltpu.SemaphoreType.DMA((layers - 1,))] * 4,
        ]

    def __init__(self, term, rows, layers, scratch):
        self.term, self.rows, self.layers = term, rows, layers
        self.up_in, self.down_in, *self.sems = scratch
        layer = lax.axis_index("fsdp")
        top = layers - 1
        up_send, up_recv, down_send, down_recv = self.sems

        @pl.when(layer == 0)
        def bottom():
            for k in range(top):
                self._up(k, self.term.at[pl.ds((top - k) * rows, rows), :]).start()

        @pl.when(layer == top)
        def ceiling():
            for k in range(top):
                self._down(k, self.term.at[pl.ds(k * rows, rows), :]).start()

    def _up(self, k, source):
        up_send, up_recv, _, _ = self.sems
        other = {"fsdp": lax.axis_index("fsdp") + 1}
        return remote(source, self.up_in.at[k], up_send.at[k], up_recv.at[k], other)

    def _down(self, k, source):
        _, _, down_send, down_recv = self.sems
        other = {"fsdp": lax.axis_index("fsdp") - 1}
        return remote(source, self.down_in.at[k], down_send.at[k], down_recv.at[k], other)

    def _add(self, sums, k, target):
        @pl.loop(0, self.rows // CHUNK)
        def add(c):
            at = chunk_rows(c)
            of_term = pl.ds(target * self.rows + pl.multiple_of(c * CHUNK, CHUNK), CHUNK)
            sums[k, at, :] = (
                sums[k, at, :].astype(F32) + self.term[of_term, :].astype(F32)
            ).astype(BF)

    def step(self, k):
        layer = lax.axis_index("fsdp")
        top = self.layers - 1
        _, up_recv, _, down_recv = self.sems
        target = top - k

        @pl.when((layer > 0) & (layer <= target))
        def from_below():
            pltpu.make_async_copy(self.up_in.at[k], self.up_in.at[k], up_recv.at[k]).wait()

        @pl.when((layer > 0) & (layer < target))
        def pass_up():
            self._add(self.up_in, k, target)
            self._up(k, self.up_in.at[k]).start()

        @pl.when((layer < top) & (layer >= k))
        def from_above():
            pltpu.make_async_copy(self.down_in.at[k], self.down_in.at[k], down_recv.at[k]).wait()

        @pl.when((layer < top) & (layer > k))
        def pass_down():
            self._add(self.down_in, k, k)
            self._down(k, self.down_in.at[k]).start()

    def finish(self, total):
        layer = lax.axis_index("fsdp")
        top = self.layers - 1
        for own in range(self.layers):

            @pl.when(layer == own)
            def here():
                @pl.loop(0, self.rows // CHUNK)
                def add(c):
                    at = chunk_rows(c)
                    of_term = pl.ds(own * self.rows + pl.multiple_of(c * CHUNK, CHUNK), CHUNK)
                    value = self.term[of_term, :].astype(F32)
                    if own > 0:
                        value = value + self.up_in[top - own, at, :].astype(F32)
                    if own < top:
                        value = value + self.down_in[own, at, :].astype(F32)
                    total[at, :] = value.astype(BF)

    def drain(self):
        layer = lax.axis_index("fsdp")
        top = self.layers - 1
        for k in range(top):

            @pl.when(layer < top - k)
            def up():
                self._up(k, self.up_in.at[k]).wait_send()

            @pl.when(layer > k)
            def down():
                self._down(k, self.down_in.at[k]).wait_send()


class Gather:
    @staticmethod
    def scratch(chips):
        return [
            pltpu.SemaphoreType.DMA((chips,)),
            pltpu.SemaphoreType.DMA((chips,)),
            pltpu.SemaphoreType.DMA((chips,)),
            pltpu.SemaphoreType.DMA((chips,)),
            pltpu.SemaphoreType.DMA,
        ]

    def __init__(self, block, full, chips, sems):
        own_send, own_recv, self.on_send, self.on_recv, local_sem = sems
        me = lax.axis_index("context")
        rows = block.shape[0]
        self.block, self.full, self.chips, self.me, self.rows = block, full, chips, me, rows
        mine = full.at[rows_at(me, rows), :]
        self.own = [
            send(block, mine, own_send.at[step], own_recv.at[step], {"context": partner(me, step, chips)})
            for step in range(1, chips)
        ]
        self.own.append(
            send(block, mine, own_send.at[0], own_recv.at[0], {"context": sibling_of(me)})
        )
        self.local = pltpu.make_async_copy(block, mine, local_sem)
        self.local.start()

    def finish(self):
        passed = []
        for step in range(1, self.chips):
            self.own[step - 1].wait_recv()
            source = partner(self.me, self.chips - step, self.chips)
            there = self.full.at[rows_at(source, self.rows), :]
            passed.append(
                send(there, there, self.on_send.at[step], self.on_recv.at[step], {"context": sibling_of(self.me)})
            )
        self.own[-1].wait_recv()
        for copy in passed:
            copy.wait_recv()
        for copy in self.own + passed:
            copy.wait_send()
        self.local.wait()


class Reduce:
    @staticmethod
    def scratch(chips, rows, width):
        return [
            pltpu.VMEM((chips, rows, width), BF),
            pltpu.VMEM((chips, rows, width), BF),
            pltpu.VMEM((chips, rows, width), BF),
            pltpu.SemaphoreType.DMA((chips,)),
            pltpu.SemaphoreType.DMA((chips,)),
            pltpu.SemaphoreType.DMA((chips,)),
            pltpu.SemaphoreType.DMA((chips,)),
        ]

    def __init__(self, part, chips, rows, scratch):
        self.near, self.summed, self.far, near_send, near_recv, self.far_send, self.far_recv = scratch
        me = lax.axis_index("context")
        self.part, self.chips, self.rows, self.me = part, chips, rows, me
        self.near_copies = {}
        for step in [*range(1, chips), 0]:
            block = partner(sibling_of(me), step, chips)
            self.near_copies[step] = send(
                part.at[rows_at(block, rows), :],
                self.near.at[step],
                near_send.at[step],
                near_recv.at[step],
                {"context": sibling_of(me)},
            )
        self.far_copies = []

    def exchange(self):
        for step in range(1, self.chips):
            self.near_copies[step].wait_recv()
            target = partner(self.me, step, self.chips)
            first = pl.multiple_of(target * self.rows, self.rows)

            @pl.loop(0, self.rows // CHUNK)
            def add(k):
                at = pl.ds(pl.multiple_of(k * CHUNK, CHUNK), CHUNK)
                from_part = pl.ds(pl.multiple_of(first + k * CHUNK, CHUNK), CHUNK)
                self.summed[step, at, :] = (
                    self.part[from_part, :].astype(F32) + self.near[step, at, :].astype(F32)
                ).astype(BF)

            self.far_copies.append(
                send(
                    self.summed.at[step],
                    self.far.at[step],
                    self.far_send.at[step],
                    self.far_recv.at[step],
                    {"context": target},
                )
            )

    def arrive(self):
        self.near_copies[0].wait_recv()
        for copy in self.far_copies:
            copy.wait_recv()

    def total(self, k):
        at = pl.ds(pl.multiple_of(k * CHUNK, CHUNK), CHUNK)
        first = pl.multiple_of(self.me * self.rows, self.rows)
        value = self.part[pl.ds(pl.multiple_of(first + k * CHUNK, CHUNK), CHUNK), :].astype(F32)
        value = value + self.near[0, at, :].astype(F32)
        for step in range(1, self.chips):
            value = value + self.far[step, at, :].astype(F32)
        return value

    def drain(self):
        for copy in list(self.near_copies.values()) + self.far_copies:
            copy.wait_send()


def chunk_rows(k):
    return pl.ds(pl.multiple_of(k * CHUNK, CHUNK), CHUNK)


def vmem_specs(count):
    return [pl.BlockSpec(memory_space=pltpu.VMEM)] * count


def comm_params(collective_id):
    return pltpu.CompilerParams(
        collective_id=collective_id, has_side_effects=True, vmem_limit_bytes=VMEM_LIMIT
    )


def spread_kernel(
    columns,
    layers,
    homes,
    docs,
    attn_ref,
    ffn_ref,
    docs_full,
    attn_shard,
    ffn_shard,
    attn_bf,
    ffn_bf,
    docs_send,
    docs_recv,
    docs_local,
    *scratch,
):
    attn_rows, ffn_rows = attn_ref.shape[0], ffn_ref.shape[0]
    me = lax.axis_index("context")

    @pl.loop(0, attn_rows // CHUNK)
    def cast_attn(k):
        attn_bf[chunk_rows(k), :] = attn_ref[chunk_rows(k), :].astype(BF)

    @pl.loop(0, ffn_rows // CHUNK)
    def cast_ffn(k):
        ffn_bf[chunk_rows(k), :] = ffn_ref[chunk_rows(k), :].astype(BF)

    greet(columns, 1, [spot[:2] for spot in homes.attn_targets() + homes.attn_owners()])
    exchanges = []
    for rows, source, target, targets, sems in (
        (attn_rows, attn_bf, attn_shard, homes.attn_targets(), scratch[0:2]),
        (ffn_rows, ffn_bf, ffn_shard, homes.ffn_targets(), scratch[2:4]),
    ):
        unit = rows // 3
        exchanges.append(
            Exchange(
                [source.at[pl.ds(k * unit, unit), :] for k in range(3)],
                functools.partial(place_rows, target, unit),
                targets,
                sems,
            )
        )
    mine = docs_full.at[pl.ds(me, 1), :]
    copies = [
        send(docs, mine, docs_send.at[step], docs_recv.at[step], {"context": lax.rem(me + step, columns)})
        for step in range(1, columns)
    ]
    local = pltpu.make_async_copy(docs, mine, docs_local)
    local.start()
    for exchange in exchanges:
        exchange.arrive()
    for copy in copies:
        copy.wait_recv()
    for copy in copies:
        copy.wait_send()
    local.wait()
    for exchange in exchanges:
        exchange.drain()


def place_rows(ref, unit, layer, place):
    return ref.at[rows_at(place, unit), :]


def spread_step(docs, attn_weights, ffn_weights, columns, layers):
    attn_rows, width = attn_weights.shape
    ffn_rows = ffn_weights.shape[0]
    homes = Homes(layers, columns, attn_rows * layers * columns)
    return pl.pallas_call(
        functools.partial(spread_kernel, columns, layers, homes),
        out_shape=(
            jax.ShapeDtypeStruct((columns, docs.shape[1]), jnp.int32),
            jax.ShapeDtypeStruct((attn_rows, width), BF),
            jax.ShapeDtypeStruct((ffn_rows, width), BF),
        ),
        in_specs=vmem_specs(3),
        out_specs=tuple([pl.BlockSpec(memory_space=pl.ANY)] * 3),
        scratch_shapes=[
            pltpu.VMEM((attn_rows, width), BF),
            pltpu.VMEM((ffn_rows, width), BF),
            pltpu.SemaphoreType.DMA((columns,)),
            pltpu.SemaphoreType.DMA((columns,)),
            pltpu.SemaphoreType.DMA,
            *Exchange.scratch(),
            *Exchange.scratch(),
        ],
        compiler_params=comm_params(1),
        name="spread_step",
        cost_estimate=pl.CostEstimate(flops=0, bytes_accessed=60_000_000, transcendentals=0),
    )(docs, attn_weights, ffn_weights)


def open_kernel(
    columns, layers, x_ref, gain_ref, dy_ref, shard_ref, h_full, dy_full, attn_col, hidden, shard_local, *scratch
):
    chips = columns // 2
    attn_rows = shard_ref.shape[0]
    layer = lax.axis_index("fsdp")
    greet(columns, layers)
    line = LineGather(attn_col, attn_rows, layers, scratch[0:4], shard_ref)
    line.step(0)
    own = pltpu.make_async_copy(shard_ref, attn_col.at[rows_at(layer, attn_rows), :], shard_local)
    own.start()

    @pl.loop(0, x_ref.shape[0] // CHUNK)
    def norm(k):
        residual = x_ref[chunk_rows(k), :].astype(F32)
        hidden[chunk_rows(k), :] = (residual * rms_scale(residual) * (1.0 + gain_ref[...])).astype(BF)

    first = Gather(hidden, h_full, chips, scratch[4:9])
    second = Gather(dy_ref, dy_full, chips, scratch[9:14])
    line.step(1)
    first.finish()
    for k in range(2, layers - 1):
        line.step(k)
    second.finish()
    line.step(layers - 1)
    line.drain()
    own.wait()


def open_step(x_own, gain_row, dy_own, attn_shard, columns, layers):
    rows, width = x_own.shape
    attn_rows = attn_shard.shape[0]
    return pl.pallas_call(
        functools.partial(open_kernel, columns, layers),
        out_shape=(
            jax.ShapeDtypeStruct((columns * rows, width), BF),
            jax.ShapeDtypeStruct((columns * rows, width), BF),
            jax.ShapeDtypeStruct((layers * attn_rows, width), BF),
        ),
        in_specs=vmem_specs(4),
        out_specs=tuple([pl.BlockSpec(memory_space=pl.ANY)] * 3),
        scratch_shapes=[
            pltpu.VMEM((rows, width), BF),
            pltpu.SemaphoreType.DMA,
            *LineGather.scratch(layers),
            *Gather.scratch(columns // 2),
            *Gather.scratch(columns // 2),
        ],
        compiler_params=comm_params(2),
        name="open_step",
        cost_estimate=pl.CostEstimate(flops=0, bytes_accessed=150_000_000, transcendentals=0),
    )(x_own, gain_row, dy_own, attn_shard)


def gather_docs_kernel(columns, block, docs, full, docs_full, *scratch):
    docs_send, docs_recv, docs_local = scratch[-3:]
    greet(columns)
    gather = Gather(block, full, columns // 2, scratch[:-3])
    me = lax.axis_index("context")
    mine = docs_full.at[pl.ds(me, 1), :]
    copies = [
        send(docs, mine, docs_send.at[step], docs_recv.at[step], {"context": lax.rem(me + step, columns)})
        for step in range(1, columns)
    ]
    local = pltpu.make_async_copy(docs, mine, docs_local)
    local.start()
    gather.finish()
    for copy in copies:
        copy.wait_recv()
    for copy in copies:
        copy.wait_send()
    local.wait()


def gather_docs(block, docs, columns):
    rows, width = block.shape
    return pl.pallas_call(
        functools.partial(gather_docs_kernel, columns),
        out_shape=(
            jax.ShapeDtypeStruct((columns * rows, width), BF),
            jax.ShapeDtypeStruct((columns, docs.shape[1]), jnp.int32),
        ),
        in_specs=vmem_specs(2),
        out_specs=(pl.BlockSpec(memory_space=pl.ANY), pl.BlockSpec(memory_space=pl.ANY)),
        scratch_shapes=[
            *Gather.scratch(columns // 2),
            pltpu.SemaphoreType.DMA((columns,)),
            pltpu.SemaphoreType.DMA((columns,)),
            pltpu.SemaphoreType.DMA,
        ],
        compiler_params=comm_params(6),
        name="gather_docs",
        cost_estimate=pl.CostEstimate(flops=0, bytes_accessed=60_000_000, transcendentals=0),
    )(block, docs)


def gather_plain_kernel(columns, block, full, *scratch):
    greet(columns)
    gather = Gather(block, full, columns // 2, scratch)
    gather.finish()


def gather_plain(block, columns):
    rows, width = block.shape
    return pl.pallas_call(
        functools.partial(gather_plain_kernel, columns),
        out_shape=jax.ShapeDtypeStruct((columns * rows, width), BF),
        in_specs=vmem_specs(1),
        out_specs=pl.BlockSpec(memory_space=pl.ANY),
        scratch_shapes=Gather.scratch(columns // 2),
        compiler_params=comm_params(7),
        name="gather_plain",
        cost_estimate=pl.CostEstimate(flops=0, bytes_accessed=60_000_000, transcendentals=0),
    )(block)


def middle_kernel(columns, part, x_ref, gain_ref, middle_ref, full, hidden, *scratch):
    chips = columns // 2
    rows = x_ref.shape[0]
    greet(columns)
    reduce = Reduce(part, chips, rows, scratch[:7])
    reduce.exchange()
    reduce.arrive()

    @pl.loop(0, rows // CHUNK)
    def finish(k):
        at = chunk_rows(k)
        middle = x_ref[at, :].astype(F32) + reduce.total(k)
        middle_ref[at, :] = middle
        hidden[at, :] = (middle * rms_scale(middle) * (1.0 + gain_ref[...])).astype(BF)

    gather = Gather(hidden, full, chips, scratch[7:])
    gather.finish()
    reduce.drain()


def middle_step(part, x_own, gain_row, columns):
    rows, width = x_own.shape
    chips = columns // 2
    return pl.pallas_call(
        functools.partial(middle_kernel, columns),
        out_shape=(
            jax.ShapeDtypeStruct((rows, width), F32),
            jax.ShapeDtypeStruct((columns * rows, width), BF),
        ),
        in_specs=vmem_specs(3),
        out_specs=(pl.BlockSpec(memory_space=pltpu.VMEM), pl.BlockSpec(memory_space=pl.ANY)),
        scratch_shapes=[
            pltpu.VMEM((rows, width), BF),
            *Reduce.scratch(chips, rows, width),
            *Gather.scratch(chips),
        ],
        compiler_params=comm_params(3),
        name="middle_step",
        cost_estimate=pl.CostEstimate(flops=0, bytes_accessed=150_000_000, transcendentals=0),
    )(part, x_own, gain_row)


def turn_kernel(columns, part, middle_ref, dy_ref, gain_ref, grad_ref, sums_ref, full, grad_bf, *scratch):
    chips = columns // 2
    rows = middle_ref.shape[0]
    greet(columns)
    reduce = Reduce(part, chips, rows, scratch[:7])
    sums_ref[...] = jnp.zeros_like(sums_ref)
    reduce.exchange()
    reduce.arrive()

    @pl.loop(0, rows // CHUNK)
    def finish(k):
        at = chunk_rows(k)
        grad_hidden = reduce.total(k)
        middle = middle_ref[at, :]
        scale = rms_scale(middle)
        normed = middle * scale
        sums_ref[0:1, :] += jnp.sum(grad_hidden * normed, axis=0, keepdims=True)
        grad = dy_ref[at, :].astype(F32) + norm_backward(grad_hidden, normed, scale, gain_ref[...])
        grad_ref[at, :] = grad
        grad_bf[at, :] = grad.astype(BF)

    gather = Gather(grad_bf, full, chips, scratch[7:])
    gather.finish()
    reduce.drain()


def turn_step(part, middle, dy_own, gain_row, columns):
    rows, width = middle.shape
    chips = columns // 2
    return pl.pallas_call(
        functools.partial(turn_kernel, columns),
        out_shape=(
            jax.ShapeDtypeStruct((rows, width), F32),
            jax.ShapeDtypeStruct((8, width), F32),
            jax.ShapeDtypeStruct((columns * rows, width), BF),
        ),
        in_specs=vmem_specs(4),
        out_specs=(*vmem_specs(2), pl.BlockSpec(memory_space=pl.ANY)),
        scratch_shapes=[
            pltpu.VMEM((rows, width), BF),
            *Reduce.scratch(chips, rows, width),
            *Gather.scratch(chips),
        ],
        compiler_params=comm_params(4),
        name="turn_step",
        cost_estimate=pl.CostEstimate(flops=0, bytes_accessed=150_000_000, transcendentals=0),
    )(part, middle, dy_own, gain_row)


def last_kernel(columns, layers, homes, *refs):
    (part_in, x_ref, grad_ref, gain_ref, sums_ref), refs = refs[:5], refs[5:]
    if homes is not None:
        (term, ffn_sum), refs = refs[:2], refs[2:]
    (input_grad_ref, gains_ref), refs = refs[:2], refs[2:]
    if homes is not None:
        (attn_back, ffn_back), refs = refs[:2], refs[2:]
    (own_sums, plane_slots, plane_sums, line_slots), refs = refs[:4], refs[4:]
    (plane_send, plane_recv, line_send, line_recv), scratch = refs[:4], refs[4:]
    chips = columns // 2
    rows = x_ref.shape[0]
    if homes is None:
        greet(columns, layers)
    else:
        attn_owners = homes.attn_owners()
        greet(columns, layers, [spot[:2] for spot in homes.attn_targets() + attn_owners])
    first = Reduce(part_in, chips, rows, scratch[:7])
    if homes is not None:
        attn_rows, ffn_rows = term.shape[0] // layers, ffn_sum.shape[0]
        attn_done = scratch[7]
        line = LineReduce(term, attn_rows, layers, scratch[8:14])
        unit_ffn = ffn_rows // 3
        ffn_owned = Exchange(
            [ffn_sum.at[pl.ds(k * unit_ffn, unit_ffn), :] for k in range(3)],
            lambda layer, piece: ffn_back.at[rows_at(piece, unit_ffn), :],
            homes.ffn_owners(),
            scratch[14:16],
        )
    first.exchange()
    if homes is not None:
        line.step(0)
    own_sums[...] = jnp.zeros_like(own_sums)
    own_sums[1:2, :] = sums_ref[0:1, :]
    if homes is not None:
        for k in range(1, layers - 1):
            line.step(k)
        line.finish(attn_done)
        unit = attn_rows // 3
        attn_owned = Exchange(
            [attn_done.at[pl.ds(k * unit, unit), :] for k in range(3)],
            lambda layer, piece: attn_back.at[rows_at(piece, unit), :],
            attn_owners,
            scratch[16:18],
        )
    first.arrive()

    @pl.loop(0, rows // CHUNK)
    def finish(k):
        at = chunk_rows(k)
        grad_hidden = first.total(k)
        residual = x_ref[at, :].astype(F32)
        scale = rms_scale(residual)
        normed = residual * scale
        own_sums[0:1, :] += jnp.sum(grad_hidden * normed, axis=0, keepdims=True)
        input_grad_ref[at, :] = grad_ref[at, :] + norm_backward(
            grad_hidden, normed, scale, gain_ref[...]
        )

    me = lax.axis_index("context")
    layer = lax.axis_index("fsdp")
    in_plane = [
        send(
            own_sums,
            plane_slots.at[step],
            plane_send.at[step],
            plane_recv.at[step],
            {"context": lax.rem(me + step, columns)},
        )
        for step in range(1, columns)
    ]
    total = own_sums[...]
    for step, copy in enumerate(in_plane):
        copy.wait_recv()
        total = total + plane_slots[step + 1]
    plane_sums[...] = total
    in_line = [
        send(
            plane_sums,
            line_slots.at[step],
            line_send.at[step],
            line_recv.at[step],
            {"fsdp": lax.rem(layer + step, layers)},
        )
        for step in range(1, layers)
    ]
    for step, copy in enumerate(in_line):
        copy.wait_recv()
        total = total + line_slots[step + 1]
    gains_ref[...] = total
    if homes is not None:
        ffn_owned.arrive()
        attn_owned.arrive()
        ffn_owned.drain()
        attn_owned.drain()
        line.drain()
    for copy in in_plane + in_line:
        copy.wait_send()
    first.drain()


def last_step(part_in, x_own, grad_middle, gain_row, sums, columns, layers, weight_sums=()):
    rows, width = x_own.shape
    chips = columns // 2
    homes = None
    back_shapes, back_scratch = [], []
    if weight_sums:
        term, ffn_sum = weight_sums
        attn_rows = term.shape[0] // layers
        homes = Homes(layers, columns, attn_rows * layers * columns)
        back_shapes = [
            jax.ShapeDtypeStruct((attn_rows, width), BF),
            jax.ShapeDtypeStruct(ffn_sum.shape, BF),
        ]
        back_scratch = [
            pltpu.VMEM((attn_rows, width), BF),
            *LineReduce.scratch(layers, attn_rows, width),
            *Exchange.scratch(),
            *Exchange.scratch(),
        ]
    return pl.pallas_call(
        functools.partial(last_kernel, columns, layers, homes),
        out_shape=(
            jax.ShapeDtypeStruct((rows, width), F32),
            jax.ShapeDtypeStruct((8, width), F32),
            *back_shapes,
        ),
        in_specs=vmem_specs(5 + len(weight_sums)),
        out_specs=tuple(vmem_specs(2) + [pl.BlockSpec(memory_space=pl.ANY)] * len(back_shapes)),
        scratch_shapes=[
            pltpu.VMEM((8, width), F32),
            pltpu.VMEM((columns, 8, width), F32),
            pltpu.VMEM((8, width), F32),
            pltpu.VMEM((layers, 8, width), F32),
            pltpu.SemaphoreType.DMA((columns,)),
            pltpu.SemaphoreType.DMA((columns,)),
            pltpu.SemaphoreType.DMA((layers,)),
            pltpu.SemaphoreType.DMA((layers,)),
            *Reduce.scratch(chips, rows, width),
            *back_scratch,
        ],
        compiler_params=comm_params(5),
        name="last_step",
        cost_estimate=pl.CostEstimate(flops=0, bytes_accessed=150_000_000, transcendentals=0),
    )(part_in, x_own, grad_middle, gain_row, sums, *weight_sums)


def turned(heads, low):
    return jnp.where(low, pltpu.roll(heads, LANES - HEAD_SIZE // 2, 1), pltpu.roll(heads, HEAD_SIZE // 2, 1))


def allowed_tile(start_ref, row_first, col_first):
    rows = row_first + lax.broadcasted_iota(jnp.int32, (TILE, TILE), 0)
    cols = col_first + lax.broadcasted_iota(jnp.int32, (TILE, TILE), 1)
    starts = jnp.broadcast_to(start_ref[row_first : row_first + TILE, 0:1], (TILE, TILE))
    return (cols <= rows) & (cols >= starts)


def attend_kernel(
    heads, h_ref, w_ref, cos_ref, sin_ref, start_ref, q_ref, k_ref, v_ref, att_ref, log_ref, part_ref, pad_ref
):
    seq = h_ref.shape[0]
    scale = HEAD_SIZE**-0.5
    for slot in range(2 * heads + 2):
        pad_ref[slot * LANES : slot * LANES + HEAD_SIZE, :] = w_ref[
            slot * HEAD_SIZE : (slot + 1) * HEAD_SIZE, :
        ]
        pad_ref[slot * LANES + HEAD_SIZE : (slot + 1) * LANES, :] = jnp.zeros(
            (LANES - HEAD_SIZE, w_ref.shape[1]), BF
        )
    width = (heads + 2) * LANES

    @pl.loop(0, seq // TILE)
    def project(i):
        at = pl.ds(pl.multiple_of(i * TILE, TILE), TILE)
        low = lax.broadcasted_iota(jnp.int32, (TILE, LANES), 1) < HEAD_SIZE // 2
        projected = product_transposed(h_ref[at, :], pad_ref[0:width, :])
        cosine, sine = cos_ref[at, :], sin_ref[at, :]
        for head in range(heads + 1):
            u = projected[:, head * LANES : (head + 1) * LANES]
            r = (u * cosine + turned(u, low) * sine).astype(BF)
            if head < heads:
                q_ref[at, head * LANES : (head + 1) * LANES] = r
            else:
                k_ref[at, :] = r
        v_ref[at, :] = projected[:, (heads + 1) * LANES :].astype(BF)

    for i in range(seq // TILE):
        rows = slice(i * TILE, (i + 1) * TILE)
        for head in range(heads):
            lanes = slice(head * LANES, (head + 1) * LANES)
            q = q_ref[rows, lanes]
            out = jnp.zeros((TILE, LANES), F32)
            total = jnp.zeros((TILE, 1), F32)
            for j in range(i + 1):
                keys = slice(j * TILE, (j + 1) * TILE)
                s = product_transposed(q, k_ref[keys, :]) * scale
                e = jnp.where(allowed_tile(start_ref, i * TILE, j * TILE), jnp.exp(s), 0.0)
                total = total + jnp.sum(e, axis=1, keepdims=True)
                out = out + plain_times(e.astype(BF), v_ref[keys, :])
            att_ref[rows, lanes] = (out / total).astype(BF)
            log_ref[rows, lanes] = jnp.broadcast_to(jnp.log(total), (TILE, LANES))

    @pl.loop(0, seq // TILE)
    def project_out(i):
        at = pl.ds(pl.multiple_of(i * TILE, TILE), TILE)
        part_ref[at, :] = plain_times(att_ref[at, :], pad_ref[width:, :]).astype(BF)


def attend(h_full, w_col, cosine, sine, starts, heads):
    seq, width = h_full.shape
    return pl.pallas_call(
        functools.partial(attend_kernel, heads),
        out_shape=(
            jax.ShapeDtypeStruct((seq, heads * LANES), BF),
            jax.ShapeDtypeStruct((seq, LANES), BF),
            jax.ShapeDtypeStruct((seq, LANES), BF),
            jax.ShapeDtypeStruct((seq, heads * LANES), BF),
            jax.ShapeDtypeStruct((seq, heads * LANES), F32),
            jax.ShapeDtypeStruct((seq, width), BF),
            jax.ShapeDtypeStruct(((2 * heads + 2) * LANES, width), BF),
        ),
        in_specs=vmem_specs(5),
        out_specs=tuple(vmem_specs(7)),
        compiler_params=pltpu.CompilerParams(vmem_limit_bytes=VMEM_LIMIT),
        name="attend",
        cost_estimate=pl.CostEstimate(flops=6_000_000_000, bytes_accessed=20_000_000, transcendentals=2_000_000),
    )(h_full, w_col, cosine, sine, starts)


def attend_back_kernel(
    columns,
    heads,
    part_ref,
    middle_ref,
    grad_ref,
    pad_ref,
    cos_ref,
    sin_ref,
    start_ref,
    q_ref,
    k_ref,
    v_ref,
    att_ref,
    log_ref,
    out_ref,
    block_out_ref,
    ga_ref,
    dk_ref,
    dv_ref,
    *scratch,
):
    seq = grad_ref.shape[0]
    own_rows = middle_ref.shape[0]
    greet(columns)
    reduce = Reduce(part_ref, columns // 2, own_rows, scratch)
    scale = HEAD_SIZE**-0.5
    width = (heads + 2) * LANES

    @pl.loop(0, seq // TILE)
    def attended_gradient(i):
        at = pl.ds(pl.multiple_of(i * TILE, TILE), TILE)
        ga_ref[at, :] = product_transposed(grad_ref[at, :], pad_ref[width:, :]).astype(BF)

    reduce.exchange()
    dk_ref[...] = jnp.zeros_like(dk_ref)
    dv_ref[...] = jnp.zeros_like(dv_ref)
    low = lax.broadcasted_iota(jnp.int32, (TILE, LANES), 1) < HEAD_SIZE // 2

    def turn_back(u, rows):
        return (u * cos_ref[rows, :] - turned(u, low) * sin_ref[rows, :]).astype(BF)

    for i in range(seq // TILE):
        rows = slice(i * TILE, (i + 1) * TILE)
        for head in range(heads):
            lanes = slice(head * LANES, (head + 1) * LANES)
            q = q_ref[rows, lanes]
            ga = ga_ref[rows, lanes]
            delta = jnp.sum(ga.astype(F32) * att_ref[rows, lanes].astype(F32), axis=1, keepdims=True)
            logs = log_ref[rows, head * LANES : head * LANES + 1]
            dq = jnp.zeros((TILE, LANES), F32)
            for j in range(i + 1):
                keys = slice(j * TILE, (j + 1) * TILE)
                s = product_transposed(q, k_ref[keys, :]) * scale
                p = jnp.where(allowed_tile(start_ref, i * TILE, j * TILE), jnp.exp(s - logs), 0.0)
                dp = product_transposed(ga, v_ref[keys, :])
                ds = (p * (dp - delta) * scale).astype(BF)
                dq = dq + plain_times(ds, k_ref[keys, :])
                dk_ref[keys, :] += transposed_times(ds, q)
                dv_ref[keys, :] += transposed_times(p.astype(BF), ga)
            out_ref[rows, lanes] = turn_back(dq, rows)
    for i in range(seq // TILE):
        rows = slice(i * TILE, (i + 1) * TILE)
        out_ref[rows, heads * LANES : (heads + 1) * LANES] = turn_back(dk_ref[rows, :], rows)
        out_ref[rows, (heads + 1) * LANES :] = dv_ref[rows, :].astype(BF)
    reduce.arrive()

    @pl.loop(0, own_rows // CHUNK)
    def finish_out(k):
        at = chunk_rows(k)
        block_out_ref[at, :] = middle_ref[at, :] + reduce.total(k)

    reduce.drain()


def attend_back(part_out, middle, grad_full, padded, cosine, sine, starts, saved, heads, columns):
    seq, width = grad_full.shape
    rows = seq // columns
    return pl.pallas_call(
        functools.partial(attend_back_kernel, columns, heads),
        out_shape=(
            jax.ShapeDtypeStruct((seq, (heads + 2) * LANES), BF),
            jax.ShapeDtypeStruct((rows, width), F32),
        ),
        in_specs=vmem_specs(12),
        out_specs=tuple(vmem_specs(2)),
        scratch_shapes=[
            pltpu.VMEM((seq, heads * LANES), BF),
            pltpu.VMEM((seq, LANES), F32),
            pltpu.VMEM((seq, LANES), F32),
            *Reduce.scratch(columns // 2, rows, width),
        ],
        compiler_params=comm_params(8),
        name="attend_back",
        cost_estimate=pl.CostEstimate(flops=8_000_000_000, bytes_accessed=20_000_000, transcendentals=2_000_000),
    )(part_out, middle, grad_full, padded, cosine, sine, starts, *saved)


def update_kernel(g_ref, p_ref, m_ref, grad_ref, new_p_ref, new_m_ref):
    gradient = g_ref[...].astype(F32)
    grad_ref[...] = gradient
    parameter = p_ref[...]
    first_moment = BETA_ONE * m_ref[0] + (1.0 - BETA_ONE) * gradient
    second_moment = BETA_TWO * m_ref[1] + (1.0 - BETA_TWO) * gradient * gradient
    new_m_ref[0] = first_moment
    new_m_ref[1] = second_moment
    first_hat = first_moment / (1.0 - BETA_ONE**STEP)
    second_hat = second_moment / (1.0 - BETA_TWO**STEP)
    new_p_ref[...] = parameter - LEARN_RATE * (
        first_hat / (jnp.sqrt(second_hat) + ADAM_EPS) + WEIGHT_DECAY * parameter
    )


def update(gradient, parameter, moments):
    rows, width = parameter.shape
    block = rows // 6 if rows % (6 * CHUNK) == 0 else rows // 3 if rows % (3 * CHUNK) == 0 else rows
    flat = pl.BlockSpec((block, width), lambda i: (i, 0))
    pair = pl.BlockSpec((2, block, width), lambda i: (0, i, 0))
    return pl.pallas_call(
        update_kernel,
        grid=(rows // block,),
        out_shape=(
            jax.ShapeDtypeStruct((rows, width), F32),
            jax.ShapeDtypeStruct((rows, width), F32),
            jax.ShapeDtypeStruct((2, rows, width), F32),
        ),
        in_specs=[flat, flat, pair],
        out_specs=(flat, flat, pair),
        compiler_params=pltpu.CompilerParams(vmem_limit_bytes=VMEM_LIMIT),
        name="update",
        cost_estimate=pl.CostEstimate(
            flops=20 * rows * width, bytes_accessed=30 * rows * width, transcendentals=rows * width
        ),
    )(gradient, parameter, moments)


def rope_tables(positions):
    half_width = HEAD_SIZE // 2
    frequency = ROPE_THETA ** (-2.0 * jnp.arange(half_width, dtype=F32) / HEAD_SIZE)
    angles = positions.astype(F32)[:, None] * frequency[None, :]
    cosine, sine = jnp.cos(angles), jnp.sin(angles)
    blank = jnp.zeros((positions.shape[0], LANES - HEAD_SIZE), F32)
    return (
        jnp.concatenate([cosine, cosine, blank], axis=1),
        jnp.concatenate([-sine, sine, blank], axis=1),
    )


def unpadded(rows, count):
    return jnp.concatenate([rows[k * LANES : k * LANES + HEAD_SIZE] for k in range(count)])


def on_device(
    block_input,
    cotangent,
    documents,
    attn_weights,
    ffn_weights,
    norm_gains,
    attn_moments,
    ffn_moments,
    gain_moments,
):
    layers, columns = lax.axis_size("fsdp"), lax.axis_size("context")
    rows, width = block_input.shape[1:]
    seq = rows * columns
    heads = QUERY_HEADS // columns
    sharers = max(1, columns // KEY_VALUE_HEADS)
    share = KEY_VALUE_HEADS * HEAD_SIZE // columns
    hidden = ffn_weights.shape[0] * layers // 3
    grad_factor = float(rows * layers * columns) ** (-0.5)
    attn_plan, ffn_plan = unit_plans(layers, columns, attn_weights.shape[0] * layers * columns)
    core = lax.rem(lax.axis_index("context"), 2)
    swap = [(c, c + 1 - 2 * (c % 2)) for c in range(columns)]

    x_own = block_input[0]
    aligned = attn_weights.shape[0] % (3 * CHUNK) == 0 and layers > 1
    if aligned:
        docs_full, attn_shard, ffn_shard = spread_step(
            documents, attn_weights, ffn_weights, columns, layers
        )
        h_full, dy_full, attn_col = open_step(
            x_own, norm_gains[0:1], cotangent[0], attn_shard, columns, layers
        )
    else:
        residual = x_own.astype(F32)
        first_hidden = (residual * rms_scale(residual) * (1.0 + norm_gains[0])).astype(BF)
        h_full, docs_full = gather_docs(first_hidden, documents, columns)
        dy_full = gather_plain(cotangent[0], columns)
        attn_col = lax.all_gather(
            attn_plan.spread(attn_weights.astype(BF)), "fsdp", axis=0, tiled=True
        )
        ffn_shard = ffn_plan.spread(ffn_weights.astype(BF))
    ffn_shard, attn_col = lax.optimization_barrier((ffn_shard, attn_col))
    ffn_col = lax.all_gather(ffn_shard, "fsdp", axis=0, tiled=True)
    query_rows = heads * HEAD_SIZE
    if sharers > 1:
        own_part = attn_col[query_rows : query_rows + 2 * share]
        other = lax.ppermute(own_part, "context", swap)

        def whole_head(first):
            mine, theirs = own_part[first : first + share], other[first : first + share]
            return jnp.where(
                core == 0, jnp.concatenate([mine, theirs]), jnp.concatenate([theirs, mine])
            )

        attn_col = jnp.concatenate(
            [
                attn_col[:query_rows],
                whole_head(0),
                whole_head(share),
                attn_col[query_rows + 2 * share :],
            ]
        )
    w_gate, w_up, w_down = ffn_col[:hidden], ffn_col[hidden : 2 * hidden], ffn_col[2 * hidden :]

    all_docs = docs_full.reshape(seq)
    starts = jnp.sum((all_docs[None, :] < all_docs[:, None]).astype(jnp.int32), axis=1)
    cosine, sine = rope_tables(jnp.arange(seq, dtype=jnp.int32) - starts)
    start_lanes = jnp.broadcast_to(starts[:, None], (seq, LANES))
    q_all, k_all, v_all, attended, logs, part, padded = attend(
        h_full, attn_col, cosine, sine, start_lanes, heads
    )
    middle, h2_full = middle_step(part, x_own, norm_gains[1:2], columns)

    gate_pre = product_transposed(h2_full, w_gate)
    up_pre = product_transposed(h2_full, w_up)
    sigmoid_gate = jax.nn.sigmoid(gate_pre)
    activated = (gate_pre * sigmoid_gate * up_pre).astype(BF)
    grad_act = product_transposed(dy_full, w_down)
    grad_gate = (grad_act * up_pre * sigmoid_gate * (1.0 + gate_pre * (1.0 - sigmoid_gate))).astype(BF)
    grad_up = (grad_act * gate_pre * sigmoid_gate).astype(BF)
    ffn_term = jnp.concatenate(
        [
            (transposed_times(grad_gate, h2_full) * grad_factor).astype(BF),
            (transposed_times(grad_up, h2_full) * grad_factor).astype(BF),
            (transposed_times(activated, dy_full) * grad_factor).astype(BF),
        ]
    )
    out_part = plain_times(activated, w_down).astype(BF)
    back_part = (plain_times(grad_gate, w_gate) + plain_times(grad_up, w_up)).astype(BF)
    back_part, ffn_term = lax.optimization_barrier((back_part, ffn_term))
    ffn_sum = lax.psum_scatter(ffn_term, "fsdp", scatter_dimension=0, tiled=True)
    grad_middle, sums, gm_full = turn_step(back_part, middle, cotangent[0], norm_gains[1:2], columns)

    grads, block_out = attend_back(
        out_part,
        middle,
        gm_full,
        padded,
        cosine,
        sine,
        start_lanes,
        (q_all, k_all, v_all, attended, logs),
        heads,
        columns,
    )
    if sharers > 1:
        shared = grads[:, heads * LANES :]
        shared = (shared.astype(F32) + lax.ppermute(shared, "context", swap).astype(F32)).astype(BF)
        lane = jnp.arange(2 * LANES, dtype=jnp.int32) % LANES // share
        grads = jnp.concatenate(
            [grads[:, : heads * LANES], jnp.where(lane == core, shared, jnp.zeros_like(shared))], axis=1
        )
    term_in = (transposed_times(grads, h_full) * grad_factor).astype(BF)
    term_out = (transposed_times(attended, gm_full) * grad_factor).astype(BF)
    if sharers > 1:
        own_rows = [
            lax.dynamic_slice_in_dim(term_in, (heads + k) * LANES + core * share, share, 0)
            for k in range(2)
        ]
        attn_term = jnp.concatenate(
            [unpadded(term_in, heads), *own_rows, unpadded(term_out, heads)]
        )
    else:
        attn_term = jnp.concatenate([unpadded(term_in, heads + 2), unpadded(term_out, heads)])
    in_part = plain_times(grads, padded[: (heads + 2) * LANES]).astype(BF)
    last_args = (in_part, x_own, grad_middle, norm_gains[0:1], sums, columns, layers)
    if aligned:
        grad_input, gain_sums, attn_shard, ffn_shard = last_step(*last_args, (attn_term, ffn_sum))
    else:
        attn_sum = lax.psum_scatter(attn_term, "fsdp", scatter_dimension=0, tiled=True)
        grad_input, gain_sums = last_step(*last_args)
        ffn_shard = ffn_plan.collect(ffn_sum)
        attn_shard = attn_plan.collect(attn_sum)

    column_count = width // (layers * columns)
    first_column = lax.axis_index(EVERY) * column_count
    gain_shard = lax.dynamic_slice_in_dim(gain_sums[:2], first_column, column_count, 1) * grad_factor
    own_gains = lax.dynamic_slice_in_dim(norm_gains, first_column, column_count, 1)
    ffn_shard, new_ffn, ffn_states = update(ffn_shard, ffn_weights, ffn_moments)
    attn_shard, new_attn, attn_states = update(attn_shard, attn_weights, attn_moments)
    new_gains, gain_states = adamw_update(own_gains, gain_shard, gain_moments, 0.0)
    return (
        block_out[None],
        grad_input[None],
        attn_shard,
        ffn_shard,
        gain_shard,
        new_attn,
        new_ffn,
        new_gains,
        attn_states,
        ffn_states,
        gain_states,
    )


def solution(mesh):
    placed = (
        P("fsdp", "context", None),
        P("fsdp", "context", None),
        P("fsdp", "context"),
        P(EVERY, None),
        P(EVERY, None),
        P(),
        P(None, EVERY, None),
        P(None, EVERY, None),
        P(None, None, EVERY),
    )
    return jax.shard_map(
        on_device,
        mesh=mesh,
        in_specs=placed,
        out_specs=(
            P("fsdp", "context", None),
            P("fsdp", "context", None),
            P(EVERY, None),
            P(EVERY, None),
            P(None, EVERY),
            P(EVERY, None),
            P(EVERY, None),
            P(None, EVERY),
            P(None, EVERY, None),
            P(None, EVERY, None),
            P(None, None, EVERY),
        ),
        check_vma=False,
    )
```

```python
import functools

import jax
import jax.numpy as jnp
import numpy as np
from jax import lax
from jax.experimental import pallas as pl
from jax.experimental.pallas import tpu as pltpu
from jax.sharding import PartitionSpec as P

QUERY_HEADS = 16
KEY_VALUE_HEADS = 8
HEAD_SIZE = 96
STEP = 3

NORM_EPS = 1e-05
ROPE_THETA = 100000.0
BETA_ONE = 0.9
BETA_TWO = 0.95
ADAM_EPS = 1e-08
LEARN_RATE = 0.02
WEIGHT_DECAY = 0.1

LANES = 128
TILE = 256
CHUNK = 16
VMEM_LIMIT = 62 * 1024 * 1024
EVERY = ("fsdp", "context")
BF = jnp.bfloat16
F32 = jnp.float32
ID_TYPE = pl.DeviceIdType.MESH


def product_transposed(left_matrix, right_matrix):
    return lax.dot_general(
        left_matrix, right_matrix, (((1,), (1,)), ((), ())), preferred_element_type=F32
    )


def transposed_times(left_matrix, right_matrix):
    return lax.dot_general(
        left_matrix, right_matrix, (((0,), (0,)), ((), ())), preferred_element_type=F32
    )


def plain_times(left_matrix, right_matrix):
    return jnp.dot(left_matrix, right_matrix, preferred_element_type=F32)


def rms_scale(tensor_in):
    return lax.rsqrt(jnp.mean(tensor_in * tensor_in, axis=-1, keepdims=True) + NORM_EPS)


def norm_backward(grad_in, normed, norm_scale, gain_row):
    scaled = grad_in * (1.0 + gain_row)
    return norm_scale * (scaled - normed * jnp.mean(scaled * normed, axis=-1, keepdims=True))


def adamw_update(parameter, gradient, moments, decay_rate):
    first_moment = BETA_ONE * moments[0] + (1.0 - BETA_ONE) * gradient
    second_moment = BETA_TWO * moments[1] + (1.0 - BETA_TWO) * gradient * gradient
    first_hat = first_moment / (1.0 - BETA_ONE**STEP)
    second_hat = second_moment / (1.0 - BETA_TWO**STEP)
    updated = parameter - LEARN_RATE * (
        first_hat / (jnp.sqrt(second_hat) + ADAM_EPS) + decay_rate * parameter
    )
    return (updated, (first_moment, second_moment))


class UnitPlan:
    def __init__(self, homes, devices):
        waiting = [[] for _ in range(devices)]
        for unit, (device, place) in enumerate(homes):
            waiting[unit // 3].append((unit % 3, device, place))
        self.rounds = []
        for _ in range(3):
            taken = [None] * devices

            def settle(source, seen):
                for piece, device, place in waiting[source]:
                    if device in seen:
                        continue
                    seen.add(device)
                    if taken[device] is None or settle(taken[device][0], seen):
                        taken[device] = (source, piece, place)
                        return True
                return False

            for source in range(devices):
                if not settle(source, set()):
                    raise ValueError("no matching")
            pairs, pieces, places = [], [0] * devices, [0] * devices
            for device, (source, piece, place) in enumerate(taken):
                pairs.append((source, device))
                pieces[source] = piece
                places[device] = place
                waiting[source].remove((piece, device, place))
            self.rounds.append((pairs, np.array(pieces), np.array(places)))

    def _reorder(self, got, columns):
        order = np.argsort(np.stack(columns, axis=1), axis=1).astype(np.int32)
        mine = jnp.asarray(order)[lax.axis_index(EVERY)]
        stacked = jnp.stack(got)
        return jnp.concatenate(
            [lax.dynamic_index_in_dim(stacked, mine[k], 0, keepdims=False) for k in range(3)]
        )

    def spread(self, rows):
        pieces = rows.reshape(3, rows.shape[0] // 3, rows.shape[1])
        me = lax.axis_index(EVERY)
        got = []
        for pairs, piece, _ in self.rounds:
            unit = lax.dynamic_index_in_dim(
                pieces, jnp.asarray(piece, jnp.int32)[me], 0, keepdims=False
            )
            got.append(lax.ppermute(unit, EVERY, pairs))
        return self._reorder(got, [place for _, _, place in self.rounds])

    def collect(self, rows):
        places_of = rows.reshape(3, rows.shape[0] // 3, rows.shape[1])
        me = lax.axis_index(EVERY)
        got = []
        for pairs, _, place in self.rounds:
            unit = lax.dynamic_index_in_dim(
                places_of, jnp.asarray(place, jnp.int32)[me], 0, keepdims=False
            )
            got.append(lax.ppermute(unit, EVERY, [(b, a) for a, b in pairs]))
        return self._reorder(got, [piece for _, piece, _ in self.rounds])


def unit_plans(layers, columns, attn_rows):
    devices = layers * columns

    def home(column, position):
        return ((position // 3) * columns + column, position % 3)

    homes = []
    for unit in range(3 * devices):
        matrix, rest = divmod(unit, devices)
        stretch, column = divmod(rest, columns)
        homes.append(home(column, matrix * layers + stretch))
    ffn_plan = UnitPlan(homes, devices)
    unit_rows = attn_rows // (3 * devices)
    query_units = QUERY_HEADS * HEAD_SIZE // columns // unit_rows
    share_units = KEY_VALUE_HEADS * HEAD_SIZE // columns // unit_rows
    homes = []
    position = 0
    for count in (query_units, share_units, share_units, query_units):
        for column in range(columns):
            for k in range(count):
                homes.append(home(column, position + k))
        position += count
    return UnitPlan(homes, devices), ffn_plan


class Homes:
    def __init__(self, layers, columns, attn_rows):
        devices = layers * columns
        unit_rows = attn_rows // (3 * devices)
        self.layers, self.columns = layers, columns
        self.counts = [
            QUERY_HEADS * HEAD_SIZE // columns // unit_rows,
            KEY_VALUE_HEADS * HEAD_SIZE // columns // unit_rows,
        ]
        query, share = self.counts
        self.first = [0, query, query + share, query + 2 * share]
        self.sizes = [query, share, share, query]

    def _spot(self, column, position):
        return position // 3, column, position % 3

    def _column(self, group):
        half = self.columns // 2
        return group % half * 2 + group // half

    def _group(self, column):
        return column % 2 * (self.columns // 2) + column // 2

    def attn_targets(self):
        device = lax.axis_index("fsdp") * self.columns + lax.axis_index("context")
        found = []
        for piece in range(3):
            unit = device * 3 + piece
            column, position = 0, 0
            for first, size in zip(self.first, self.sizes):
                inside = unit - first * self.columns
                begun = inside >= 0
                column = jnp.where(begun, self._column(inside // size), column)
                position = jnp.where(begun, first + inside % size, position)
            found.append(self._spot(column, position))
        return found

    def attn_owners(self):
        group = self._group(lax.axis_index("context"))
        found = []
        for place in range(3):
            position = lax.axis_index("fsdp") * 3 + place
            unit = 0
            for first, size in zip(self.first, self.sizes):
                inside = position - first
                unit = jnp.where(inside >= 0, first * self.columns + group * size + inside, unit)
            device = unit // 3
            found.append((device // self.columns, device % self.columns, unit % 3))
        return found

    def ffn_targets(self):
        layer, column = lax.axis_index("fsdp"), lax.axis_index("context")
        return [
            (layer, (3 * column + piece) % self.columns, (3 * column + piece) // self.columns)
            for piece in range(3)
        ]

    def ffn_owners(self):
        layer, column = lax.axis_index("fsdp"), lax.axis_index("context")
        return [
            (layer, (place * self.columns + column) // 3, (place * self.columns + column) % 3)
            for place in range(3)
        ]


def partner(me, step, chips):
    return lax.rem(me // 2 + step, chips) * 2 + lax.rem(me, 2)


def sibling_of(me):
    return me + 1 - 2 * lax.rem(me, 2)


def rows_at(index, rows):
    return pl.ds(pl.multiple_of(index * rows, rows), rows)


def greet(columns, layers=1, others=()):
    barrier = pltpu.get_barrier_semaphore()
    me = lax.axis_index("context")
    awaited = columns - 1 + layers - 1
    for layer, column in others:
        apart = (layer != lax.axis_index("fsdp")) | (column != me)
        awaited = awaited + jnp.where(apart, 1, 0)

        @pl.when(apart)
        def there():
            pl.semaphore_signal(
                barrier, inc=1, device_id={"fsdp": layer, "context": column}, device_id_type=ID_TYPE
            )

    for step in range(1, columns):
        pl.semaphore_signal(
            barrier, inc=1, device_id={"context": lax.rem(me + step, columns)}, device_id_type=ID_TYPE
        )
    if layers > 1:
        layer = lax.axis_index("fsdp")
        for step in range(1, layers):
            pl.semaphore_signal(
                barrier, inc=1, device_id={"fsdp": lax.rem(layer + step, layers)}, device_id_type=ID_TYPE
            )
    pl.semaphore_wait(barrier, awaited)


def send(source, target, send_sem, recv_sem, device):
    copy = pltpu.make_async_remote_copy(
        src_ref=source,
        dst_ref=target,
        send_sem=send_sem,
        recv_sem=recv_sem,
        device_id=device,
        device_id_type=ID_TYPE,
    )
    copy.start()
    return copy


def remote(source, target, send_sem, recv_sem, device):
    return pltpu.make_async_remote_copy(
        src_ref=source,
        dst_ref=target,
        send_sem=send_sem,
        recv_sem=recv_sem,
        device_id=device,
        device_id_type=ID_TYPE,
    )


class Exchange:
    @staticmethod
    def scratch():
        return [pltpu.SemaphoreType.DMA((3,)), pltpu.SemaphoreType.DMA((3,))]

    def __init__(self, sources, targets, homes, sems):
        send_sem, recv_sem = sems
        self.parts = []
        for i, (layer, column, place) in enumerate(homes):
            itself = (layer == lax.axis_index("fsdp")) & (column == lax.axis_index("context"))
            target = targets(layer, place)
            copy = functools.partial(
                remote,
                sources[i],
                target,
                send_sem.at[i],
                recv_sem.at[place],
                {"fsdp": layer, "context": column},
            )
            stay = functools.partial(pltpu.make_async_copy, sources[i], target, recv_sem.at[place])

            @pl.when(itself)
            def here():
                stay().start()

            @pl.when(jnp.logical_not(itself))
            def there():
                copy().start()

            self.parts.append((itself, copy))
        self.landing = [
            functools.partial(pltpu.make_async_copy, sources[k], sources[k], recv_sem.at[k])
            for k in range(3)
        ]

    def arrive(self):
        for landed in self.landing:
            landed().wait()

    def drain(self):
        for itself, copy in self.parts:

            @pl.when(jnp.logical_not(itself))
            def sent():
                copy().wait_send()


class LineGather:
    @staticmethod
    def scratch(layers, pieces):
        return [*[pltpu.SemaphoreType.DMA(((layers - 1) * pieces,))] * 4, pltpu.SemaphoreType.DMA]

    def __init__(self, full, own, layers, pieces, sems):
        self.full, self.own, self.layers, self.pieces = full, own, layers, pieces
        *self.sems, local_sem = sems
        self.rows = own.shape[0]
        self.size = self.rows // pieces
        self.count = (layers - 1) * pieces
        self.local = pltpu.make_async_copy(
            own, full.at[rows_at(lax.axis_index("fsdp"), self.rows), :], local_sem
        )
        for m in range(pieces):
            self._send(m)
        self.local.start()
        self.next = pieces

    def _block(self, shard, piece):
        first = pl.multiple_of(shard * self.rows + piece * self.size, self.size)
        return self.full.at[pl.ds(first, self.size), :]

    def _moves(self, m):
        k, piece = divmod(m, self.pieces)
        layer = lax.axis_index("fsdp")
        up_send, up_recv, down_send, down_recv = self.sems
        top = self.layers - 1
        for first, last, other, shard, send_sem, recv_sem in (
            (layer - k >= 0, layer < top, layer + 1, layer - k, up_send, up_recv),
            (layer + k <= top, layer > 0, layer - 1, layer + k, down_send, down_recv),
        ):
            block = self._block(shard, piece)
            source = self.own.at[pl.ds(piece * self.size, self.size), :] if k == 0 else block
            yield first & last, functools.partial(
                remote, source, block, send_sem.at[m], recv_sem.at[m], {"fsdp": other}
            )

    def _send(self, m):
        for go, copy in self._moves(m):

            @pl.when(go)
            def start():
                copy().start()

    def _land(self, m):
        k, piece = divmod(m, self.pieces)
        layer = lax.axis_index("fsdp")
        _, up_recv, _, down_recv = self.sems
        for there, shard, recv_sem in (
            (layer - 1 - k >= 0, layer - 1 - k, up_recv),
            (layer + 1 + k <= self.layers - 1, layer + 1 + k, down_recv),
        ):
            block = self._block(shard, piece)
            copy = functools.partial(pltpu.make_async_copy, block, block, recv_sem.at[m])

            @pl.when(there)
            def landed():
                copy().wait()

    def relay(self, count=None):
        stop = self.count if count is None else min(self.count, self.next + count)
        for m in range(self.next, stop):
            self._land(m - self.pieces)
            self._send(m)
        self.next = stop

    def finish(self):
        self.relay()
        for m in range(self.count - self.pieces, self.count):
            self._land(m)
        for m in range(self.count):
            for go, copy in self._moves(m):

                @pl.when(go)
                def sent():
                    copy().wait_send()

        self.local.wait()


class LineReduce:
    @staticmethod
    def scratch(layers, pieces, rows, width):
        count = (layers - 1) * pieces
        return [
            pltpu.VMEM((count, rows // pieces, width), BF),
            pltpu.VMEM((count, rows // pieces, width), BF),
            *[pltpu.SemaphoreType.DMA((count,))] * 4,
        ]

    def __init__(self, term, layers, pieces, scratch):
        self.term, self.layers, self.pieces = term, layers, pieces
        self.rows = term.shape[0] // layers
        self.size = self.rows // pieces
        self.up_in, self.down_in, *self.sems = scratch
        self.count = (layers - 1) * pieces
        self.slots = self.count + layers - 1
        self.next = 1
        layer = lax.axis_index("fsdp")
        top = layers - 1

        @pl.when(layer == 0)
        def bottom():
            for m in range(self.count):
                self._up(m, self._block(top - m // pieces, m % pieces)).start()

        @pl.when(layer == top)
        def ceiling():
            for m in range(self.count):
                self._down(m, self._block(m // pieces, m % pieces)).start()

    def _block(self, target, piece):
        return self.term.at[pl.ds(target * self.rows + piece * self.size, self.size), :]

    def _up(self, m, source):
        up_send, up_recv, _, _ = self.sems
        other = {"fsdp": lax.axis_index("fsdp") + 1}
        return remote(source, self.up_in.at[m], up_send.at[m], up_recv.at[m], other)

    def _down(self, m, source):
        _, _, down_send, down_recv = self.sems
        other = {"fsdp": lax.axis_index("fsdp") - 1}
        return remote(source, self.down_in.at[m], down_send.at[m], down_recv.at[m], other)

    def _add(self, sums, m, target):
        first = pl.multiple_of(target * self.rows + m % self.pieces * self.size, CHUNK)

        @pl.loop(0, self.size // CHUNK)
        def add(c):
            at = chunk_rows(c)
            of_term = pl.ds(pl.multiple_of(first + c * CHUNK, CHUNK), CHUNK)
            sums[m, at, :] = (
                sums[m, at, :].astype(F32) + self.term[of_term, :].astype(F32)
            ).astype(BF)

    def _slot(self, slot):
        layer = lax.axis_index("fsdp")
        top = self.layers - 1
        _, up_recv, _, down_recv = self.sems
        m = slot - layer
        target = top - m // self.pieces

        @pl.when((layer > 0) & (m >= 0) & (m < self.count) & (layer <= target))
        def from_below():
            pltpu.make_async_copy(self.up_in.at[m], self.up_in.at[m], up_recv.at[m]).wait()

            @pl.when(layer < target)
            def pass_up():
                self._add(self.up_in, m, target)
                self._up(m, self.up_in.at[m]).start()

        n = slot - (top - layer)
        goal = n // self.pieces

        @pl.when((layer < top) & (n >= 0) & (n < self.count) & (layer >= goal))
        def from_above():
            pltpu.make_async_copy(self.down_in.at[n], self.down_in.at[n], down_recv.at[n]).wait()

            @pl.when(layer > goal)
            def pass_down():
                self._add(self.down_in, n, goal)
                self._down(n, self.down_in.at[n]).start()

    def relay(self, count=None):
        stop = self.slots if count is None else min(self.slots, self.next + count)
        if stop > self.next:

            @pl.loop(self.next, stop)
            def slots(slot):
                self._slot(slot)

        self.next = stop

    def finish(self, total):
        self.relay()
        layer = lax.axis_index("fsdp")
        top = self.layers - 1
        for own in range(self.layers):

            @pl.when(layer == own)
            def here():
                for piece in range(self.pieces):

                    @pl.loop(0, self.size // CHUNK)
                    def add(c):
                        start = pl.multiple_of(c * CHUNK, CHUNK)
                        at = pl.ds(start, CHUNK)
                        value = self.term[
                            pl.ds(own * self.rows + piece * self.size + start, CHUNK), :
                        ].astype(F32)
                        if own > 0:
                            m = (top - own) * self.pieces + piece
                            value = value + self.up_in[m, at, :].astype(F32)
                        if own < top:
                            m = own * self.pieces + piece
                            value = value + self.down_in[m, at, :].astype(F32)
                        total[pl.ds(piece * self.size + start, CHUNK), :] = value.astype(BF)

    def drain(self):
        layer = lax.axis_index("fsdp")
        top = self.layers - 1
        for m in range(self.count):
            k = m // self.pieces

            @pl.when(layer < top - k)
            def up():
                self._up(m, self.up_in.at[m]).wait_send()

            @pl.when(layer > k)
            def down():
                self._down(m, self.down_in.at[m]).wait_send()


class Gather:
    @staticmethod
    def scratch(chips):
        return [
            pltpu.SemaphoreType.DMA((chips,)),
            pltpu.SemaphoreType.DMA((chips,)),
            pltpu.SemaphoreType.DMA((chips,)),
            pltpu.SemaphoreType.DMA((chips,)),
            pltpu.SemaphoreType.DMA,
        ]

    def __init__(self, block, full, chips, sems):
        own_send, own_recv, self.on_send, self.on_recv, local_sem = sems
        me = lax.axis_index("context")
        rows = block.shape[0]
        self.block, self.full, self.chips, self.me, self.rows = block, full, chips, me, rows
        mine = full.at[rows_at(me, rows), :]
        self.own = [
            send(block, mine, own_send.at[step], own_recv.at[step], {"context": partner(me, step, chips)})
            for step in range(1, chips)
        ]
        self.own.append(
            send(block, mine, own_send.at[0], own_recv.at[0], {"context": sibling_of(me)})
        )
        self.local = pltpu.make_async_copy(block, mine, local_sem)
        self.local.start()

        self.passed = []

    def pass_on(self):
        for step in range(1, self.chips):
            self.own[step - 1].wait_recv()
            source = partner(self.me, self.chips - step, self.chips)
            there = self.full.at[rows_at(source, self.rows), :]
            self.passed.append(
                send(there, there, self.on_send.at[step], self.on_recv.at[step], {"context": sibling_of(self.me)})
            )

    def finish(self):
        if not self.passed:
            self.pass_on()
        self.own[-1].wait_recv()
        for copy in self.passed:
            copy.wait_recv()
        for copy in self.own + self.passed:
            copy.wait_send()
        self.local.wait()


class Reduce:
    @staticmethod
    def scratch(chips, rows, width):
        return [
            pltpu.VMEM((chips, rows, width), BF),
            pltpu.VMEM((chips, rows, width), BF),
            pltpu.VMEM((chips, rows, width), BF),
            pltpu.SemaphoreType.DMA((chips,)),
            pltpu.SemaphoreType.DMA((chips,)),
            pltpu.SemaphoreType.DMA((chips,)),
            pltpu.SemaphoreType.DMA((chips,)),
        ]

    def __init__(self, part, chips, rows, scratch):
        self.near, self.summed, self.far, near_send, near_recv, self.far_send, self.far_recv = scratch
        me = lax.axis_index("context")
        self.part, self.chips, self.rows, self.me = part, chips, rows, me
        self.near_copies = {}
        for step in [*range(1, chips), 0]:
            block = partner(sibling_of(me), step, chips)
            self.near_copies[step] = send(
                part.at[rows_at(block, rows), :],
                self.near.at[step],
                near_send.at[step],
                near_recv.at[step],
                {"context": sibling_of(me)},
            )
        self.far_copies = []

    def exchange(self):
        for step in range(1, self.chips):
            self.near_copies[step].wait_recv()
            target = partner(self.me, step, self.chips)
            first = pl.multiple_of(target * self.rows, self.rows)

            @pl.loop(0, self.rows // CHUNK)
            def add(k):
                at = pl.ds(pl.multiple_of(k * CHUNK, CHUNK), CHUNK)
                from_part = pl.ds(pl.multiple_of(first + k * CHUNK, CHUNK), CHUNK)
                self.summed[step, at, :] = (
                    self.part[from_part, :].astype(F32) + self.near[step, at, :].astype(F32)
                ).astype(BF)

            self.far_copies.append(
                send(
                    self.summed.at[step],
                    self.far.at[step],
                    self.far_send.at[step],
                    self.far_recv.at[step],
                    {"context": target},
                )
            )

    def arrive(self):
        self.near_copies[0].wait_recv()
        for copy in self.far_copies:
            copy.wait_recv()

    def total(self, k):
        at = pl.ds(pl.multiple_of(k * CHUNK, CHUNK), CHUNK)
        first = pl.multiple_of(self.me * self.rows, self.rows)
        value = self.part[pl.ds(pl.multiple_of(first + k * CHUNK, CHUNK), CHUNK), :].astype(F32)
        value = value + self.near[0, at, :].astype(F32)
        for step in range(1, self.chips):
            value = value + self.far[step, at, :].astype(F32)
        return value

    def drain(self):
        for copy in list(self.near_copies.values()) + self.far_copies:
            copy.wait_send()


def chunk_rows(k):
    return pl.ds(pl.multiple_of(k * CHUNK, CHUNK), CHUNK)


def vmem_specs(count):
    return [pl.BlockSpec(memory_space=pltpu.VMEM)] * count


def comm_params(collective_id):
    return pltpu.CompilerParams(
        collective_id=collective_id, has_side_effects=True, vmem_limit_bytes=VMEM_LIMIT
    )


def place_rows(ref, unit, layer, place):
    return ref.at[rows_at(place, unit), :]


class Docs:
    @staticmethod
    def scratch(columns):
        return [
            pltpu.SemaphoreType.DMA((columns,)),
            pltpu.SemaphoreType.DMA((columns,)),
            pltpu.SemaphoreType.DMA,
        ]

    def __init__(self, docs, docs_full, columns, sems):
        docs_send, docs_recv, docs_local = sems
        me = lax.axis_index("context")
        mine = docs_full.at[pl.ds(me, 1), :]
        self.copies = [
            send(docs, mine, docs_send.at[step], docs_recv.at[step], {"context": lax.rem(me + step, columns)})
            for step in range(1, columns)
        ]
        self.local = pltpu.make_async_copy(docs, mine, docs_local)
        self.local.start()

    def finish(self):
        for copy in self.copies:
            copy.wait_recv()
        for copy in self.copies:
            copy.wait_send()
        self.local.wait()


def open_kernel(
    columns,
    layers,
    homes,
    x_ref,
    gain_ref,
    docs,
    attn_ref,
    ffn_ref,
    h_full,
    docs_full,
    attn_col,
    ffn_shard,
    hidden,
    attn_bf,
    ffn_bf,
    attn_shard,
    *scratch,
):
    attn_rows, ffn_rows = attn_ref.shape[0], ffn_ref.shape[0]

    @pl.loop(0, attn_rows // CHUNK)
    def cast_attn(k):
        attn_bf[chunk_rows(k), :] = attn_ref[chunk_rows(k), :].astype(BF)

    targets = homes.attn_targets()
    greet(columns, layers, [spot[:2] for spot in targets + homes.attn_owners()])
    unit = attn_rows // 3
    attn_spread = Exchange(
        [attn_bf.at[pl.ds(k * unit, unit), :] for k in range(3)],
        functools.partial(place_rows, attn_shard, unit),
        targets,
        scratch[0:2],
    )

    @pl.loop(0, x_ref.shape[0] // CHUNK)
    def norm(k):
        residual = x_ref[chunk_rows(k), :].astype(F32)
        hidden[chunk_rows(k), :] = (residual * rms_scale(residual) * (1.0 + gain_ref[...])).astype(BF)

    documents = Docs(docs, docs_full, columns, scratch[2:5])
    gather = Gather(hidden, h_full, columns // 2, scratch[5:10])

    @pl.loop(0, ffn_rows // CHUNK)
    def cast_ffn(k):
        ffn_bf[chunk_rows(k), :] = ffn_ref[chunk_rows(k), :].astype(BF)

    attn_spread.arrive()
    line = LineGather(attn_col, attn_shard, layers, 1, scratch[10:15])
    unit = ffn_rows // 3
    ffn_spread = Exchange(
        [ffn_bf.at[pl.ds(k * unit, unit), :] for k in range(3)],
        functools.partial(place_rows, ffn_shard, unit),
        homes.ffn_targets(),
        scratch[15:17],
    )
    line.relay(1)
    gather.pass_on()
    line.relay()
    documents.finish()
    gather.finish()
    ffn_spread.arrive()
    line.finish()
    attn_spread.drain()
    ffn_spread.drain()


def open_step(x_own, gain_row, docs, attn_weights, ffn_weights, columns, layers):
    rows, width = x_own.shape
    attn_rows, ffn_rows = attn_weights.shape[0], ffn_weights.shape[0]
    homes = Homes(layers, columns, attn_rows * layers * columns)
    return pl.pallas_call(
        functools.partial(open_kernel, columns, layers, homes),
        out_shape=(
            jax.ShapeDtypeStruct((columns * rows, width), BF),
            jax.ShapeDtypeStruct((columns, docs.shape[1]), jnp.int32),
            jax.ShapeDtypeStruct((layers * attn_rows, width), BF),
            jax.ShapeDtypeStruct((ffn_rows, width), BF),
        ),
        in_specs=vmem_specs(5),
        out_specs=tuple([pl.BlockSpec(memory_space=pl.ANY)] * 4),
        scratch_shapes=[
            pltpu.VMEM((rows, width), BF),
            pltpu.VMEM((attn_rows, width), BF),
            pltpu.VMEM((ffn_rows, width), BF),
            pltpu.VMEM((attn_rows, width), BF),
            *Exchange.scratch(),
            *Docs.scratch(columns),
            *Gather.scratch(columns // 2),
            *LineGather.scratch(layers, 1),
            *Exchange.scratch(),
        ],
        compiler_params=comm_params(1),
        name="open_step",
        cost_estimate=pl.CostEstimate(flops=0, bytes_accessed=150_000_000, transcendentals=0),
    )(x_own, gain_row, docs, attn_weights, ffn_weights)


def gather_docs_kernel(columns, block, docs, full, docs_full, *scratch):
    greet(columns)
    gather = Gather(block, full, columns // 2, scratch[:5])
    documents = Docs(docs, docs_full, columns, scratch[5:])
    gather.finish()
    documents.finish()


def gather_docs(block, docs, columns):
    rows, width = block.shape
    return pl.pallas_call(
        functools.partial(gather_docs_kernel, columns),
        out_shape=(
            jax.ShapeDtypeStruct((columns * rows, width), BF),
            jax.ShapeDtypeStruct((columns, docs.shape[1]), jnp.int32),
        ),
        in_specs=vmem_specs(2),
        out_specs=(pl.BlockSpec(memory_space=pl.ANY), pl.BlockSpec(memory_space=pl.ANY)),
        scratch_shapes=[*Gather.scratch(columns // 2), *Docs.scratch(columns)],
        compiler_params=comm_params(2),
        name="gather_docs",
        cost_estimate=pl.CostEstimate(flops=0, bytes_accessed=60_000_000, transcendentals=0),
    )(block, docs)


def last_kernel(columns, layers, homes, *refs):
    (part_in, x_ref, grad_ref, gain_ref, sums_ref), refs = refs[:5], refs[5:]
    if homes is not None:
        (term, ffn_sum), refs = refs[:2], refs[2:]
    (input_grad_ref, gains_ref), refs = refs[:2], refs[2:]
    if homes is not None:
        (attn_back, ffn_back), refs = refs[:2], refs[2:]
    (own_sums, plane_slots, plane_sums, line_slots), refs = refs[:4], refs[4:]
    (plane_send, plane_recv, line_send, line_recv), scratch = refs[:4], refs[4:]
    chips = columns // 2
    rows = x_ref.shape[0]
    if homes is None:
        greet(columns, layers)
    else:
        attn_owners = homes.attn_owners()
        greet(columns, layers, [spot[:2] for spot in homes.attn_targets() + attn_owners])
    first = Reduce(part_in, chips, rows, scratch[:7])
    if homes is not None:
        attn_rows, ffn_rows = term.shape[0] // layers, ffn_sum.shape[0]
        attn_done = scratch[7]
        line = LineReduce(term, layers, 3, scratch[8:14])
        unit_ffn = ffn_rows // 3
    first.exchange()
    if homes is not None:
        ffn_owned = Exchange(
            [ffn_sum.at[pl.ds(k * unit_ffn, unit_ffn), :] for k in range(3)],
            functools.partial(place_rows, ffn_back, unit_ffn),
            homes.ffn_owners(),
            scratch[14:16],
        )
        line.relay(3)
    own_sums[...] = jnp.zeros_like(own_sums)
    own_sums[1:2, :] = sums_ref[0:1, :]
    if homes is not None:
        line.relay(3)
    first.arrive()

    @pl.loop(0, rows // CHUNK)
    def finish(k):
        at = chunk_rows(k)
        grad_hidden = first.total(k)
        residual = x_ref[at, :].astype(F32)
        scale = rms_scale(residual)
        normed = residual * scale
        own_sums[0:1, :] += jnp.sum(grad_hidden * normed, axis=0, keepdims=True)
        input_grad_ref[at, :] = grad_ref[at, :] + norm_backward(
            grad_hidden, normed, scale, gain_ref[...]
        )

    me = lax.axis_index("context")
    layer = lax.axis_index("fsdp")
    in_plane = [
        send(
            own_sums,
            plane_slots.at[step],
            plane_send.at[step],
            plane_recv.at[step],
            {"context": lax.rem(me + step, columns)},
        )
        for step in range(1, columns)
    ]
    if homes is not None:
        line.finish(attn_done)
        unit = attn_rows // 3
        attn_owned = Exchange(
            [attn_done.at[pl.ds(k * unit, unit), :] for k in range(3)],
            functools.partial(place_rows, attn_back, unit),
            attn_owners,
            scratch[16:18],
        )
    total = own_sums[...]
    for step, copy in enumerate(in_plane):
        copy.wait_recv()
        total = total + plane_slots[step + 1]
    plane_sums[...] = total
    in_line = [
        send(
            plane_sums,
            line_slots.at[step],
            line_send.at[step],
            line_recv.at[step],
            {"fsdp": lax.rem(layer + step, layers)},
        )
        for step in range(1, layers)
    ]
    for step, copy in enumerate(in_line):
        copy.wait_recv()
        total = total + line_slots[step + 1]
    gains_ref[...] = total
    if homes is not None:
        ffn_owned.arrive()
        attn_owned.arrive()
        ffn_owned.drain()
        attn_owned.drain()
        line.drain()
    for copy in in_plane + in_line:
        copy.wait_send()
    first.drain()


def last_step(part_in, x_own, grad_middle, gain_row, sums, columns, layers, weight_sums=()):
    rows, width = x_own.shape
    chips = columns // 2
    homes = None
    back_shapes, back_scratch = [], []
    if weight_sums:
        term, ffn_sum = weight_sums
        attn_rows = term.shape[0] // layers
        homes = Homes(layers, columns, attn_rows * layers * columns)
        back_shapes = [
            jax.ShapeDtypeStruct((attn_rows, width), BF),
            jax.ShapeDtypeStruct(ffn_sum.shape, BF),
        ]
        back_scratch = [
            pltpu.VMEM((attn_rows, width), BF),
            *LineReduce.scratch(layers, 3, attn_rows, width),
            *Exchange.scratch(),
            *Exchange.scratch(),
        ]
    return pl.pallas_call(
        functools.partial(last_kernel, columns, layers, homes),
        out_shape=(
            jax.ShapeDtypeStruct((rows, width), F32),
            jax.ShapeDtypeStruct((8, width), F32),
            *back_shapes,
        ),
        in_specs=vmem_specs(5 + len(weight_sums)),
        out_specs=tuple(vmem_specs(2) + [pl.BlockSpec(memory_space=pl.ANY)] * len(back_shapes)),
        scratch_shapes=[
            pltpu.VMEM((8, width), F32),
            pltpu.VMEM((columns, 8, width), F32),
            pltpu.VMEM((8, width), F32),
            pltpu.VMEM((layers, 8, width), F32),
            pltpu.SemaphoreType.DMA((columns,)),
            pltpu.SemaphoreType.DMA((columns,)),
            pltpu.SemaphoreType.DMA((layers,)),
            pltpu.SemaphoreType.DMA((layers,)),
            *Reduce.scratch(chips, rows, width),
            *back_scratch,
        ],
        compiler_params=comm_params(5),
        name="last_step",
        cost_estimate=pl.CostEstimate(flops=0, bytes_accessed=150_000_000, transcendentals=0),
    )(part_in, x_own, grad_middle, gain_row, sums, *weight_sums)


def turned(heads, low):
    return jnp.where(low, pltpu.roll(heads, LANES - HEAD_SIZE // 2, 1), pltpu.roll(heads, HEAD_SIZE // 2, 1))


def allowed_tile(start_ref, row_first, col_first):
    rows = row_first + lax.broadcasted_iota(jnp.int32, (TILE, TILE), 0)
    cols = col_first + lax.broadcasted_iota(jnp.int32, (TILE, TILE), 1)
    starts = jnp.broadcast_to(start_ref[row_first : row_first + TILE, 0:1], (TILE, TILE))
    return (cols <= rows) & (cols >= starts)


def forward_kernel(columns, layers, heads, *refs):
    (h_ref, w_ref, cos_ref, sin_ref, start_ref, x_ref, gain_ref, dy_ref, ffn_shard), refs = refs[:9], refs[9:]
    (q_ref, k_ref, v_ref, att_ref, log_ref, pad_ref, middle_ref), refs = refs[:7], refs[7:]
    (h2_full, dy_full, ffn_col), (part_ref, hidden, *scratch) = refs[:3], refs[3:]
    seq, own_rows, chips = h_ref.shape[0], x_ref.shape[0], columns // 2
    greet(columns, layers)
    line = LineGather(ffn_col, ffn_shard, layers, 3, scratch[0:5])
    dy_gather = Gather(dy_ref, dy_full, chips, scratch[5:10])
    scale = HEAD_SIZE**-0.5
    for slot in range(2 * heads + 2):
        pad_ref[slot * LANES : slot * LANES + HEAD_SIZE, :] = w_ref[
            slot * HEAD_SIZE : (slot + 1) * HEAD_SIZE, :
        ]
        pad_ref[slot * LANES + HEAD_SIZE : (slot + 1) * LANES, :] = jnp.zeros(
            (LANES - HEAD_SIZE, w_ref.shape[1]), BF
        )
    width = (heads + 2) * LANES

    @pl.loop(0, seq // TILE)
    def project(i):
        at = pl.ds(pl.multiple_of(i * TILE, TILE), TILE)
        low = lax.broadcasted_iota(jnp.int32, (TILE, LANES), 1) < HEAD_SIZE // 2
        projected = product_transposed(h_ref[at, :], pad_ref[0:width, :])
        cosine, sine = cos_ref[at, :], sin_ref[at, :]
        for head in range(heads + 1):
            u = projected[:, head * LANES : (head + 1) * LANES]
            r = (u * cosine + turned(u, low) * sine).astype(BF)
            if head < heads:
                q_ref[at, head * LANES : (head + 1) * LANES] = r
            else:
                k_ref[at, :] = r
        v_ref[at, :] = projected[:, (heads + 1) * LANES :].astype(BF)

    for i in range(seq // TILE):
        rows = slice(i * TILE, (i + 1) * TILE)
        for head in range(heads):
            lanes = slice(head * LANES, (head + 1) * LANES)
            q = q_ref[rows, lanes]
            out = jnp.zeros((TILE, LANES), F32)
            total = jnp.zeros((TILE, 1), F32)
            for j in range(i + 1):
                keys = slice(j * TILE, (j + 1) * TILE)
                s = product_transposed(q, k_ref[keys, :]) * scale
                e = jnp.where(allowed_tile(start_ref, i * TILE, j * TILE), jnp.exp(s), 0.0)
                total = total + jnp.sum(e, axis=1, keepdims=True)
                out = out + plain_times(e.astype(BF), v_ref[keys, :])
            att_ref[rows, lanes] = (out / total).astype(BF)
            log_ref[rows, lanes] = jnp.broadcast_to(jnp.log(total), (TILE, LANES))

    @pl.loop(0, seq // TILE)
    def project_out(i):
        at = pl.ds(pl.multiple_of(i * TILE, TILE), TILE)
        part_ref[at, :] = plain_times(att_ref[at, :], pad_ref[width:, :]).astype(BF)

    reduce = Reduce(part_ref, chips, own_rows, scratch[10:17])
    line.relay(1)
    reduce.exchange()
    line.relay(1)
    dy_gather.pass_on()
    line.relay(1)
    reduce.arrive()

    @pl.loop(0, own_rows // CHUNK)
    def finish(k):
        at = chunk_rows(k)
        middle = x_ref[at, :].astype(F32) + reduce.total(k)
        middle_ref[at, :] = middle
        hidden[at, :] = (middle * rms_scale(middle) * (1.0 + gain_ref[...])).astype(BF)

    gather = Gather(hidden, h2_full, chips, scratch[17:22])
    line.relay(2)
    gather.pass_on()
    line.relay()
    gather.finish()
    dy_gather.finish()
    reduce.drain()
    line.finish()


def forward_step(h_full, w_col, cosine, sine, starts, x_own, gain_row, dy_own, ffn_shard, heads, columns, layers):
    seq, width = h_full.shape
    rows = x_own.shape[0]
    chips = columns // 2
    return pl.pallas_call(
        functools.partial(forward_kernel, columns, layers, heads),
        out_shape=(
            jax.ShapeDtypeStruct((seq, heads * LANES), BF),
            jax.ShapeDtypeStruct((seq, LANES), BF),
            jax.ShapeDtypeStruct((seq, LANES), BF),
            jax.ShapeDtypeStruct((seq, heads * LANES), BF),
            jax.ShapeDtypeStruct((seq, heads * LANES), F32),
            jax.ShapeDtypeStruct(((2 * heads + 2) * LANES, width), BF),
            jax.ShapeDtypeStruct((rows, width), F32),
            jax.ShapeDtypeStruct((seq, width), BF),
            jax.ShapeDtypeStruct((seq, width), BF),
            jax.ShapeDtypeStruct((layers * ffn_shard.shape[0], width), BF),
        ),
        in_specs=vmem_specs(9),
        out_specs=tuple(vmem_specs(7) + [pl.BlockSpec(memory_space=pl.ANY)] * 3),
        scratch_shapes=[
            pltpu.VMEM((seq, width), BF),
            pltpu.VMEM((rows, width), BF),
            *LineGather.scratch(layers, 3),
            *Gather.scratch(chips),
            *Reduce.scratch(chips, rows, width),
            *Gather.scratch(chips),
        ],
        compiler_params=comm_params(3),
        name="forward_step",
        cost_estimate=pl.CostEstimate(flops=6_000_000_000, bytes_accessed=150_000_000, transcendentals=2_000_000),
    )(h_full, w_col, cosine, sine, starts, x_own, gain_row, dy_own, ffn_shard)


def backward_kernel(columns, layers, heads, *refs):
    (part_back, part_out, term, middle_ref, dy_ref, gain_ref, pad_ref), refs = refs[:7], refs[7:]
    (cos_ref, sin_ref, start_ref, q_ref, k_ref, v_ref, att_ref, log_ref), refs = refs[:8], refs[8:]
    (out_ref, block_out_ref, grad_ref, sums_ref, gm_full, ffn_sum), refs = refs[:6], refs[6:]
    (grad_bf, ga_ref, dk_ref, dv_ref), scratch = refs[:4], refs[4:]
    seq, own_rows, chips = gm_full.shape[0], middle_ref.shape[0], columns // 2
    greet(columns, layers)
    back = Reduce(part_back, chips, own_rows, scratch[0:7])
    line = LineReduce(term, layers, 3, scratch[7:13])
    sums_ref[...] = jnp.zeros_like(sums_ref)
    back.exchange()
    out = Reduce(part_out, chips, own_rows, scratch[13:20])
    line.relay(1)
    back.arrive()

    @pl.loop(0, own_rows // CHUNK)
    def turn(k):
        at = chunk_rows(k)
        grad_hidden = back.total(k)
        middle = middle_ref[at, :]
        scale = rms_scale(middle)
        normed = middle * scale
        sums_ref[0:1, :] += jnp.sum(grad_hidden * normed, axis=0, keepdims=True)
        grad = dy_ref[at, :].astype(F32) + norm_backward(grad_hidden, normed, scale, gain_ref[...])
        grad_ref[at, :] = grad
        grad_bf[at, :] = grad.astype(BF)

    gather = Gather(grad_bf, gm_full, chips, scratch[20:25])
    line.relay(2)
    out.exchange()
    gather.pass_on()
    line.relay(1)
    gather.finish()
    line.relay(1)

    scale = HEAD_SIZE**-0.5
    width = (heads + 2) * LANES

    @pl.loop(0, seq // TILE)
    def attended_gradient(i):
        at = pl.ds(pl.multiple_of(i * TILE, TILE), TILE)
        ga_ref[at, :] = product_transposed(gm_full[at, :], pad_ref[width:, :]).astype(BF)

    dk_ref[...] = jnp.zeros_like(dk_ref)
    dv_ref[...] = jnp.zeros_like(dv_ref)
    low = lax.broadcasted_iota(jnp.int32, (TILE, LANES), 1) < HEAD_SIZE // 2

    def turn_back(u, rows):
        return (u * cos_ref[rows, :] - turned(u, low) * sin_ref[rows, :]).astype(BF)

    for i in range(seq // TILE):
        rows = slice(i * TILE, (i + 1) * TILE)
        for head in range(heads):
            lanes = slice(head * LANES, (head + 1) * LANES)
            q = q_ref[rows, lanes]
            ga = ga_ref[rows, lanes]
            delta = jnp.sum(ga.astype(F32) * att_ref[rows, lanes].astype(F32), axis=1, keepdims=True)
            logs = log_ref[rows, head * LANES : head * LANES + 1]
            dq = jnp.zeros((TILE, LANES), F32)
            for j in range(i + 1):
                keys = slice(j * TILE, (j + 1) * TILE)
                s = product_transposed(q, k_ref[keys, :]) * scale
                p = jnp.where(allowed_tile(start_ref, i * TILE, j * TILE), jnp.exp(s - logs), 0.0)
                dp = product_transposed(ga, v_ref[keys, :])
                ds = (p * (dp - delta) * scale).astype(BF)
                dq = dq + plain_times(ds, k_ref[keys, :])
                dk_ref[keys, :] += transposed_times(ds, q)
                dv_ref[keys, :] += transposed_times(p.astype(BF), ga)
            out_ref[rows, lanes] = turn_back(dq, rows)
    for i in range(seq // TILE):
        rows = slice(i * TILE, (i + 1) * TILE)
        out_ref[rows, heads * LANES : (heads + 1) * LANES] = turn_back(dk_ref[rows, :], rows)
        out_ref[rows, (heads + 1) * LANES :] = dv_ref[rows, :].astype(BF)
    line.relay(2)
    out.arrive()

    @pl.loop(0, own_rows // CHUNK)
    def finish_out(k):
        at = chunk_rows(k)
        block_out_ref[at, :] = middle_ref[at, :] + out.total(k)

    line.finish(ffn_sum)
    line.drain()
    back.drain()
    out.drain()


def backward_step(
    part_back, part_out, term, middle, dy_own, gain_row, padded, tables, saved, heads, columns, layers
):
    seq, width = part_back.shape
    rows = seq // columns
    chips = columns // 2
    ffn_rows = term.shape[0] // layers
    return pl.pallas_call(
        functools.partial(backward_kernel, columns, layers, heads),
        out_shape=(
            jax.ShapeDtypeStruct((seq, (heads + 2) * LANES), BF),
            jax.ShapeDtypeStruct((rows, width), F32),
            jax.ShapeDtypeStruct((rows, width), F32),
            jax.ShapeDtypeStruct((8, width), F32),
            jax.ShapeDtypeStruct((seq, width), BF),
            jax.ShapeDtypeStruct((ffn_rows, width), BF),
        ),
        in_specs=vmem_specs(15),
        out_specs=tuple(vmem_specs(6)),
        scratch_shapes=[
            pltpu.VMEM((rows, width), BF),
            pltpu.VMEM((seq, heads * LANES), BF),
            pltpu.VMEM((seq, LANES), F32),
            pltpu.VMEM((seq, LANES), F32),
            *Reduce.scratch(chips, rows, width),
            *LineReduce.scratch(layers, 3, ffn_rows, width),
            *Reduce.scratch(chips, rows, width),
            *Gather.scratch(chips),
        ],
        compiler_params=comm_params(4),
        name="backward_step",
        cost_estimate=pl.CostEstimate(flops=8_000_000_000, bytes_accessed=150_000_000, transcendentals=2_000_000),
    )(part_back, part_out, term, middle, dy_own, gain_row, padded, *tables, *saved)


def update_rows(g_ref, p_ref, m_ref, grad_ref, new_p_ref, new_m_ref):
    gradient = g_ref[...].astype(F32)
    grad_ref[...] = gradient
    parameter = p_ref[...]
    first_moment = BETA_ONE * m_ref[0] + (1.0 - BETA_ONE) * gradient
    second_moment = BETA_TWO * m_ref[1] + (1.0 - BETA_TWO) * gradient * gradient
    new_m_ref[0] = first_moment
    new_m_ref[1] = second_moment
    below = jnp.sqrt(second_moment * (1.0 / (1.0 - BETA_TWO**STEP))) + ADAM_EPS
    step = first_moment * (LEARN_RATE / (1.0 - BETA_ONE**STEP)) / below
    new_p_ref[...] = parameter * (1.0 - LEARN_RATE * WEIGHT_DECAY) - step


def update_kernel(steps, *refs):
    first = pl.program_id(0) < steps

    @pl.when(first)
    def one():
        update_rows(*refs[0:3], *refs[6:9])

    @pl.when(jnp.logical_not(first))
    def other():
        update_rows(*refs[3:6], *refs[9:12])


def update_all(first, second):
    specs, shapes = [], []
    blocks = []
    for gradient, parameter, _ in (first, second):
        rows = parameter.shape[0]
        whole = [n for n in (48, 32) if rows % n == 0]
        blocks.append(whole[0] if whole else rows)
    steps = first[1].shape[0] // blocks[0]
    rest = second[1].shape[0] // blocks[1]
    for block, place, (_, parameter, _) in (
        (blocks[0], lambda i: jnp.minimum(i, steps - 1), first),
        (blocks[1], lambda i: jnp.maximum(i - steps, 0), second),
    ):
        rows, width = parameter.shape
        flat = pl.BlockSpec((block, width), lambda i, place=place: (place(i), 0))
        pair = pl.BlockSpec((2, block, width), lambda i, place=place: (0, place(i), 0))
        specs.append([flat, flat, pair])
        shapes += [
            jax.ShapeDtypeStruct((rows, width), F32),
            jax.ShapeDtypeStruct((rows, width), F32),
            jax.ShapeDtypeStruct((2, rows, width), F32),
        ]
    out = pl.pallas_call(
        functools.partial(update_kernel, steps),
        grid=(steps + rest,),
        out_shape=tuple(shapes),
        in_specs=specs[0] + specs[1],
        out_specs=tuple(specs[0] + specs[1]),
        compiler_params=pltpu.CompilerParams(vmem_limit_bytes=VMEM_LIMIT),
        name="update_all",
        cost_estimate=pl.CostEstimate(flops=20_000_000, bytes_accessed=25_000_000, transcendentals=1_000_000),
    )(*first, *second)
    return out[:3], out[3:]


def rope_tables(positions):
    half_width = HEAD_SIZE // 2
    frequency = ROPE_THETA ** (-2.0 * jnp.arange(half_width, dtype=F32) / HEAD_SIZE)
    angles = positions.astype(F32)[:, None] * frequency[None, :]
    cosine, sine = jnp.cos(angles), jnp.sin(angles)
    blank = jnp.zeros((positions.shape[0], LANES - HEAD_SIZE), F32)
    return (
        jnp.concatenate([cosine, cosine, blank], axis=1),
        jnp.concatenate([-sine, sine, blank], axis=1),
    )


def unpadded(rows, count):
    return jnp.concatenate([rows[k * LANES : k * LANES + HEAD_SIZE] for k in range(count)])


def on_device(
    block_input,
    cotangent,
    documents,
    attn_weights,
    ffn_weights,
    norm_gains,
    attn_moments,
    ffn_moments,
    gain_moments,
):
    layers, columns = lax.axis_size("fsdp"), lax.axis_size("context")
    rows, width = block_input.shape[1:]
    seq = rows * columns
    heads = QUERY_HEADS // columns
    sharers = max(1, columns // KEY_VALUE_HEADS)
    share = KEY_VALUE_HEADS * HEAD_SIZE // columns
    hidden = ffn_weights.shape[0] * layers // 3
    grad_factor = float(rows * layers * columns) ** (-0.5)
    attn_plan, ffn_plan = unit_plans(layers, columns, attn_weights.shape[0] * layers * columns)
    core = lax.rem(lax.axis_index("context"), 2)
    swap = [(c, c + 1 - 2 * (c % 2)) for c in range(columns)]

    x_own, dy_own = block_input[0], cotangent[0]
    aligned = attn_weights.shape[0] % (3 * CHUNK) == 0 and layers > 1
    if aligned:
        h_full, docs_full, attn_col, ffn_shard = open_step(
            x_own, norm_gains[0:1], documents, attn_weights, ffn_weights, columns, layers
        )
    else:
        residual = x_own.astype(F32)
        first_hidden = (residual * rms_scale(residual) * (1.0 + norm_gains[0])).astype(BF)
        h_full, docs_full = gather_docs(first_hidden, documents, columns)
        attn_col = lax.all_gather(
            attn_plan.spread(attn_weights.astype(BF)), "fsdp", axis=0, tiled=True
        )
        ffn_shard = ffn_plan.spread(ffn_weights.astype(BF))
    query_rows = heads * HEAD_SIZE
    if sharers > 1:
        own_part = attn_col[query_rows : query_rows + 2 * share]
        other = lax.ppermute(own_part, "context", swap)

        def whole_head(first):
            mine, theirs = own_part[first : first + share], other[first : first + share]
            return jnp.where(
                core == 0, jnp.concatenate([mine, theirs]), jnp.concatenate([theirs, mine])
            )

        attn_col = jnp.concatenate(
            [
                attn_col[:query_rows],
                whole_head(0),
                whole_head(share),
                attn_col[query_rows + 2 * share :],
            ]
        )

    all_docs = docs_full.reshape(seq)
    starts = jnp.sum((all_docs[None, :] < all_docs[:, None]).astype(jnp.int32), axis=1)
    cosine, sine = rope_tables(jnp.arange(seq, dtype=jnp.int32) - starts)
    start_lanes = jnp.broadcast_to(starts[:, None], (seq, LANES))
    tables = (cosine, sine, start_lanes)
    *saved, padded, middle, h2_full, dy_full, ffn_col = forward_step(
        h_full, attn_col, *tables, x_own, norm_gains[1:2], dy_own, ffn_shard, heads, columns, layers
    )
    attended = saved[3]
    w_gate, w_up, w_down = ffn_col[:hidden], ffn_col[hidden : 2 * hidden], ffn_col[2 * hidden :]

    gate_pre = product_transposed(h2_full, w_gate)
    up_pre = product_transposed(h2_full, w_up)
    sigmoid_gate = jax.nn.sigmoid(gate_pre)
    activated = (gate_pre * sigmoid_gate * up_pre).astype(BF)
    grad_act = product_transposed(dy_full, w_down)
    grad_gate = (grad_act * up_pre * sigmoid_gate * (1.0 + gate_pre * (1.0 - sigmoid_gate))).astype(BF)
    grad_up = (grad_act * gate_pre * sigmoid_gate).astype(BF)
    ffn_term = jnp.concatenate(
        [
            (transposed_times(grad_gate, h2_full) * grad_factor).astype(BF),
            (transposed_times(grad_up, h2_full) * grad_factor).astype(BF),
            (transposed_times(activated, dy_full) * grad_factor).astype(BF),
        ]
    )
    out_part = plain_times(activated, w_down).astype(BF)
    back_part = (plain_times(grad_gate, w_gate) + plain_times(grad_up, w_up)).astype(BF)

    grads, block_out, grad_middle, sums, gm_full, ffn_sum = backward_step(
        back_part,
        out_part,
        ffn_term,
        middle,
        dy_own,
        norm_gains[1:2],
        padded,
        tables,
        saved,
        heads,
        columns,
        layers,
    )
    if sharers > 1:
        shared = grads[:, heads * LANES :]
        shared = (shared.astype(F32) + lax.ppermute(shared, "context", swap).astype(F32)).astype(BF)
        lane = jnp.arange(2 * LANES, dtype=jnp.int32) % LANES // share
        grads = jnp.concatenate(
            [grads[:, : heads * LANES], jnp.where(lane == core, shared, jnp.zeros_like(shared))], axis=1
        )
    term_in = (transposed_times(grads, h_full) * grad_factor).astype(BF)
    term_out = (transposed_times(attended, gm_full) * grad_factor).astype(BF)
    if sharers > 1:
        own_rows = [
            lax.dynamic_slice_in_dim(term_in, (heads + k) * LANES + core * share, share, 0)
            for k in range(2)
        ]
        attn_term = jnp.concatenate(
            [unpadded(term_in, heads), *own_rows, unpadded(term_out, heads)]
        )
    else:
        attn_term = jnp.concatenate([unpadded(term_in, heads + 2), unpadded(term_out, heads)])
    in_part = plain_times(grads, padded[: (heads + 2) * LANES]).astype(BF)
    last_args = (in_part, x_own, grad_middle, norm_gains[0:1], sums, columns, layers)
    if aligned:
        grad_input, gain_sums, attn_shard, ffn_shard = last_step(*last_args, (attn_term, ffn_sum))
    else:
        attn_sum = lax.psum_scatter(attn_term, "fsdp", scatter_dimension=0, tiled=True)
        grad_input, gain_sums = last_step(*last_args)
        ffn_shard = ffn_plan.collect(ffn_sum)
        attn_shard = attn_plan.collect(attn_sum)

    column_count = width // (layers * columns)
    first_column = lax.axis_index(EVERY) * column_count
    gain_shard = lax.dynamic_slice_in_dim(gain_sums[:2], first_column, column_count, 1) * grad_factor
    own_gains = lax.dynamic_slice_in_dim(norm_gains, first_column, column_count, 1)
    (ffn_shard, new_ffn, ffn_states), (attn_shard, new_attn, attn_states) = update_all(
        (ffn_shard, ffn_weights, ffn_moments), (attn_shard, attn_weights, attn_moments)
    )
    new_gains, gain_states = adamw_update(own_gains, gain_shard, gain_moments, 0.0)
    return (
        block_out[None],
        grad_input[None],
        attn_shard,
        ffn_shard,
        gain_shard,
        new_attn,
        new_ffn,
        new_gains,
        attn_states,
        ffn_states,
        jnp.stack(gain_states),
    )


def solution(mesh):
    placed = (
        P("fsdp", "context", None),
        P("fsdp", "context", None),
        P("fsdp", "context"),
        P(EVERY, None),
        P(EVERY, None),
        P(),
        P(None, EVERY, None),
        P(None, EVERY, None),
        P(None, None, EVERY),
    )
    return jax.shard_map(
        on_device,
        mesh=mesh,
        in_specs=placed,
        out_specs=(
            P("fsdp", "context", None),
            P("fsdp", "context", None),
            P(EVERY, None),
            P(EVERY, None),
            P(None, EVERY),
            P(EVERY, None),
            P(EVERY, None),
            P(None, EVERY),
            P(None, EVERY, None),
            P(None, EVERY, None),
            P(None, None, EVERY),
        ),
        check_vma=False,
    )
```

```python
import functools

import jax
import jax.numpy as jnp
import numpy as np
from jax import lax
from jax.experimental import pallas as pl
from jax.experimental.pallas import tpu as pltpu
from jax.sharding import PartitionSpec as P

QUERY_HEADS = 16
KEY_VALUE_HEADS = 8
HEAD_SIZE = 96
STEP = 3

NORM_EPS = 1e-05
ROPE_THETA = 100000.0
BETA_ONE = 0.9
BETA_TWO = 0.95
ADAM_EPS = 1e-08
LEARN_RATE = 0.02
WEIGHT_DECAY = 0.1

LANES = 128
TILE = 256
CHUNK = 16
VMEM_LIMIT = 67_000_000
EVERY = ("fsdp", "context")
BF = jnp.bfloat16
F32 = jnp.float32
ID_TYPE = pl.DeviceIdType.MESH


def product_transposed(left_matrix, right_matrix):
    return lax.dot_general(
        left_matrix, right_matrix, (((1,), (1,)), ((), ())), preferred_element_type=F32
    )


def transposed_times(left_matrix, right_matrix):
    return lax.dot_general(
        left_matrix, right_matrix, (((0,), (0,)), ((), ())), preferred_element_type=F32
    )


def plain_times(left_matrix, right_matrix):
    return jnp.dot(left_matrix, right_matrix, preferred_element_type=F32)


def rms_scale(tensor_in):
    return lax.rsqrt(jnp.mean(tensor_in * tensor_in, axis=-1, keepdims=True) + NORM_EPS)


def norm_backward(grad_in, normed, norm_scale, gain_row):
    scaled = grad_in * (1.0 + gain_row)
    return norm_scale * (scaled - normed * jnp.mean(scaled * normed, axis=-1, keepdims=True))


def adamw_update(parameter, gradient, moments, decay_rate):
    first_moment = BETA_ONE * moments[0] + (1.0 - BETA_ONE) * gradient
    second_moment = BETA_TWO * moments[1] + (1.0 - BETA_TWO) * gradient * gradient
    first_hat = first_moment / (1.0 - BETA_ONE**STEP)
    second_hat = second_moment / (1.0 - BETA_TWO**STEP)
    updated = parameter - LEARN_RATE * (
        first_hat / (jnp.sqrt(second_hat) + ADAM_EPS) + decay_rate * parameter
    )
    return (updated, (first_moment, second_moment))


class UnitPlan:
    def __init__(self, homes, devices):
        waiting = [[] for _ in range(devices)]
        for unit, (device, place) in enumerate(homes):
            waiting[unit // 3].append((unit % 3, device, place))
        self.rounds = []
        for _ in range(3):
            taken = [None] * devices

            def settle(source, seen):
                for piece, device, place in waiting[source]:
                    if device in seen:
                        continue
                    seen.add(device)
                    if taken[device] is None or settle(taken[device][0], seen):
                        taken[device] = (source, piece, place)
                        return True
                return False

            for source in range(devices):
                if not settle(source, set()):
                    raise ValueError("no matching")
            pairs, pieces, places = [], [0] * devices, [0] * devices
            for device, (source, piece, place) in enumerate(taken):
                pairs.append((source, device))
                pieces[source] = piece
                places[device] = place
                waiting[source].remove((piece, device, place))
            self.rounds.append((pairs, np.array(pieces), np.array(places)))

    def _reorder(self, got, columns):
        order = np.argsort(np.stack(columns, axis=1), axis=1).astype(np.int32)
        mine = jnp.asarray(order)[lax.axis_index(EVERY)]
        stacked = jnp.stack(got)
        return jnp.concatenate(
            [lax.dynamic_index_in_dim(stacked, mine[k], 0, keepdims=False) for k in range(3)]
        )

    def spread(self, rows):
        pieces = rows.reshape(3, rows.shape[0] // 3, rows.shape[1])
        me = lax.axis_index(EVERY)
        got = []
        for pairs, piece, _ in self.rounds:
            unit = lax.dynamic_index_in_dim(
                pieces, jnp.asarray(piece, jnp.int32)[me], 0, keepdims=False
            )
            got.append(lax.ppermute(unit, EVERY, pairs))
        return self._reorder(got, [place for _, _, place in self.rounds])

    def collect(self, rows):
        places_of = rows.reshape(3, rows.shape[0] // 3, rows.shape[1])
        me = lax.axis_index(EVERY)
        got = []
        for pairs, _, place in self.rounds:
            unit = lax.dynamic_index_in_dim(
                places_of, jnp.asarray(place, jnp.int32)[me], 0, keepdims=False
            )
            got.append(lax.ppermute(unit, EVERY, [(b, a) for a, b in pairs]))
        return self._reorder(got, [piece for _, piece, _ in self.rounds])


def unit_plans(layers, columns, attn_rows):
    devices = layers * columns

    def home(column, position):
        return ((position // 3) * columns + column, position % 3)

    homes = []
    for unit in range(3 * devices):
        matrix, rest = divmod(unit, devices)
        stretch, column = divmod(rest, columns)
        homes.append(home(column, matrix * layers + stretch))
    ffn_plan = UnitPlan(homes, devices)
    unit_rows = attn_rows // (3 * devices)
    query_units = QUERY_HEADS * HEAD_SIZE // columns // unit_rows
    share_units = KEY_VALUE_HEADS * HEAD_SIZE // columns // unit_rows
    homes = []
    position = 0
    for count in (query_units, share_units, share_units, query_units):
        for column in range(columns):
            for k in range(count):
                homes.append(home(column, position + k))
        position += count
    return UnitPlan(homes, devices), ffn_plan


class Homes:
    def __init__(self, layers, columns, attn_rows):
        devices = layers * columns
        unit_rows = attn_rows // (3 * devices)
        self.layers, self.columns = layers, columns
        self.counts = [
            QUERY_HEADS * HEAD_SIZE // columns // unit_rows,
            KEY_VALUE_HEADS * HEAD_SIZE // columns // unit_rows,
        ]
        query, share = self.counts
        self.first = [0, query, query + share, query + 2 * share]
        self.sizes = [query, share, share, query]

    def _spot(self, column, position):
        return position // 3, column, position % 3

    def _column(self, group):
        half = self.columns // 2
        return group % half * 2 + group // half

    def _group(self, column):
        return column % 2 * (self.columns // 2) + column // 2

    def attn_targets(self):
        device = lax.axis_index("fsdp") * self.columns + lax.axis_index("context")
        found = []
        for piece in range(3):
            unit = device * 3 + piece
            column, position = 0, 0
            for first, size in zip(self.first, self.sizes):
                inside = unit - first * self.columns
                begun = inside >= 0
                column = jnp.where(begun, self._column(inside // size), column)
                position = jnp.where(begun, first + inside % size, position)
            found.append(self._spot(column, position))
        return found

    def attn_owners(self):
        group = self._group(lax.axis_index("context"))
        found = []
        for place in range(3):
            position = lax.axis_index("fsdp") * 3 + place
            unit = 0
            for first, size in zip(self.first, self.sizes):
                inside = position - first
                unit = jnp.where(inside >= 0, first * self.columns + group * size + inside, unit)
            device = unit // 3
            found.append((device // self.columns, device % self.columns, unit % 3))
        return found

    def ffn_targets(self):
        layer, column = lax.axis_index("fsdp"), lax.axis_index("context")
        return [
            (layer, (3 * column + piece) % self.columns, (3 * column + piece) // self.columns)
            for piece in range(3)
        ]

    def ffn_owners(self):
        layer, column = lax.axis_index("fsdp"), lax.axis_index("context")
        return [
            (layer, (place * self.columns + column) // 3, (place * self.columns + column) % 3)
            for place in range(3)
        ]


def partner(me, step, chips):
    return lax.rem(me // 2 + step, chips) * 2 + lax.rem(me, 2)


def sibling_of(me):
    return me + 1 - 2 * lax.rem(me, 2)


def rows_at(index, rows):
    return pl.ds(pl.multiple_of(index * rows, rows), rows)


def greet(columns, layers=1, others=()):
    barrier = pltpu.get_barrier_semaphore()
    me = lax.axis_index("context")
    awaited = columns - 1 + layers - 1
    for layer, column in others:
        apart = (layer != lax.axis_index("fsdp")) | (column != me)
        awaited = awaited + jnp.where(apart, 1, 0)

        @pl.when(apart)
        def there():
            pl.semaphore_signal(
                barrier, inc=1, device_id={"fsdp": layer, "context": column}, device_id_type=ID_TYPE
            )

    for step in range(1, columns):
        pl.semaphore_signal(
            barrier, inc=1, device_id={"context": lax.rem(me + step, columns)}, device_id_type=ID_TYPE
        )
    if layers > 1:
        layer = lax.axis_index("fsdp")
        for step in range(1, layers):
            pl.semaphore_signal(
                barrier, inc=1, device_id={"fsdp": lax.rem(layer + step, layers)}, device_id_type=ID_TYPE
            )
    pl.semaphore_wait(barrier, awaited)


def send(source, target, send_sem, recv_sem, device):
    copy = pltpu.make_async_remote_copy(
        src_ref=source,
        dst_ref=target,
        send_sem=send_sem,
        recv_sem=recv_sem,
        device_id=device,
        device_id_type=ID_TYPE,
    )
    copy.start()
    return copy


def remote(source, target, send_sem, recv_sem, device):
    return pltpu.make_async_remote_copy(
        src_ref=source,
        dst_ref=target,
        send_sem=send_sem,
        recv_sem=recv_sem,
        device_id=device,
        device_id_type=ID_TYPE,
    )


class Exchange:
    @staticmethod
    def scratch():
        return [pltpu.SemaphoreType.DMA((3,)), pltpu.SemaphoreType.DMA((3,))]

    def __init__(self, sources, targets, homes, sems):
        send_sem, recv_sem = sems
        self.parts = []
        for i, (layer, column, place) in enumerate(homes):
            itself = (layer == lax.axis_index("fsdp")) & (column == lax.axis_index("context"))
            target = targets(layer, place)
            copy = functools.partial(
                remote,
                sources[i],
                target,
                send_sem.at[i],
                recv_sem.at[place],
                {"fsdp": layer, "context": column},
            )
            stay = functools.partial(pltpu.make_async_copy, sources[i], target, recv_sem.at[place])

            @pl.when(itself)
            def here():
                stay().start()

            @pl.when(jnp.logical_not(itself))
            def there():
                copy().start()

            self.parts.append((itself, copy))
        self.landing = [
            functools.partial(pltpu.make_async_copy, sources[k], sources[k], recv_sem.at[k])
            for k in range(3)
        ]

    def arrive(self):
        for landed in self.landing:
            landed().wait()

    def drain(self):
        for itself, copy in self.parts:

            @pl.when(jnp.logical_not(itself))
            def sent():
                copy().wait_send()


class LineGather:
    @staticmethod
    def scratch(layers, pieces):
        return [*[pltpu.SemaphoreType.DMA(((layers - 1) * pieces,))] * 4, pltpu.SemaphoreType.DMA]

    def __init__(self, full, own, layers, pieces, sems):
        self.full, self.own, self.layers, self.pieces = full, own, layers, pieces
        *self.sems, local_sem = sems
        self.rows = own.shape[0]
        self.size = self.rows // pieces
        self.count = (layers - 1) * pieces
        self.local = pltpu.make_async_copy(
            own, full.at[rows_at(lax.axis_index("fsdp"), self.rows), :], local_sem
        )
        for m in range(pieces):
            self._send(m)
        self.local.start()
        self.next = pieces

    def _block(self, shard, piece):
        first = pl.multiple_of(shard * self.rows + piece * self.size, self.size)
        return self.full.at[pl.ds(first, self.size), :]

    def _moves(self, m):
        k, piece = divmod(m, self.pieces)
        layer = lax.axis_index("fsdp")
        up_send, up_recv, down_send, down_recv = self.sems
        top = self.layers - 1
        for first, last, other, shard, send_sem, recv_sem in (
            (layer - k >= 0, layer < top, layer + 1, layer - k, up_send, up_recv),
            (layer + k <= top, layer > 0, layer - 1, layer + k, down_send, down_recv),
        ):
            block = self._block(shard, piece)
            source = self.own.at[pl.ds(piece * self.size, self.size), :] if k == 0 else block
            yield first & last, functools.partial(
                remote, source, block, send_sem.at[m], recv_sem.at[m], {"fsdp": other}
            )

    def _send(self, m):
        for go, copy in self._moves(m):

            @pl.when(go)
            def start():
                copy().start()

    def _land(self, m):
        k, piece = divmod(m, self.pieces)
        layer = lax.axis_index("fsdp")
        _, up_recv, _, down_recv = self.sems
        for there, shard, recv_sem in (
            (layer - 1 - k >= 0, layer - 1 - k, up_recv),
            (layer + 1 + k <= self.layers - 1, layer + 1 + k, down_recv),
        ):
            block = self._block(shard, piece)
            copy = functools.partial(pltpu.make_async_copy, block, block, recv_sem.at[m])

            @pl.when(there)
            def landed():
                copy().wait()

    def relay(self, count=None):
        stop = self.count if count is None else min(self.count, self.next + count)
        for m in range(self.next, stop):
            self._land(m - self.pieces)
            self._send(m)
        self.next = stop

    def finish(self):
        self.relay()
        for m in range(self.count - self.pieces, self.count):
            self._land(m)
        for m in range(self.count):
            for go, copy in self._moves(m):

                @pl.when(go)
                def sent():
                    copy().wait_send()

        self.local.wait()


class LineReduce:
    @staticmethod
    def scratch(layers, pieces, rows, width):
        count = (layers - 1) * pieces
        return [
            pltpu.VMEM((count, rows // pieces, width), BF),
            pltpu.VMEM((count, rows // pieces, width), BF),
            *[pltpu.SemaphoreType.DMA((count,))] * 4,
        ]

    def __init__(self, term, layers, pieces, scratch):
        self.term, self.layers, self.pieces = term, layers, pieces
        self.rows = term.shape[0] // layers
        self.size = self.rows // pieces
        self.up_in, self.down_in, *self.sems = scratch
        self.count = (layers - 1) * pieces
        self.slots = self.count + layers - 1
        self.next = 1
        layer = lax.axis_index("fsdp")
        top = layers - 1

        @pl.when(layer == 0)
        def bottom():
            for m in range(self.count):
                self._up(m, self._block(top - m // pieces, m % pieces)).start()

        @pl.when(layer == top)
        def ceiling():
            for m in range(self.count):
                self._down(m, self._block(m // pieces, m % pieces)).start()

    def _block(self, target, piece):
        return self.term.at[pl.ds(target * self.rows + piece * self.size, self.size), :]

    def _up(self, m, source):
        up_send, up_recv, _, _ = self.sems
        other = {"fsdp": lax.axis_index("fsdp") + 1}
        return remote(source, self.up_in.at[m], up_send.at[m], up_recv.at[m], other)

    def _down(self, m, source):
        _, _, down_send, down_recv = self.sems
        other = {"fsdp": lax.axis_index("fsdp") - 1}
        return remote(source, self.down_in.at[m], down_send.at[m], down_recv.at[m], other)

    def _add(self, sums, m, target):
        first = pl.multiple_of(target * self.rows + m % self.pieces * self.size, CHUNK)

        @pl.loop(0, self.size // CHUNK)
        def add(c):
            at = chunk_rows(c)
            of_term = pl.ds(pl.multiple_of(first + c * CHUNK, CHUNK), CHUNK)
            sums[m, at, :] = (
                sums[m, at, :].astype(F32) + self.term[of_term, :].astype(F32)
            ).astype(BF)

    def _slot(self, slot):
        layer = lax.axis_index("fsdp")
        top = self.layers - 1
        _, up_recv, _, down_recv = self.sems
        m = slot - layer
        target = top - m // self.pieces

        @pl.when((layer > 0) & (m >= 0) & (m < self.count) & (layer <= target))
        def from_below():
            pltpu.make_async_copy(self.up_in.at[m], self.up_in.at[m], up_recv.at[m]).wait()

            @pl.when(layer < target)
            def pass_up():
                self._add(self.up_in, m, target)
                self._up(m, self.up_in.at[m]).start()

        n = slot - (top - layer)
        goal = n // self.pieces

        @pl.when((layer < top) & (n >= 0) & (n < self.count) & (layer >= goal))
        def from_above():
            pltpu.make_async_copy(self.down_in.at[n], self.down_in.at[n], down_recv.at[n]).wait()

            @pl.when(layer > goal)
            def pass_down():
                self._add(self.down_in, n, goal)
                self._down(n, self.down_in.at[n]).start()

    def relay(self, count=None):
        stop = self.slots if count is None else min(self.slots, self.next + count)
        if stop > self.next:

            @pl.loop(self.next, stop)
            def slots(slot):
                self._slot(slot)

        self.next = stop

    def finish(self, total):
        self.relay()
        layer = lax.axis_index("fsdp")
        top = self.layers - 1
        for own in range(self.layers):

            @pl.when(layer == own)
            def here():
                for piece in range(self.pieces):

                    @pl.loop(0, self.size // CHUNK)
                    def add(c):
                        start = pl.multiple_of(c * CHUNK, CHUNK)
                        at = pl.ds(start, CHUNK)
                        value = self.term[
                            pl.ds(own * self.rows + piece * self.size + start, CHUNK), :
                        ].astype(F32)
                        if own > 0:
                            m = (top - own) * self.pieces + piece
                            value = value + self.up_in[m, at, :].astype(F32)
                        if own < top:
                            m = own * self.pieces + piece
                            value = value + self.down_in[m, at, :].astype(F32)
                        total[pl.ds(piece * self.size + start, CHUNK), :] = value.astype(BF)

    def drain(self):
        layer = lax.axis_index("fsdp")
        top = self.layers - 1
        for m in range(self.count):
            k = m // self.pieces

            @pl.when(layer < top - k)
            def up():
                self._up(m, self.up_in.at[m]).wait_send()

            @pl.when(layer > k)
            def down():
                self._down(m, self.down_in.at[m]).wait_send()


class Gather:
    @staticmethod
    def scratch(chips):
        return [
            pltpu.SemaphoreType.DMA((chips,)),
            pltpu.SemaphoreType.DMA((chips,)),
            pltpu.SemaphoreType.DMA((chips,)),
            pltpu.SemaphoreType.DMA((chips,)),
            pltpu.SemaphoreType.DMA,
        ]

    def __init__(self, block, full, chips, sems):
        own_send, own_recv, self.on_send, self.on_recv, local_sem = sems
        me = lax.axis_index("context")
        rows = block.shape[0]
        self.block, self.full, self.chips, self.me, self.rows = block, full, chips, me, rows
        mine = full.at[rows_at(me, rows), :]
        self.own = [
            send(block, mine, own_send.at[step], own_recv.at[step], {"context": partner(me, step, chips)})
            for step in range(1, chips)
        ]
        self.own.append(
            send(block, mine, own_send.at[0], own_recv.at[0], {"context": sibling_of(me)})
        )
        self.local = pltpu.make_async_copy(block, mine, local_sem)
        self.local.start()

        self.passed = []

    def pass_on(self):
        for step in range(1, self.chips):
            self.own[step - 1].wait_recv()
            source = partner(self.me, self.chips - step, self.chips)
            there = self.full.at[rows_at(source, self.rows), :]
            self.passed.append(
                send(there, there, self.on_send.at[step], self.on_recv.at[step], {"context": sibling_of(self.me)})
            )

    def finish(self):
        if not self.passed:
            self.pass_on()
        self.own[-1].wait_recv()
        for copy in self.passed:
            copy.wait_recv()
        for copy in self.own + self.passed:
            copy.wait_send()
        self.local.wait()


class Reduce:
    @staticmethod
    def buffers(chips, rows, width):
        return [pltpu.VMEM((chips, rows, width), BF), pltpu.VMEM((chips - 1, rows, width), BF)]

    @staticmethod
    def semaphores(chips):
        return [pltpu.SemaphoreType.DMA((chips,))] * 4

    def __init__(self, part, chips, rows, buffers, semaphores):
        self.near, self.far = buffers
        near_send, near_recv, self.far_send, self.far_recv = semaphores
        me = lax.axis_index("context")
        self.part, self.chips, self.rows, self.me = part, chips, rows, me
        self.near_copies = {}
        for step in [*range(1, chips), 0]:
            block = partner(sibling_of(me), step, chips)
            self.near_copies[step] = send(
                part.at[rows_at(block, rows), :],
                self.near.at[step],
                near_send.at[step],
                near_recv.at[step],
                {"context": sibling_of(me)},
            )
        self.far_copies = []

    def exchange(self):
        for step in range(1, self.chips):
            self.near_copies[step].wait_recv()
            target = partner(self.me, step, self.chips)
            first = pl.multiple_of(target * self.rows, self.rows)

            @pl.loop(0, self.rows // CHUNK)
            def add(k):
                at = chunk_rows(k)
                from_part = pl.ds(pl.multiple_of(first + k * CHUNK, CHUNK), CHUNK)
                self.near[step, at, :] = (
                    self.part[from_part, :].astype(F32) + self.near[step, at, :].astype(F32)
                ).astype(BF)

            self.far_copies.append(
                send(
                    self.near.at[step],
                    self.far.at[step - 1],
                    self.far_send.at[step],
                    self.far_recv.at[step],
                    {"context": target},
                )
            )

    def arrive(self):
        self.near_copies[0].wait_recv()
        for copy in self.far_copies:
            copy.wait_recv()

    def total(self, k):
        at = chunk_rows(k)
        first = pl.multiple_of(self.me * self.rows, self.rows)
        value = self.part[pl.ds(pl.multiple_of(first + k * CHUNK, CHUNK), CHUNK), :].astype(F32)
        value = value + self.near[0, at, :].astype(F32)
        for step in range(1, self.chips):
            value = value + self.far[step - 1, at, :].astype(F32)
        return value

    def drain(self):
        for copy in list(self.near_copies.values()) + self.far_copies:
            copy.wait_send()


def chunk_rows(k):
    return pl.ds(pl.multiple_of(k * CHUNK, CHUNK), CHUNK)


def vmem_specs(count):
    return [pl.BlockSpec(memory_space=pltpu.VMEM)] * count


def comm_params(collective_id):
    return pltpu.CompilerParams(
        collective_id=collective_id, has_side_effects=True, vmem_limit_bytes=VMEM_LIMIT
    )


def place_rows(ref, unit, layer, place):
    return ref.at[rows_at(place, unit), :]


class Docs:
    @staticmethod
    def scratch(columns):
        return [
            pltpu.SemaphoreType.DMA((columns,)),
            pltpu.SemaphoreType.DMA((columns,)),
            pltpu.SemaphoreType.DMA,
        ]

    def __init__(self, docs, docs_full, columns, sems):
        docs_send, docs_recv, docs_local = sems
        me = lax.axis_index("context")
        mine = docs_full.at[pl.ds(me, 1), :]
        self.copies = [
            send(docs, mine, docs_send.at[step], docs_recv.at[step], {"context": lax.rem(me + step, columns)})
            for step in range(1, columns)
        ]
        self.local = pltpu.make_async_copy(docs, mine, docs_local)
        self.local.start()

    def finish(self):
        for copy in self.copies:
            copy.wait_recv()
        for copy in self.copies:
            copy.wait_send()
        self.local.wait()


def open_kernel(
    columns,
    layers,
    homes,
    x_ref,
    gain_ref,
    docs,
    attn_ref,
    ffn_ref,
    h_full,
    docs_full,
    attn_col,
    ffn_shard,
    hidden,
    attn_bf,
    ffn_bf,
    attn_shard,
    *scratch,
):
    attn_rows, ffn_rows = attn_ref.shape[0], ffn_ref.shape[0]

    @pl.loop(0, attn_rows // CHUNK)
    def cast_attn(k):
        attn_bf[chunk_rows(k), :] = attn_ref[chunk_rows(k), :].astype(BF)

    targets = homes.attn_targets()
    greet(columns, layers, [spot[:2] for spot in targets + homes.attn_owners()])
    unit = attn_rows // 3
    attn_spread = Exchange(
        [attn_bf.at[pl.ds(k * unit, unit), :] for k in range(3)],
        functools.partial(place_rows, attn_shard, unit),
        targets,
        scratch[0:2],
    )

    @pl.loop(0, x_ref.shape[0] // CHUNK)
    def norm(k):
        residual = x_ref[chunk_rows(k), :].astype(F32)
        hidden[chunk_rows(k), :] = (residual * rms_scale(residual) * (1.0 + gain_ref[...])).astype(BF)

    documents = Docs(docs, docs_full, columns, scratch[2:5])
    gather = Gather(hidden, h_full, columns // 2, scratch[5:10])

    @pl.loop(0, ffn_rows // CHUNK)
    def cast_ffn(k):
        ffn_bf[chunk_rows(k), :] = ffn_ref[chunk_rows(k), :].astype(BF)

    attn_spread.arrive()
    line = LineGather(attn_col, attn_shard, layers, 1, scratch[10:15])
    unit = ffn_rows // 3
    ffn_spread = Exchange(
        [ffn_bf.at[pl.ds(k * unit, unit), :] for k in range(3)],
        functools.partial(place_rows, ffn_shard, unit),
        homes.ffn_targets(),
        scratch[15:17],
    )
    line.relay(1)
    gather.pass_on()
    line.relay()
    documents.finish()
    gather.finish()
    ffn_spread.arrive()
    line.finish()
    attn_spread.drain()
    ffn_spread.drain()


def open_step(x_own, gain_row, docs, attn_weights, ffn_weights, columns, layers):
    rows, width = x_own.shape
    attn_rows, ffn_rows = attn_weights.shape[0], ffn_weights.shape[0]
    homes = Homes(layers, columns, attn_rows * layers * columns)
    return pl.pallas_call(
        functools.partial(open_kernel, columns, layers, homes),
        out_shape=(
            jax.ShapeDtypeStruct((columns * rows, width), BF),
            jax.ShapeDtypeStruct((columns, docs.shape[1]), jnp.int32),
            jax.ShapeDtypeStruct((layers * attn_rows, width), BF),
            jax.ShapeDtypeStruct((ffn_rows, width), BF),
        ),
        in_specs=vmem_specs(5),
        out_specs=tuple([pl.BlockSpec(memory_space=pl.ANY)] * 4),
        scratch_shapes=[
            pltpu.VMEM((rows, width), BF),
            pltpu.VMEM((attn_rows, width), BF),
            pltpu.VMEM((ffn_rows, width), BF),
            pltpu.VMEM((attn_rows, width), BF),
            *Exchange.scratch(),
            *Docs.scratch(columns),
            *Gather.scratch(columns // 2),
            *LineGather.scratch(layers, 1),
            *Exchange.scratch(),
        ],
        compiler_params=comm_params(1),
        name="open_step",
        cost_estimate=pl.CostEstimate(flops=0, bytes_accessed=150_000_000, transcendentals=0),
    )(x_own, gain_row, docs, attn_weights, ffn_weights)


def gather_docs_kernel(columns, block, docs, full, docs_full, *scratch):
    greet(columns)
    gather = Gather(block, full, columns // 2, scratch[:5])
    documents = Docs(docs, docs_full, columns, scratch[5:])
    gather.finish()
    documents.finish()


def gather_docs(block, docs, columns):
    rows, width = block.shape
    return pl.pallas_call(
        functools.partial(gather_docs_kernel, columns),
        out_shape=(
            jax.ShapeDtypeStruct((columns * rows, width), BF),
            jax.ShapeDtypeStruct((columns, docs.shape[1]), jnp.int32),
        ),
        in_specs=vmem_specs(2),
        out_specs=(pl.BlockSpec(memory_space=pl.ANY), pl.BlockSpec(memory_space=pl.ANY)),
        scratch_shapes=[*Gather.scratch(columns // 2), *Docs.scratch(columns)],
        compiler_params=comm_params(2),
        name="gather_docs",
        cost_estimate=pl.CostEstimate(flops=0, bytes_accessed=60_000_000, transcendentals=0),
    )(block, docs)


def last_kernel(columns, layers, homes, *refs):
    (part_in, x_ref, grad_ref, gain_ref, sums_ref), refs = refs[:5], refs[5:]
    if homes is not None:
        (term, ffn_sum), refs = refs[:2], refs[2:]
    (input_grad_ref, gains_ref), refs = refs[:2], refs[2:]
    if homes is not None:
        (attn_back, ffn_back), refs = refs[:2], refs[2:]
    (own_sums, plane_slots, plane_sums, line_slots), refs = refs[:4], refs[4:]
    (plane_send, plane_recv, line_send, line_recv), scratch = refs[:4], refs[4:]
    chips = columns // 2
    rows = x_ref.shape[0]
    if homes is None:
        greet(columns, layers)
    else:
        attn_owners = homes.attn_owners()
        greet(columns, layers, [spot[:2] for spot in homes.attn_targets() + attn_owners])
    first = Reduce(part_in, chips, rows, scratch[0:2], scratch[2:6])
    if homes is not None:
        attn_rows, ffn_rows = term.shape[0] // layers, ffn_sum.shape[0]
        attn_done = scratch[6]
        line = LineReduce(term, layers, 3, scratch[7:13])
        unit_ffn = ffn_rows // 3
    first.exchange()
    if homes is not None:
        ffn_owned = Exchange(
            [ffn_sum.at[pl.ds(k * unit_ffn, unit_ffn), :] for k in range(3)],
            functools.partial(place_rows, ffn_back, unit_ffn),
            homes.ffn_owners(),
            scratch[13:15],
        )
        line.relay(3)
    own_sums[...] = jnp.zeros_like(own_sums)
    own_sums[1:2, :] = sums_ref[0:1, :]
    if homes is not None:
        line.relay(3)
    first.arrive()

    @pl.loop(0, rows // CHUNK)
    def finish(k):
        at = chunk_rows(k)
        grad_hidden = first.total(k)
        residual = x_ref[at, :].astype(F32)
        scale = rms_scale(residual)
        normed = residual * scale
        own_sums[0:1, :] += jnp.sum(grad_hidden * normed, axis=0, keepdims=True)
        input_grad_ref[at, :] = grad_ref[at, :] + norm_backward(
            grad_hidden, normed, scale, gain_ref[...]
        )

    me = lax.axis_index("context")
    layer = lax.axis_index("fsdp")
    in_plane = [
        send(
            own_sums,
            plane_slots.at[step],
            plane_send.at[step],
            plane_recv.at[step],
            {"context": lax.rem(me + step, columns)},
        )
        for step in range(1, columns)
    ]
    if homes is not None:
        line.finish(attn_done)
        unit = attn_rows // 3
        attn_owned = Exchange(
            [attn_done.at[pl.ds(k * unit, unit), :] for k in range(3)],
            functools.partial(place_rows, attn_back, unit),
            attn_owners,
            scratch[15:17],
        )
    total = own_sums[...]
    for step, copy in enumerate(in_plane):
        copy.wait_recv()
        total = total + plane_slots[step + 1]
    plane_sums[...] = total
    in_line = [
        send(
            plane_sums,
            line_slots.at[step],
            line_send.at[step],
            line_recv.at[step],
            {"fsdp": lax.rem(layer + step, layers)},
        )
        for step in range(1, layers)
    ]
    for step, copy in enumerate(in_line):
        copy.wait_recv()
        total = total + line_slots[step + 1]
    gains_ref[...] = total
    if homes is not None:
        ffn_owned.arrive()
        attn_owned.arrive()
        ffn_owned.drain()
        attn_owned.drain()
        line.drain()
    for copy in in_plane + in_line:
        copy.wait_send()
    first.drain()


def last_step(part_in, x_own, grad_middle, gain_row, sums, columns, layers, weight_sums=()):
    rows, width = x_own.shape
    chips = columns // 2
    homes = None
    back_shapes, back_scratch = [], []
    if weight_sums:
        term, ffn_sum = weight_sums
        attn_rows = term.shape[0] // layers
        homes = Homes(layers, columns, attn_rows * layers * columns)
        back_shapes = [
            jax.ShapeDtypeStruct((attn_rows, width), BF),
            jax.ShapeDtypeStruct(ffn_sum.shape, BF),
        ]
        back_scratch = [
            pltpu.VMEM((attn_rows, width), BF),
            *LineReduce.scratch(layers, 3, attn_rows, width),
            *Exchange.scratch(),
            *Exchange.scratch(),
        ]
    return pl.pallas_call(
        functools.partial(last_kernel, columns, layers, homes),
        out_shape=(
            jax.ShapeDtypeStruct((rows, width), F32),
            jax.ShapeDtypeStruct((8, width), F32),
            *back_shapes,
        ),
        in_specs=vmem_specs(5 + len(weight_sums)),
        out_specs=tuple(vmem_specs(2) + [pl.BlockSpec(memory_space=pl.ANY)] * len(back_shapes)),
        scratch_shapes=[
            pltpu.VMEM((8, width), F32),
            pltpu.VMEM((columns, 8, width), F32),
            pltpu.VMEM((8, width), F32),
            pltpu.VMEM((layers, 8, width), F32),
            pltpu.SemaphoreType.DMA((columns,)),
            pltpu.SemaphoreType.DMA((columns,)),
            pltpu.SemaphoreType.DMA((layers,)),
            pltpu.SemaphoreType.DMA((layers,)),
            *Reduce.buffers(chips, rows, width),
            *Reduce.semaphores(chips),
            *back_scratch,
        ],
        compiler_params=comm_params(5),
        name="last_step",
        cost_estimate=pl.CostEstimate(flops=0, bytes_accessed=150_000_000, transcendentals=0),
    )(part_in, x_own, grad_middle, gain_row, sums, *weight_sums)


def turned(heads, low):
    return jnp.where(low, pltpu.roll(heads, LANES - HEAD_SIZE // 2, 1), pltpu.roll(heads, HEAD_SIZE // 2, 1))


def allowed_tile(start_ref, row_first, col_first):
    rows = row_first + lax.broadcasted_iota(jnp.int32, (TILE, TILE), 0)
    cols = col_first + lax.broadcasted_iota(jnp.int32, (TILE, TILE), 1)
    starts = jnp.broadcast_to(start_ref[row_first : row_first + TILE, 0:1], (TILE, TILE))
    return (cols <= rows) & (cols >= starts)


def forward_kernel(columns, layers, heads, *refs):
    (h_ref, w_ref, cos_ref, sin_ref, start_ref, x_ref, gain_ref, dy_ref, ffn_shard), refs = refs[:9], refs[9:]
    (q_ref, k_ref, v_ref, att_ref, log_ref, pad_ref, middle_ref), refs = refs[:7], refs[7:]
    (h2_full, dy_full, ffn_col), (part_ref, hidden, *scratch) = refs[:3], refs[3:]
    seq, own_rows, chips = h_ref.shape[0], x_ref.shape[0], columns // 2
    greet(columns, layers)
    line = LineGather(ffn_col, ffn_shard, layers, 3, scratch[0:5])
    dy_gather = Gather(dy_ref, dy_full, chips, scratch[5:10])
    scale = HEAD_SIZE**-0.5
    for slot in range(2 * heads + 2):
        pad_ref[slot * LANES : slot * LANES + HEAD_SIZE, :] = w_ref[
            slot * HEAD_SIZE : (slot + 1) * HEAD_SIZE, :
        ]
        pad_ref[slot * LANES + HEAD_SIZE : (slot + 1) * LANES, :] = jnp.zeros(
            (LANES - HEAD_SIZE, w_ref.shape[1]), BF
        )
    width = (heads + 2) * LANES

    @pl.loop(0, seq // TILE)
    def project(i):
        at = pl.ds(pl.multiple_of(i * TILE, TILE), TILE)
        low = lax.broadcasted_iota(jnp.int32, (TILE, LANES), 1) < HEAD_SIZE // 2
        projected = product_transposed(h_ref[at, :], pad_ref[0:width, :])
        cosine, sine = cos_ref[at, :], sin_ref[at, :]
        for head in range(heads + 1):
            u = projected[:, head * LANES : (head + 1) * LANES]
            r = (u * cosine + turned(u, low) * sine).astype(BF)
            if head < heads:
                q_ref[at, head * LANES : (head + 1) * LANES] = r
            else:
                k_ref[at, :] = r
        v_ref[at, :] = projected[:, (heads + 1) * LANES :].astype(BF)

    for i in range(seq // TILE):
        rows = slice(i * TILE, (i + 1) * TILE)
        for head in range(heads):
            lanes = slice(head * LANES, (head + 1) * LANES)
            q = q_ref[rows, lanes]
            out = jnp.zeros((TILE, LANES), F32)
            total = jnp.zeros((TILE, 1), F32)
            for j in range(i + 1):
                keys = slice(j * TILE, (j + 1) * TILE)
                s = product_transposed(q, k_ref[keys, :]) * scale
                e = jnp.where(allowed_tile(start_ref, i * TILE, j * TILE), jnp.exp(s), 0.0)
                total = total + jnp.sum(e, axis=1, keepdims=True)
                out = out + plain_times(e.astype(BF), v_ref[keys, :])
            att_ref[rows, lanes] = (out / total).astype(BF)
            log_ref[rows, lanes] = jnp.broadcast_to(jnp.log(total), (TILE, LANES))

    @pl.loop(0, seq // TILE)
    def project_out(i):
        at = pl.ds(pl.multiple_of(i * TILE, TILE), TILE)
        part_ref[at, :] = plain_times(att_ref[at, :], pad_ref[width:, :]).astype(BF)

    reduce = Reduce(part_ref, chips, own_rows, scratch[10:12], scratch[12:16])
    line.relay(1)
    reduce.exchange()
    line.relay(1)
    dy_gather.pass_on()
    line.relay(1)
    reduce.arrive()

    @pl.loop(0, own_rows // CHUNK)
    def finish(k):
        at = chunk_rows(k)
        middle = x_ref[at, :].astype(F32) + reduce.total(k)
        middle_ref[at, :] = middle
        hidden[at, :] = (middle * rms_scale(middle) * (1.0 + gain_ref[...])).astype(BF)

    gather = Gather(hidden, h2_full, chips, scratch[16:21])
    line.relay(2)
    gather.pass_on()
    line.relay()
    gather.finish()
    dy_gather.finish()
    reduce.drain()
    line.finish()


def forward_step(h_full, w_col, cosine, sine, starts, x_own, gain_row, dy_own, ffn_shard, heads, columns, layers):
    seq, width = h_full.shape
    rows = x_own.shape[0]
    chips = columns // 2
    return pl.pallas_call(
        functools.partial(forward_kernel, columns, layers, heads),
        out_shape=(
            jax.ShapeDtypeStruct((seq, heads * LANES), BF),
            jax.ShapeDtypeStruct((seq, LANES), BF),
            jax.ShapeDtypeStruct((seq, LANES), BF),
            jax.ShapeDtypeStruct((seq, heads * LANES), BF),
            jax.ShapeDtypeStruct((seq, heads * LANES), F32),
            jax.ShapeDtypeStruct(((2 * heads + 2) * LANES, width), BF),
            jax.ShapeDtypeStruct((rows, width), F32),
            jax.ShapeDtypeStruct((seq, width), BF),
            jax.ShapeDtypeStruct((seq, width), BF),
            jax.ShapeDtypeStruct((layers * ffn_shard.shape[0], width), BF),
        ),
        in_specs=vmem_specs(9),
        out_specs=tuple(vmem_specs(7) + [pl.BlockSpec(memory_space=pl.ANY)] * 3),
        scratch_shapes=[
            pltpu.VMEM((seq, width), BF),
            pltpu.VMEM((rows, width), BF),
            *LineGather.scratch(layers, 3),
            *Gather.scratch(chips),
            *Reduce.buffers(chips, rows, width),
            *Reduce.semaphores(chips),
            *Gather.scratch(chips),
        ],
        compiler_params=comm_params(3),
        name="forward_step",
        cost_estimate=pl.CostEstimate(flops=6_000_000_000, bytes_accessed=150_000_000, transcendentals=2_000_000),
    )(h_full, w_col, cosine, sine, starts, x_own, gain_row, dy_own, ffn_shard)


class Load:
    def __init__(self, source, target, sems, blocks=1):
        size = source.shape[0] // blocks
        self.copies = []
        for k in range(blocks):
            at = pl.ds(k * size, size)
            copy = pltpu.make_async_copy(source.at[at, :], target.at[at, :], sems.at[k])
            copy.start()
            self.copies.append(copy)
        self.next = 0

    def wait(self, count=None):
        stop = len(self.copies) if count is None else self.next + count
        for copy in self.copies[self.next : stop]:
            copy.wait()
        self.next = stop


def columns_of(width, most=512):
    return most, width // most


def backward_kernel(columns, layers, heads, sharers, factor, *refs):
    (h2_hbm, dy_hbm, w_hbm, h_hbm, pad_hbm), refs = refs[:5], refs[5:]
    (cos_hbm, sin_hbm, start_hbm, q_hbm, k_hbm, v_hbm, att_hbm, log_hbm), refs = refs[:8], refs[8:]
    (middle_ref, dy_ref, gain_ref), refs = refs[:3], refs[3:]
    (block_out_ref, grad_ref, sums_ref, ffn_sum, term_in, in_part), refs = refs[:6], refs[6:]
    (x_ref, y_ref, w_ref, pad_ref, cos_ref, sin_ref, start_ref), refs = refs[:7], refs[7:]
    (q_ref, k_ref, v_ref, att_ref, log_ref), refs = refs[:5], refs[5:]
    (act_ref, gg_ref, gu_ref, act_t, gg_t, gu_t, term, part_ref), refs = refs[:8], refs[8:]
    (gm_full, grad_bf, dk_ref, dv_ref, out_ref, out_t), refs = refs[:6], refs[6:]
    ga_ref, shared_ref = gg_ref.at[:, 0 : heads * LANES], act_ref.at[:, 0 : 2 * LANES]
    load_sems, store_sem, shared_send, shared_recv, *scratch = refs
    seq, own_rows, chips = gm_full.shape[0], middle_ref.shape[0], columns // 2
    hidden = w_ref.shape[0] // 3
    tiles = seq // TILE
    block, blocks = columns_of(w_ref.shape[1])
    w_load = Load(w_hbm, w_ref, load_sems.at[pl.ds(0, 3)], 3)
    h2_load = Load(h2_hbm, x_ref, load_sems.at[pl.ds(3, 1)])
    dy_load = Load(dy_hbm, y_ref, load_sems.at[pl.ds(4, 1)])
    later = [
        Load(source, target, load_sems.at[pl.ds(5 + k, 1)])
        for k, (source, target) in enumerate(
            (
                (pad_hbm, pad_ref),
                (cos_hbm, cos_ref),
                (sin_hbm, sin_ref),
                (start_hbm, start_ref),
                (q_hbm, q_ref),
                (k_hbm, k_ref),
                (v_hbm, v_ref),
                (att_hbm, att_ref),
                (log_hbm, log_ref),
            )
        )
    ]
    greet(columns, layers)
    w_gate, w_up, w_down = (pl.ds(k * hidden, hidden) for k in range(3))

    w_load.wait()
    h2_load.wait()
    dy_load.wait()

    @pl.loop(0, tiles)
    def feed_forward(i):
        at = pl.ds(pl.multiple_of(i * TILE, TILE), TILE)
        gate = product_transposed(x_ref[at, :], w_ref[w_gate, :])
        up = product_transposed(x_ref[at, :], w_ref[w_up, :])
        grad_act = product_transposed(y_ref[at, :], w_ref[w_down, :])
        sigmoid = 1.0 / (1.0 + jnp.exp(-gate))
        swish = gate * sigmoid
        act_ref[at, :] = (swish * up).astype(BF)
        gg_ref[at, :] = (grad_act * up * sigmoid * (1.0 + gate * (1.0 - sigmoid))).astype(BF)
        gu_ref[at, :] = (grad_act * swish).astype(BF)
        act_t[:, at] = jnp.transpose(act_ref[at, :])
        gg_t[:, at] = jnp.transpose(gg_ref[at, :])
        gu_t[:, at] = jnp.transpose(gu_ref[at, :])

    @pl.loop(0, blocks)
    def weight_gradients(j):
        at = pl.ds(pl.multiple_of(j * block, block), block)
        for rows, left, right in ((w_gate, gg_t, x_ref), (w_up, gu_t, x_ref), (w_down, act_t, y_ref)):
            term[rows, at] = (plain_times(left[...], right[:, at]) * factor).astype(BF)

    line = LineReduce(term, layers, 3, scratch[0:6])
    h_load = Load(h_hbm, x_ref, load_sems.at[pl.ds(14, 1)])

    @pl.loop(0, tiles)
    def back_part(i):
        at = pl.ds(pl.multiple_of(i * TILE, TILE), TILE)
        part_ref[at, :] = (
            plain_times(gg_ref[at, :], w_ref[w_gate, :]) + plain_times(gu_ref[at, :], w_ref[w_up, :])
        ).astype(BF)

    back = Reduce(part_ref, chips, own_rows, scratch[6:8], scratch[8:12])
    sums_ref[...] = jnp.zeros_like(sums_ref)

    @pl.loop(0, tiles)
    def out_part(i):
        at = pl.ds(pl.multiple_of(i * TILE, TILE), TILE)
        y_ref[at, :] = plain_times(act_ref[at, :], w_ref[w_down, :]).astype(BF)

    back.exchange()
    line.relay(2)
    back.arrive()
    back.drain()

    @pl.loop(0, own_rows // CHUNK)
    def turn(k):
        at = chunk_rows(k)
        grad_hidden = back.total(k)
        middle = middle_ref[at, :]
        scale = rms_scale(middle)
        normed = middle * scale
        sums_ref[0:1, :] += jnp.sum(grad_hidden * normed, axis=0, keepdims=True)
        grad = dy_ref[at, :].astype(F32) + norm_backward(grad_hidden, normed, scale, gain_ref[...])
        grad_ref[at, :] = grad
        grad_bf[at, :] = grad.astype(BF)

    gather = Gather(grad_bf, gm_full, chips, scratch[12:17])
    line.relay(1)
    gather.pass_on()
    line.relay(2)
    gather.finish()
    out = Reduce(y_ref, chips, own_rows, scratch[6:8], scratch[17:21])
    for load in later:
        load.wait()

    scale = HEAD_SIZE**-0.5
    width = (heads + 2) * LANES

    @pl.loop(0, tiles)
    def attended_gradient(i):
        at = pl.ds(pl.multiple_of(i * TILE, TILE), TILE)
        ga_ref[at, :] = product_transposed(gm_full[at, :], pad_ref[width:, :]).astype(BF)

    out.exchange()
    dk_ref[...] = jnp.zeros_like(dk_ref)
    dv_ref[...] = jnp.zeros_like(dv_ref)
    low = lax.broadcasted_iota(jnp.int32, (TILE, LANES), 1) < HEAD_SIZE // 2

    def turn_back(u, rows):
        return (u * cos_ref[rows, :] - turned(u, low) * sin_ref[rows, :]).astype(BF)

    for i in range(tiles):
        rows = slice(i * TILE, (i + 1) * TILE)
        for head in range(heads):
            lanes = slice(head * LANES, (head + 1) * LANES)
            q = q_ref[rows, lanes]
            ga = ga_ref[rows, lanes]
            delta = jnp.sum(ga.astype(F32) * att_ref[rows, lanes].astype(F32), axis=1, keepdims=True)
            logs = log_ref[rows, head * LANES : head * LANES + 1]
            dq = jnp.zeros((TILE, LANES), F32)
            for j in range(i + 1):
                keys = slice(j * TILE, (j + 1) * TILE)
                s = product_transposed(q, k_ref[keys, :]) * scale
                p = jnp.where(allowed_tile(start_ref, i * TILE, j * TILE), jnp.exp(s - logs), 0.0)
                dp = product_transposed(ga, v_ref[keys, :])
                ds = (p * (dp - delta) * scale).astype(BF)
                dq = dq + plain_times(ds, k_ref[keys, :])
                dk_ref[keys, :] += transposed_times(ds, q)
                dv_ref[keys, :] += transposed_times(p.astype(BF), ga)
            out_ref[rows, lanes] = turn_back(dq, rows)
        if i == tiles // 2:
            line.relay(1)
    line.relay(1)
    for i in range(tiles):
        rows = slice(i * TILE, (i + 1) * TILE)
        out_ref[rows, heads * LANES : (heads + 1) * LANES] = turn_back(dk_ref[rows, :], rows)
        out_ref[rows, (heads + 1) * LANES :] = dv_ref[rows, :].astype(BF)
    if sharers > 1:
        me = lax.axis_index("context")
        both = pl.ds(heads * LANES, 2 * LANES)
        copy = send(
            out_ref.at[:, both], shared_ref, shared_send, shared_recv, {"context": sibling_of(me)}
        )
        copy.wait()
        lane = lax.broadcasted_iota(jnp.int32, (TILE, 2 * LANES), 1) % LANES
        kept = lane // (HEAD_SIZE // sharers) == lax.rem(me, 2)
        for i in range(tiles):
            rows = slice(i * TILE, (i + 1) * TILE)
            value = out_ref[rows, both].astype(F32) + shared_ref[rows, :].astype(F32)
            out_ref[rows, both] = jnp.where(kept, value, 0.0).astype(BF)
    for i in range(tiles):
        rows = slice(i * TILE, (i + 1) * TILE)
        out_t[0:width, rows] = jnp.transpose(out_ref[rows, :])
        out_t[width:, rows] = jnp.transpose(att_ref[rows, :])

    @pl.loop(0, tiles)
    def input_part(i):
        at = pl.ds(pl.multiple_of(i * TILE, TILE), TILE)
        part_ref[at, :] = plain_times(out_ref[at, :], pad_ref[0:width, :]).astype(BF)

    store = pltpu.make_async_copy(part_ref, in_part, store_sem)
    store.start()
    h_load.wait()

    @pl.loop(0, blocks)
    def attention_gradients(j):
        at = pl.ds(pl.multiple_of(j * block, block), block)
        inner = (plain_times(out_t[0:width, :], x_ref[:, at]) * factor).astype(BF)
        outer = (plain_times(out_t[width:, :], gm_full[:, at]) * factor).astype(BF)
        for value, first, count in ((inner, 0, heads + 2), (outer, heads + 2, heads)):
            for k in range(count):
                if sharers > 1:
                    term_in[pl.ds((first + k) * LANES, LANES), at] = value[k * LANES : (k + 1) * LANES, :]
                else:
                    term_in[pl.ds((first + k) * HEAD_SIZE, HEAD_SIZE), at] = value[
                        k * LANES : k * LANES + HEAD_SIZE, :
                    ]

    out.arrive()

    @pl.loop(0, own_rows // CHUNK)
    def finish_out(k):
        at = chunk_rows(k)
        block_out_ref[at, :] = middle_ref[at, :] + out.total(k)

    line.finish(ffn_sum)
    store.wait()
    line.drain()
    out.drain()


def backward_step(
    h2_full, dy_full, ffn_col, h_full, padded, tables, saved, middle, dy_own, gain_row, heads, columns, layers, sharers
):
    seq, width = h2_full.shape
    rows = seq // columns
    chips = columns // 2
    hidden = ffn_col.shape[0] // 3
    ffn_rows = ffn_col.shape[0] // layers
    each = HEAD_SIZE if sharers == 1 else LANES
    loaded = [ffn_col, padded, *tables, *saved]
    return pl.pallas_call(
        functools.partial(
            backward_kernel, columns, layers, heads, sharers, float(seq * layers) ** (-0.5)
        ),
        out_shape=(
            jax.ShapeDtypeStruct((rows, width), F32),
            jax.ShapeDtypeStruct((rows, width), F32),
            jax.ShapeDtypeStruct((8, width), F32),
            jax.ShapeDtypeStruct((ffn_rows, width), BF),
            jax.ShapeDtypeStruct(((2 * heads + 2) * each, width), BF),
            jax.ShapeDtypeStruct((seq, width), BF),
        ),
        in_specs=[pl.BlockSpec(memory_space=pl.ANY)] * 13 + vmem_specs(3),
        out_specs=tuple(vmem_specs(5) + [pl.BlockSpec(memory_space=pl.ANY)]),
        scratch_shapes=[
            pltpu.VMEM((seq, width), BF),
            pltpu.VMEM((seq, width), BF),
            *[pltpu.VMEM(array.shape, array.dtype) for array in loaded],
            *[pltpu.VMEM((seq, hidden), BF)] * 3,
            *[pltpu.VMEM((hidden, seq), BF)] * 3,
            pltpu.VMEM(ffn_col.shape, BF),
            pltpu.VMEM((seq, width), BF),
            pltpu.VMEM((seq, width), BF),
            pltpu.VMEM((rows, width), BF),
            pltpu.VMEM((seq, LANES), F32),
            pltpu.VMEM((seq, LANES), F32),
            pltpu.VMEM((seq, (heads + 2) * LANES), BF),
            pltpu.VMEM(((2 * heads + 2) * LANES, seq), BF),
            pltpu.SemaphoreType.DMA((15,)),
            pltpu.SemaphoreType.DMA,
            pltpu.SemaphoreType.DMA,
            pltpu.SemaphoreType.DMA,
            *LineReduce.scratch(layers, 3, ffn_rows, width),
            *Reduce.buffers(chips, rows, width),
            *Reduce.semaphores(chips),
            *Gather.scratch(chips),
            *Reduce.semaphores(chips),
        ],
        compiler_params=comm_params(4),
        name="backward_step",
        cost_estimate=pl.CostEstimate(flops=28_000_000_000, bytes_accessed=150_000_000, transcendentals=4_000_000),
    )(h2_full, dy_full, ffn_col, h_full, padded, *tables, *saved, middle, dy_own, gain_row)


def update_rows(g_ref, p_ref, m_ref, grad_ref, new_p_ref, new_m_ref):
    gradient = g_ref[...].astype(F32)
    grad_ref[...] = gradient
    parameter = p_ref[...]
    first_moment = BETA_ONE * m_ref[0] + (1.0 - BETA_ONE) * gradient
    second_moment = BETA_TWO * m_ref[1] + (1.0 - BETA_TWO) * gradient * gradient
    new_m_ref[0] = first_moment
    new_m_ref[1] = second_moment
    below = jnp.sqrt(second_moment * (1.0 / (1.0 - BETA_TWO**STEP))) + ADAM_EPS
    step = first_moment * (LEARN_RATE / (1.0 - BETA_ONE**STEP)) / below
    new_p_ref[...] = parameter * (1.0 - LEARN_RATE * WEIGHT_DECAY) - step


def update_kernel(steps, *refs):
    first = pl.program_id(0) < steps

    @pl.when(first)
    def one():
        update_rows(*refs[0:3], *refs[6:9])

    @pl.when(jnp.logical_not(first))
    def other():
        update_rows(*refs[3:6], *refs[9:12])


def update_all(first, second):
    specs, shapes = [], []
    blocks = []
    for gradient, parameter, _ in (first, second):
        rows = parameter.shape[0]
        whole = [n for n in (48, 32) if rows % n == 0]
        blocks.append(whole[0] if whole else rows)
    steps = first[1].shape[0] // blocks[0]
    rest = second[1].shape[0] // blocks[1]
    for block, place, (_, parameter, _) in (
        (blocks[0], lambda i: jnp.minimum(i, steps - 1), first),
        (blocks[1], lambda i: jnp.maximum(i - steps, 0), second),
    ):
        rows, width = parameter.shape
        flat = pl.BlockSpec((block, width), lambda i, place=place: (place(i), 0))
        pair = pl.BlockSpec((2, block, width), lambda i, place=place: (0, place(i), 0))
        specs.append([flat, flat, pair])
        shapes += [
            jax.ShapeDtypeStruct((rows, width), F32),
            jax.ShapeDtypeStruct((rows, width), F32),
            jax.ShapeDtypeStruct((2, rows, width), F32),
        ]
    out = pl.pallas_call(
        functools.partial(update_kernel, steps),
        grid=(steps + rest,),
        out_shape=tuple(shapes),
        in_specs=specs[0] + specs[1],
        out_specs=tuple(specs[0] + specs[1]),
        compiler_params=pltpu.CompilerParams(vmem_limit_bytes=VMEM_LIMIT),
        name="update_all",
        cost_estimate=pl.CostEstimate(flops=20_000_000, bytes_accessed=25_000_000, transcendentals=1_000_000),
    )(*first, *second)
    return out[:3], out[3:]


def rope_tables(positions):
    half_width = HEAD_SIZE // 2
    frequency = ROPE_THETA ** (-2.0 * jnp.arange(half_width, dtype=F32) / HEAD_SIZE)
    angles = positions.astype(F32)[:, None] * frequency[None, :]
    cosine, sine = jnp.cos(angles), jnp.sin(angles)
    blank = jnp.zeros((positions.shape[0], LANES - HEAD_SIZE), F32)
    return (
        jnp.concatenate([cosine, cosine, blank], axis=1),
        jnp.concatenate([-sine, sine, blank], axis=1),
    )


def unpadded(rows, count):
    return jnp.concatenate([rows[k * LANES : k * LANES + HEAD_SIZE] for k in range(count)])


def on_device(
    block_input,
    cotangent,
    documents,
    attn_weights,
    ffn_weights,
    norm_gains,
    attn_moments,
    ffn_moments,
    gain_moments,
):
    layers, columns = lax.axis_size("fsdp"), lax.axis_size("context")
    rows, width = block_input.shape[1:]
    seq = rows * columns
    heads = QUERY_HEADS // columns
    sharers = max(1, columns // KEY_VALUE_HEADS)
    share = KEY_VALUE_HEADS * HEAD_SIZE // columns
    grad_factor = float(rows * layers * columns) ** (-0.5)
    attn_plan, ffn_plan = unit_plans(layers, columns, attn_weights.shape[0] * layers * columns)
    core = lax.rem(lax.axis_index("context"), 2)
    swap = [(c, c + 1 - 2 * (c % 2)) for c in range(columns)]

    x_own, dy_own = block_input[0], cotangent[0]
    aligned = attn_weights.shape[0] % (3 * CHUNK) == 0 and layers > 1
    if aligned:
        h_full, docs_full, attn_col, ffn_shard = open_step(
            x_own, norm_gains[0:1], documents, attn_weights, ffn_weights, columns, layers
        )
    else:
        residual = x_own.astype(F32)
        first_hidden = (residual * rms_scale(residual) * (1.0 + norm_gains[0])).astype(BF)
        h_full, docs_full = gather_docs(first_hidden, documents, columns)
        attn_col = lax.all_gather(
            attn_plan.spread(attn_weights.astype(BF)), "fsdp", axis=0, tiled=True
        )
        ffn_shard = ffn_plan.spread(ffn_weights.astype(BF))
    query_rows = heads * HEAD_SIZE
    if sharers > 1:
        own_part = attn_col[query_rows : query_rows + 2 * share]
        other = lax.ppermute(own_part, "context", swap)

        def whole_head(first):
            mine, theirs = own_part[first : first + share], other[first : first + share]
            return jnp.where(
                core == 0, jnp.concatenate([mine, theirs]), jnp.concatenate([theirs, mine])
            )

        attn_col = jnp.concatenate(
            [
                attn_col[:query_rows],
                whole_head(0),
                whole_head(share),
                attn_col[query_rows + 2 * share :],
            ]
        )

    all_docs = docs_full.reshape(seq)
    starts = jnp.sum((all_docs[None, :] < all_docs[:, None]).astype(jnp.int32), axis=1)
    cosine, sine = rope_tables(jnp.arange(seq, dtype=jnp.int32) - starts)
    start_lanes = jnp.broadcast_to(starts[:, None], (seq, LANES))
    tables = (cosine, sine, start_lanes)
    *saved, padded, middle, h2_full, dy_full, ffn_col = forward_step(
        h_full, attn_col, *tables, x_own, norm_gains[1:2], dy_own, ffn_shard, heads, columns, layers
    )

    block_out, grad_middle, sums, ffn_sum, attn_term, in_part = backward_step(
        h2_full,
        dy_full,
        ffn_col,
        h_full,
        padded,
        tables,
        saved,
        middle,
        dy_own,
        norm_gains[1:2],
        heads,
        columns,
        layers,
        sharers,
    )
    if sharers > 1:
        own_rows = [
            lax.dynamic_slice_in_dim(attn_term, (heads + k) * LANES + core * share, share, 0)
            for k in range(2)
        ]
        attn_term = jnp.concatenate(
            [
                unpadded(attn_term, heads),
                *own_rows,
                unpadded(attn_term[(heads + 2) * LANES :], heads),
            ]
        )
    last_args = (in_part, x_own, grad_middle, norm_gains[0:1], sums, columns, layers)
    if aligned:
        grad_input, gain_sums, attn_shard, ffn_shard = last_step(*last_args, (attn_term, ffn_sum))
    else:
        attn_sum = lax.psum_scatter(attn_term, "fsdp", scatter_dimension=0, tiled=True)
        grad_input, gain_sums = last_step(*last_args)
        ffn_shard = ffn_plan.collect(ffn_sum)
        attn_shard = attn_plan.collect(attn_sum)

    column_count = width // (layers * columns)
    first_column = lax.axis_index(EVERY) * column_count
    gain_shard = lax.dynamic_slice_in_dim(gain_sums[:2], first_column, column_count, 1) * grad_factor
    own_gains = lax.dynamic_slice_in_dim(norm_gains, first_column, column_count, 1)
    (ffn_shard, new_ffn, ffn_states), (attn_shard, new_attn, attn_states) = update_all(
        (ffn_shard, ffn_weights, ffn_moments), (attn_shard, attn_weights, attn_moments)
    )
    new_gains, gain_states = adamw_update(own_gains, gain_shard, gain_moments, 0.0)
    return (
        block_out[None],
        grad_input[None],
        attn_shard,
        ffn_shard,
        gain_shard,
        new_attn,
        new_ffn,
        new_gains,
        attn_states,
        ffn_states,
        jnp.stack(gain_states),
    )


def solution(mesh):
    placed = (
        P("fsdp", "context", None),
        P("fsdp", "context", None),
        P("fsdp", "context"),
        P(EVERY, None),
        P(EVERY, None),
        P(),
        P(None, EVERY, None),
        P(None, EVERY, None),
        P(None, None, EVERY),
    )
    return jax.shard_map(
        on_device,
        mesh=mesh,
        in_specs=placed,
        out_specs=(
            P("fsdp", "context", None),
            P("fsdp", "context", None),
            P(EVERY, None),
            P(EVERY, None),
            P(None, EVERY),
            P(EVERY, None),
            P(EVERY, None),
            P(None, EVERY),
            P(None, EVERY, None),
            P(None, EVERY, None),
            P(None, None, EVERY),
        ),
        check_vma=False,
    )
```

```python
import functools

import jax
import jax.numpy as jnp
import numpy as np
from jax import lax
from jax.experimental import pallas as pl
from jax.experimental.pallas import tpu as pltpu
from jax.sharding import PartitionSpec as P

QUERY_HEADS = 16
KEY_VALUE_HEADS = 8
HEAD_SIZE = 96
STEP = 3

NORM_EPS = 1e-05
ROPE_THETA = 100000.0
BETA_ONE = 0.9
BETA_TWO = 0.95
ADAM_EPS = 1e-08
LEARN_RATE = 0.02
WEIGHT_DECAY = 0.1

LANES = 128
TILE = 256
CHUNK = 16
VMEM_LIMIT = 67_000_000
EVERY = ("fsdp", "context")
BF = jnp.bfloat16
F32 = jnp.float32
ID_TYPE = pl.DeviceIdType.MESH


def product_transposed(left_matrix, right_matrix):
    return lax.dot_general(
        left_matrix, right_matrix, (((1,), (1,)), ((), ())), preferred_element_type=F32
    )


def transposed_times(left_matrix, right_matrix):
    return lax.dot_general(
        left_matrix, right_matrix, (((0,), (0,)), ((), ())), preferred_element_type=F32
    )


def plain_times(left_matrix, right_matrix):
    return jnp.dot(left_matrix, right_matrix, preferred_element_type=F32)


def rms_scale(tensor_in):
    return lax.rsqrt(jnp.mean(tensor_in * tensor_in, axis=-1, keepdims=True) + NORM_EPS)


def norm_backward(grad_in, normed, norm_scale, gain_row):
    scaled = grad_in * (1.0 + gain_row)
    return norm_scale * (scaled - normed * jnp.mean(scaled * normed, axis=-1, keepdims=True))


def adamw_update(parameter, gradient, moments, decay_rate):
    first_moment = BETA_ONE * moments[0] + (1.0 - BETA_ONE) * gradient
    second_moment = BETA_TWO * moments[1] + (1.0 - BETA_TWO) * gradient * gradient
    first_hat = first_moment / (1.0 - BETA_ONE**STEP)
    second_hat = second_moment / (1.0 - BETA_TWO**STEP)
    updated = parameter - LEARN_RATE * (
        first_hat / (jnp.sqrt(second_hat) + ADAM_EPS) + decay_rate * parameter
    )
    return (updated, (first_moment, second_moment))


class UnitPlan:
    def __init__(self, homes, devices):
        waiting = [[] for _ in range(devices)]
        for unit, (device, place) in enumerate(homes):
            waiting[unit // 3].append((unit % 3, device, place))
        self.rounds = []
        for _ in range(3):
            taken = [None] * devices

            def settle(source, seen):
                for piece, device, place in waiting[source]:
                    if device in seen:
                        continue
                    seen.add(device)
                    if taken[device] is None or settle(taken[device][0], seen):
                        taken[device] = (source, piece, place)
                        return True
                return False

            for source in range(devices):
                if not settle(source, set()):
                    raise ValueError("no matching")
            pairs, pieces, places = [], [0] * devices, [0] * devices
            for device, (source, piece, place) in enumerate(taken):
                pairs.append((source, device))
                pieces[source] = piece
                places[device] = place
                waiting[source].remove((piece, device, place))
            self.rounds.append((pairs, np.array(pieces), np.array(places)))

    def _reorder(self, got, columns):
        order = np.argsort(np.stack(columns, axis=1), axis=1).astype(np.int32)
        mine = jnp.asarray(order)[lax.axis_index(EVERY)]
        stacked = jnp.stack(got)
        return jnp.concatenate(
            [lax.dynamic_index_in_dim(stacked, mine[k], 0, keepdims=False) for k in range(3)]
        )

    def spread(self, rows):
        pieces = rows.reshape(3, rows.shape[0] // 3, rows.shape[1])
        me = lax.axis_index(EVERY)
        got = []
        for pairs, piece, _ in self.rounds:
            unit = lax.dynamic_index_in_dim(
                pieces, jnp.asarray(piece, jnp.int32)[me], 0, keepdims=False
            )
            got.append(lax.ppermute(unit, EVERY, pairs))
        return self._reorder(got, [place for _, _, place in self.rounds])

    def collect(self, rows):
        places_of = rows.reshape(3, rows.shape[0] // 3, rows.shape[1])
        me = lax.axis_index(EVERY)
        got = []
        for pairs, _, place in self.rounds:
            unit = lax.dynamic_index_in_dim(
                places_of, jnp.asarray(place, jnp.int32)[me], 0, keepdims=False
            )
            got.append(lax.ppermute(unit, EVERY, [(b, a) for a, b in pairs]))
        return self._reorder(got, [piece for _, piece, _ in self.rounds])


def unit_plans(layers, columns, attn_rows):
    devices = layers * columns

    def home(column, position):
        return ((position // 3) * columns + column, position % 3)

    homes = []
    for unit in range(3 * devices):
        matrix, rest = divmod(unit, devices)
        stretch, column = divmod(rest, columns)
        homes.append(home(column, matrix * layers + stretch))
    ffn_plan = UnitPlan(homes, devices)
    unit_rows = attn_rows // (3 * devices)
    query_units = QUERY_HEADS * HEAD_SIZE // columns // unit_rows
    share_units = KEY_VALUE_HEADS * HEAD_SIZE // columns // unit_rows
    homes = []
    position = 0
    for count in (query_units, share_units, share_units, query_units):
        for column in range(columns):
            for k in range(count):
                homes.append(home(column, position + k))
        position += count
    return UnitPlan(homes, devices), ffn_plan


class Homes:
    def __init__(self, layers, columns, attn_rows):
        devices = layers * columns
        unit_rows = attn_rows // (3 * devices)
        self.layers, self.columns = layers, columns
        self.counts = [
            QUERY_HEADS * HEAD_SIZE // columns // unit_rows,
            KEY_VALUE_HEADS * HEAD_SIZE // columns // unit_rows,
        ]
        query, share = self.counts
        self.first = [0, query, query + share, query + 2 * share]
        self.sizes = [query, share, share, query]

    def _spot(self, column, position):
        return position // 3, column, position % 3

    def _column(self, group):
        half = self.columns // 2
        return group % half * 2 + group // half

    def _group(self, column):
        return column % 2 * (self.columns // 2) + column // 2

    def attn_targets(self):
        device = lax.axis_index("fsdp") * self.columns + lax.axis_index("context")
        found = []
        for piece in range(3):
            unit = device * 3 + piece
            column, position = 0, 0
            for first, size in zip(self.first, self.sizes):
                inside = unit - first * self.columns
                begun = inside >= 0
                column = jnp.where(begun, self._column(inside // size), column)
                position = jnp.where(begun, first + inside % size, position)
            found.append(self._spot(column, position))
        return found

    def attn_owners(self):
        group = self._group(lax.axis_index("context"))
        found = []
        for place in range(3):
            position = lax.axis_index("fsdp") * 3 + place
            unit = 0
            for first, size in zip(self.first, self.sizes):
                inside = position - first
                unit = jnp.where(inside >= 0, first * self.columns + group * size + inside, unit)
            device = unit // 3
            found.append((device // self.columns, device % self.columns, unit % 3))
        return found

    def ffn_targets(self):
        layer, column = lax.axis_index("fsdp"), lax.axis_index("context")
        return [
            (layer, (3 * column + piece) % self.columns, (3 * column + piece) // self.columns)
            for piece in range(3)
        ]

    def ffn_owners(self):
        layer, column = lax.axis_index("fsdp"), lax.axis_index("context")
        return [
            (layer, (place * self.columns + column) // 3, (place * self.columns + column) % 3)
            for place in range(3)
        ]


def partner(me, step, chips):
    return lax.rem(me // 2 + step, chips) * 2 + lax.rem(me, 2)


def sibling_of(me):
    return me + 1 - 2 * lax.rem(me, 2)


def rows_at(index, rows):
    return pl.ds(pl.multiple_of(index * rows, rows), rows)


def greet(columns, layers=1, others=()):
    barrier = pltpu.get_barrier_semaphore()
    me = lax.axis_index("context")
    awaited = columns - 1 + layers - 1
    for layer, column in others:
        apart = (layer != lax.axis_index("fsdp")) | (column != me)
        awaited = awaited + jnp.where(apart, 1, 0)

        @pl.when(apart)
        def there():
            pl.semaphore_signal(
                barrier, inc=1, device_id={"fsdp": layer, "context": column}, device_id_type=ID_TYPE
            )

    for step in range(1, columns):
        pl.semaphore_signal(
            barrier, inc=1, device_id={"context": lax.rem(me + step, columns)}, device_id_type=ID_TYPE
        )
    if layers > 1:
        layer = lax.axis_index("fsdp")
        for step in range(1, layers):
            pl.semaphore_signal(
                barrier, inc=1, device_id={"fsdp": lax.rem(layer + step, layers)}, device_id_type=ID_TYPE
            )
    pl.semaphore_wait(barrier, awaited)


def send(source, target, send_sem, recv_sem, device):
    copy = pltpu.make_async_remote_copy(
        src_ref=source,
        dst_ref=target,
        send_sem=send_sem,
        recv_sem=recv_sem,
        device_id=device,
        device_id_type=ID_TYPE,
    )
    copy.start()
    return copy


def remote(source, target, send_sem, recv_sem, device):
    return pltpu.make_async_remote_copy(
        src_ref=source,
        dst_ref=target,
        send_sem=send_sem,
        recv_sem=recv_sem,
        device_id=device,
        device_id_type=ID_TYPE,
    )


class Exchange:
    @staticmethod
    def scratch():
        return [pltpu.SemaphoreType.DMA((3,)), pltpu.SemaphoreType.DMA((3,))]

    def __init__(self, sources, targets, homes, sems):
        send_sem, recv_sem = sems
        self.parts = []
        for i, (layer, column, place) in enumerate(homes):
            itself = (layer == lax.axis_index("fsdp")) & (column == lax.axis_index("context"))
            target = targets(layer, place)
            copy = functools.partial(
                remote,
                sources[i],
                target,
                send_sem.at[i],
                recv_sem.at[place],
                {"fsdp": layer, "context": column},
            )
            stay = functools.partial(pltpu.make_async_copy, sources[i], target, recv_sem.at[place])

            @pl.when(itself)
            def here():
                stay().start()

            @pl.when(jnp.logical_not(itself))
            def there():
                copy().start()

            self.parts.append((itself, copy))
        self.landing = [
            functools.partial(pltpu.make_async_copy, sources[k], sources[k], recv_sem.at[k])
            for k in range(3)
        ]

    def arrive(self):
        for landed in self.landing:
            landed().wait()

    def drain(self):
        for itself, copy in self.parts:

            @pl.when(jnp.logical_not(itself))
            def sent():
                copy().wait_send()


class LineGather:
    @staticmethod
    def scratch(layers, pieces):
        return [*[pltpu.SemaphoreType.DMA(((layers - 1) * pieces,))] * 4, pltpu.SemaphoreType.DMA]

    def __init__(self, full, own, layers, pieces, sems):
        self.full, self.own, self.layers, self.pieces = full, own, layers, pieces
        *self.sems, local_sem = sems
        self.rows = own.shape[0]
        self.size = self.rows // pieces
        self.count = (layers - 1) * pieces
        self.local = pltpu.make_async_copy(
            own, full.at[rows_at(lax.axis_index("fsdp"), self.rows), :], local_sem
        )
        for m in range(pieces):
            self._send(m)
        self.local.start()
        self.next = pieces

    def _block(self, shard, piece):
        first = pl.multiple_of(shard * self.rows + piece * self.size, self.size)
        return self.full.at[pl.ds(first, self.size), :]

    def _moves(self, m):
        k, piece = divmod(m, self.pieces)
        layer = lax.axis_index("fsdp")
        up_send, up_recv, down_send, down_recv = self.sems
        top = self.layers - 1
        for first, last, other, shard, send_sem, recv_sem in (
            (layer - k >= 0, layer < top, layer + 1, layer - k, up_send, up_recv),
            (layer + k <= top, layer > 0, layer - 1, layer + k, down_send, down_recv),
        ):
            block = self._block(shard, piece)
            source = self.own.at[pl.ds(piece * self.size, self.size), :] if k == 0 else block
            yield first & last, functools.partial(
                remote, source, block, send_sem.at[m], recv_sem.at[m], {"fsdp": other}
            )

    def _send(self, m):
        for go, copy in self._moves(m):

            @pl.when(go)
            def start():
                copy().start()

    def _land(self, m):
        k, piece = divmod(m, self.pieces)
        layer = lax.axis_index("fsdp")
        _, up_recv, _, down_recv = self.sems
        for there, shard, recv_sem in (
            (layer - 1 - k >= 0, layer - 1 - k, up_recv),
            (layer + 1 + k <= self.layers - 1, layer + 1 + k, down_recv),
        ):
            block = self._block(shard, piece)
            copy = functools.partial(pltpu.make_async_copy, block, block, recv_sem.at[m])

            @pl.when(there)
            def landed():
                copy().wait()

    def relay(self, count=None):
        stop = self.count if count is None else min(self.count, self.next + count)
        for m in range(self.next, stop):
            self._land(m - self.pieces)
            self._send(m)
        self.next = stop

    def finish(self):
        self.relay()
        for m in range(self.count - self.pieces, self.count):
            self._land(m)
        for m in range(self.count):
            for go, copy in self._moves(m):

                @pl.when(go)
                def sent():
                    copy().wait_send()

        self.local.wait()


class LineReduce:
    @staticmethod
    def scratch(layers, pieces, rows, width):
        count = (layers - 1) * pieces
        return [
            pltpu.VMEM((count, rows // pieces, width), BF),
            pltpu.VMEM((count, rows // pieces, width), BF),
            *[pltpu.SemaphoreType.DMA((count,))] * 4,
        ]

    def __init__(self, term, layers, pieces, scratch):
        self.term, self.layers, self.pieces = term, layers, pieces
        self.rows = term.shape[0] // layers
        self.size = self.rows // pieces
        self.up_in, self.down_in, *self.sems = scratch
        self.count = (layers - 1) * pieces
        self.slots = self.count + layers - 1
        self.next = 1
        layer = lax.axis_index("fsdp")
        top = layers - 1

        @pl.when(layer == 0)
        def bottom():
            for m in range(self.count):
                self._up(m, self._block(top - m // pieces, m % pieces)).start()

        @pl.when(layer == top)
        def ceiling():
            for m in range(self.count):
                self._down(m, self._block(m // pieces, m % pieces)).start()

    def _block(self, target, piece):
        return self.term.at[pl.ds(target * self.rows + piece * self.size, self.size), :]

    def _up(self, m, source):
        up_send, up_recv, _, _ = self.sems
        other = {"fsdp": lax.axis_index("fsdp") + 1}
        return remote(source, self.up_in.at[m], up_send.at[m], up_recv.at[m], other)

    def _down(self, m, source):
        _, _, down_send, down_recv = self.sems
        other = {"fsdp": lax.axis_index("fsdp") - 1}
        return remote(source, self.down_in.at[m], down_send.at[m], down_recv.at[m], other)

    def _add(self, sums, m, target):
        first = pl.multiple_of(target * self.rows + m % self.pieces * self.size, CHUNK)

        @pl.loop(0, self.size // CHUNK)
        def add(c):
            at = chunk_rows(c)
            of_term = pl.ds(pl.multiple_of(first + c * CHUNK, CHUNK), CHUNK)
            sums[m, at, :] = (
                sums[m, at, :].astype(F32) + self.term[of_term, :].astype(F32)
            ).astype(BF)

    def _slot(self, slot):
        layer = lax.axis_index("fsdp")
        top = self.layers - 1
        _, up_recv, _, down_recv = self.sems
        m = slot - layer
        target = top - m // self.pieces

        @pl.when((layer > 0) & (m >= 0) & (m < self.count) & (layer <= target))
        def from_below():
            pltpu.make_async_copy(self.up_in.at[m], self.up_in.at[m], up_recv.at[m]).wait()

            @pl.when(layer < target)
            def pass_up():
                self._add(self.up_in, m, target)
                self._up(m, self.up_in.at[m]).start()

        n = slot - (top - layer)
        goal = n // self.pieces

        @pl.when((layer < top) & (n >= 0) & (n < self.count) & (layer >= goal))
        def from_above():
            pltpu.make_async_copy(self.down_in.at[n], self.down_in.at[n], down_recv.at[n]).wait()

            @pl.when(layer > goal)
            def pass_down():
                self._add(self.down_in, n, goal)
                self._down(n, self.down_in.at[n]).start()

    def relay(self, count=None):
        stop = self.slots if count is None else min(self.slots, self.next + count)
        if stop > self.next:

            @pl.loop(self.next, stop)
            def slots(slot):
                self._slot(slot)

        self.next = stop

    def finish(self, total):
        self.relay()
        layer = lax.axis_index("fsdp")
        top = self.layers - 1
        for own in range(self.layers):

            @pl.when(layer == own)
            def here():
                for piece in range(self.pieces):

                    @pl.loop(0, self.size // CHUNK)
                    def add(c):
                        start = pl.multiple_of(c * CHUNK, CHUNK)
                        at = pl.ds(start, CHUNK)
                        value = self.term[
                            pl.ds(own * self.rows + piece * self.size + start, CHUNK), :
                        ].astype(F32)
                        if own > 0:
                            m = (top - own) * self.pieces + piece
                            value = value + self.up_in[m, at, :].astype(F32)
                        if own < top:
                            m = own * self.pieces + piece
                            value = value + self.down_in[m, at, :].astype(F32)
                        total[pl.ds(piece * self.size + start, CHUNK), :] = value.astype(BF)

    def drain(self):
        layer = lax.axis_index("fsdp")
        top = self.layers - 1
        for m in range(self.count):
            k = m // self.pieces

            @pl.when(layer < top - k)
            def up():
                self._up(m, self.up_in.at[m]).wait_send()

            @pl.when(layer > k)
            def down():
                self._down(m, self.down_in.at[m]).wait_send()


class Gather:
    @staticmethod
    def scratch(chips):
        return [
            pltpu.SemaphoreType.DMA((chips,)),
            pltpu.SemaphoreType.DMA((chips,)),
            pltpu.SemaphoreType.DMA((chips,)),
            pltpu.SemaphoreType.DMA((chips,)),
            pltpu.SemaphoreType.DMA,
        ]

    def __init__(self, block, full, chips, sems):
        own_send, own_recv, self.on_send, self.on_recv, local_sem = sems
        me = lax.axis_index("context")
        rows = block.shape[0]
        self.block, self.full, self.chips, self.me, self.rows = block, full, chips, me, rows
        mine = full.at[rows_at(me, rows), :]
        self.own = [
            send(block, mine, own_send.at[step], own_recv.at[step], {"context": partner(me, step, chips)})
            for step in range(1, chips)
        ]
        self.own.append(
            send(block, mine, own_send.at[0], own_recv.at[0], {"context": sibling_of(me)})
        )
        self.local = pltpu.make_async_copy(block, mine, local_sem)
        self.local.start()

        self.passed = []

    def pass_on(self):
        for step in range(1, self.chips):
            self.own[step - 1].wait_recv()
            source = partner(self.me, self.chips - step, self.chips)
            there = self.full.at[rows_at(source, self.rows), :]
            self.passed.append(
                send(there, there, self.on_send.at[step], self.on_recv.at[step], {"context": sibling_of(self.me)})
            )

    def finish(self):
        if not self.passed:
            self.pass_on()
        self.own[-1].wait_recv()
        for copy in self.passed:
            copy.wait_recv()
        for copy in self.own + self.passed:
            copy.wait_send()
        self.local.wait()


class Reduce:
    @staticmethod
    def buffers(chips, rows, width):
        return [pltpu.VMEM((chips, rows, width), BF), pltpu.VMEM((chips - 1, rows, width), BF)]

    @staticmethod
    def semaphores(chips):
        return [pltpu.SemaphoreType.DMA((chips,))] * 4

    def __init__(self, part, chips, rows, buffers, semaphores):
        self.near, self.far = buffers
        near_send, near_recv, self.far_send, self.far_recv = semaphores
        me = lax.axis_index("context")
        self.part, self.chips, self.rows, self.me = part, chips, rows, me
        self.near_copies = {}
        for step in [*range(1, chips), 0]:
            block = partner(sibling_of(me), step, chips)
            self.near_copies[step] = send(
                part.at[rows_at(block, rows), :],
                self.near.at[step],
                near_send.at[step],
                near_recv.at[step],
                {"context": sibling_of(me)},
            )
        self.far_copies = []

    def exchange(self):
        for step in range(1, self.chips):
            self.near_copies[step].wait_recv()
            target = partner(self.me, step, self.chips)
            first = pl.multiple_of(target * self.rows, self.rows)

            @pl.loop(0, self.rows // CHUNK)
            def add(k):
                at = chunk_rows(k)
                from_part = pl.ds(pl.multiple_of(first + k * CHUNK, CHUNK), CHUNK)
                self.near[step, at, :] = (
                    self.part[from_part, :].astype(F32) + self.near[step, at, :].astype(F32)
                ).astype(BF)

            self.far_copies.append(
                send(
                    self.near.at[step],
                    self.far.at[step - 1],
                    self.far_send.at[step],
                    self.far_recv.at[step],
                    {"context": target},
                )
            )

    def arrive(self):
        self.near_copies[0].wait_recv()
        for copy in self.far_copies:
            copy.wait_recv()

    def total(self, k):
        at = chunk_rows(k)
        first = pl.multiple_of(self.me * self.rows, self.rows)
        value = self.part[pl.ds(pl.multiple_of(first + k * CHUNK, CHUNK), CHUNK), :].astype(F32)
        value = value + self.near[0, at, :].astype(F32)
        for step in range(1, self.chips):
            value = value + self.far[step - 1, at, :].astype(F32)
        return value

    def drain(self):
        for copy in list(self.near_copies.values()) + self.far_copies:
            copy.wait_send()


def chunk_rows(k):
    return pl.ds(pl.multiple_of(k * CHUNK, CHUNK), CHUNK)


def vmem_specs(count):
    return [pl.BlockSpec(memory_space=pltpu.VMEM)] * count


def comm_params(collective_id):
    return pltpu.CompilerParams(
        collective_id=collective_id, has_side_effects=True, vmem_limit_bytes=VMEM_LIMIT
    )


def place_rows(ref, unit, layer, place):
    return ref.at[rows_at(place, unit), :]


class Docs:
    @staticmethod
    def scratch(columns):
        return [
            pltpu.SemaphoreType.DMA((columns,)),
            pltpu.SemaphoreType.DMA((columns,)),
            pltpu.SemaphoreType.DMA,
        ]

    def __init__(self, docs, docs_full, columns, sems):
        docs_send, docs_recv, docs_local = sems
        me = lax.axis_index("context")
        mine = docs_full.at[pl.ds(me, 1), :]
        self.copies = [
            send(docs, mine, docs_send.at[step], docs_recv.at[step], {"context": lax.rem(me + step, columns)})
            for step in range(1, columns)
        ]
        self.local = pltpu.make_async_copy(docs, mine, docs_local)
        self.local.start()

    def finish(self):
        for copy in self.copies:
            copy.wait_recv()
        for copy in self.copies:
            copy.wait_send()
        self.local.wait()


def last_kernel(columns, layers, homes, *refs):
    (part_in, x_ref, grad_ref, gain_ref, sums_ref), refs = refs[:5], refs[5:]
    if homes is not None:
        (term, ffn_sum), refs = refs[:2], refs[2:]
    (input_grad_ref, gains_ref), refs = refs[:2], refs[2:]
    if homes is not None:
        (attn_back, ffn_back), refs = refs[:2], refs[2:]
    (own_sums, plane_slots, plane_sums, line_slots), refs = refs[:4], refs[4:]
    (plane_send, plane_recv, line_send, line_recv), scratch = refs[:4], refs[4:]
    chips = columns // 2
    rows = x_ref.shape[0]
    if homes is None:
        greet(columns, layers)
    else:
        attn_owners = homes.attn_owners()
        greet(columns, layers, [spot[:2] for spot in homes.attn_targets() + attn_owners])
    first = Reduce(part_in, chips, rows, scratch[0:2], scratch[2:6])
    if homes is not None:
        attn_rows, ffn_rows = term.shape[0] // layers, ffn_sum.shape[0]
        attn_done = scratch[6]
        line = LineReduce(term, layers, 3, scratch[7:13])
        unit_ffn = ffn_rows // 3
    first.exchange()
    if homes is not None:
        ffn_owned = Exchange(
            [ffn_sum.at[pl.ds(k * unit_ffn, unit_ffn), :] for k in range(3)],
            functools.partial(place_rows, ffn_back, unit_ffn),
            homes.ffn_owners(),
            scratch[13:15],
        )
        line.relay(3)
    own_sums[...] = jnp.zeros_like(own_sums)
    own_sums[1:2, :] = sums_ref[0:1, :]
    if homes is not None:
        line.relay(3)
    first.arrive()

    @pl.loop(0, rows // CHUNK)
    def finish(k):
        at = chunk_rows(k)
        grad_hidden = first.total(k)
        residual = x_ref[at, :].astype(F32)
        scale = rms_scale(residual)
        normed = residual * scale
        own_sums[0:1, :] += jnp.sum(grad_hidden * normed, axis=0, keepdims=True)
        input_grad_ref[at, :] = grad_ref[at, :] + norm_backward(
            grad_hidden, normed, scale, gain_ref[...]
        )

    me = lax.axis_index("context")
    layer = lax.axis_index("fsdp")
    in_plane = [
        send(
            own_sums,
            plane_slots.at[step],
            plane_send.at[step],
            plane_recv.at[step],
            {"context": lax.rem(me + step, columns)},
        )
        for step in range(1, columns)
    ]
    if homes is not None:
        line.finish(attn_done)
        unit = attn_rows // 3
        attn_owned = Exchange(
            [attn_done.at[pl.ds(k * unit, unit), :] for k in range(3)],
            functools.partial(place_rows, attn_back, unit),
            attn_owners,
            scratch[15:17],
        )
    total = own_sums[...]
    for step, copy in enumerate(in_plane):
        copy.wait_recv()
        total = total + plane_slots[step + 1]
    plane_sums[...] = total
    in_line = [
        send(
            plane_sums,
            line_slots.at[step],
            line_send.at[step],
            line_recv.at[step],
            {"fsdp": lax.rem(layer + step, layers)},
        )
        for step in range(1, layers)
    ]
    for step, copy in enumerate(in_line):
        copy.wait_recv()
        total = total + line_slots[step + 1]
    gains_ref[...] = total
    if homes is not None:
        ffn_owned.arrive()
        attn_owned.arrive()
        ffn_owned.drain()
        attn_owned.drain()
        line.drain()
    for copy in in_plane + in_line:
        copy.wait_send()
    first.drain()


def last_step(part_in, x_own, grad_middle, gain_row, sums, columns, layers, weight_sums=()):
    rows, width = x_own.shape
    chips = columns // 2
    homes = None
    back_shapes, back_scratch = [], []
    if weight_sums:
        term, ffn_sum = weight_sums
        attn_rows = term.shape[0] // layers
        homes = Homes(layers, columns, attn_rows * layers * columns)
        back_shapes = [
            jax.ShapeDtypeStruct((attn_rows, width), BF),
            jax.ShapeDtypeStruct(ffn_sum.shape, BF),
        ]
        back_scratch = [
            pltpu.VMEM((attn_rows, width), BF),
            *LineReduce.scratch(layers, 3, attn_rows, width),
            *Exchange.scratch(),
            *Exchange.scratch(),
        ]
    return pl.pallas_call(
        functools.partial(last_kernel, columns, layers, homes),
        out_shape=(
            jax.ShapeDtypeStruct((rows, width), F32),
            jax.ShapeDtypeStruct((8, width), F32),
            *back_shapes,
        ),
        in_specs=vmem_specs(5 + len(weight_sums)),
        out_specs=tuple(vmem_specs(2) + [pl.BlockSpec(memory_space=pl.ANY)] * len(back_shapes)),
        scratch_shapes=[
            pltpu.VMEM((8, width), F32),
            pltpu.VMEM((columns, 8, width), F32),
            pltpu.VMEM((8, width), F32),
            pltpu.VMEM((layers, 8, width), F32),
            pltpu.SemaphoreType.DMA((columns,)),
            pltpu.SemaphoreType.DMA((columns,)),
            pltpu.SemaphoreType.DMA((layers,)),
            pltpu.SemaphoreType.DMA((layers,)),
            *Reduce.buffers(chips, rows, width),
            *Reduce.semaphores(chips),
            *back_scratch,
        ],
        compiler_params=comm_params(5),
        name="last_step",
        cost_estimate=pl.CostEstimate(flops=0, bytes_accessed=150_000_000, transcendentals=0),
    )(part_in, x_own, grad_middle, gain_row, sums, *weight_sums)


def turned(heads, low):
    return jnp.where(low, pltpu.roll(heads, LANES - HEAD_SIZE // 2, 1), pltpu.roll(heads, HEAD_SIZE // 2, 1))


def allowed_tile(start_ref, row_first, col_first):
    rows = row_first + lax.broadcasted_iota(jnp.int32, (TILE, TILE), 0)
    cols = col_first + lax.broadcasted_iota(jnp.int32, (TILE, TILE), 1)
    starts = jnp.broadcast_to(start_ref[row_first : row_first + TILE, 0:1], (TILE, TILE))
    return (cols <= rows) & (cols >= starts)


def place_tables(docs_ref, freq_ref, cos_ref, sin_ref, start_ref):
    blocks = docs_ref.shape[0]

    @pl.loop(0, blocks)
    def one_block(r):
        at = pl.ds(pl.multiple_of(r * LANES, LANES), LANES)
        mine = jnp.transpose(
            jnp.broadcast_to(docs_ref[pl.ds(r, 1), :].astype(F32), (LANES, LANES))
        )
        earlier = jnp.zeros((LANES, LANES), F32)
        for other in range(blocks):
            theirs = docs_ref[other : other + 1, :].astype(F32)
            earlier = earlier + jnp.where(theirs < mine, 1.0, 0.0)
        starts = jnp.broadcast_to(jnp.sum(earlier, axis=1, keepdims=True), (LANES, LANES))
        start_ref[at, :] = starts.astype(jnp.int32)
        token = r * LANES + lax.broadcasted_iota(jnp.int32, (LANES, LANES), 0)
        angles = (token.astype(F32) - starts) * freq_ref[...]
        lane = lax.broadcasted_iota(jnp.int32, (LANES, LANES), 1)
        sine = jnp.sin(angles)
        cos_ref[at, :] = jnp.where(lane < HEAD_SIZE, jnp.cos(angles), 0.0)
        sin_ref[at, :] = jnp.where(
            lane < HEAD_SIZE // 2, -sine, jnp.where(lane < HEAD_SIZE, sine, 0.0)
        )


def forward_kernel(columns, layers, heads, homes, aligned, *refs):
    (x_ref, gains_ref, docs_ref, freq_ref, dy_ref, attn_ref, ffn_ref), refs = refs[:7], refs[7:]
    (q_ref, k_ref, v_ref, att_ref, log_ref, pad_ref, middle_ref), refs = refs[:7], refs[7:]
    (cos_ref, sin_ref, start_ref, h_ref), refs = refs[:4], refs[4:]
    (h2_full, dy_full, ffn_col), refs = refs[:3], refs[3:]
    (part_ref, hidden, hidden_two, docs_full, ffn_bf, ffn_shard), refs = refs[:6], refs[6:]
    if aligned:
        (attn_bf, attn_shard, attn_col, *attn_scratch), refs = refs[:10], refs[10:]
    scratch = refs
    seq, own_rows, chips = h_ref.shape[0], x_ref.shape[0], columns // 2
    ffn_rows = ffn_ref.shape[0]
    if aligned:
        attn_rows = attn_ref.shape[0]

        @pl.loop(0, attn_rows // CHUNK)
        def cast_attn(k):
            attn_bf[chunk_rows(k), :] = attn_ref[chunk_rows(k), :].astype(BF)

        targets = homes.attn_targets()
        greet(columns, layers, [spot[:2] for spot in targets + homes.attn_owners()])
        unit = attn_rows // 3
        attn_spread = Exchange(
            [attn_bf.at[pl.ds(k * unit, unit), :] for k in range(3)],
            functools.partial(place_rows, attn_shard, unit),
            targets,
            attn_scratch[0:2],
        )
    else:
        greet(columns, layers)
    documents = Docs(docs_ref, docs_full, columns, scratch[0:3])

    @pl.loop(0, own_rows // CHUNK)
    def norm(k):
        residual = x_ref[chunk_rows(k), :].astype(F32)
        gain = 1.0 + gains_ref[0:1, :]
        hidden[chunk_rows(k), :] = (residual * rms_scale(residual) * gain).astype(BF)

    h_gather = Gather(hidden, h_ref, chips, scratch[3:8])

    @pl.loop(0, ffn_rows // CHUNK)
    def cast_ffn(k):
        ffn_bf[chunk_rows(k), :] = ffn_ref[chunk_rows(k), :].astype(BF)

    unit_ffn = ffn_rows // 3
    if aligned:
        attn_spread.arrive()
        attn_line = LineGather(attn_col, attn_shard, layers, 1, attn_scratch[2:7])
    ffn_spread = Exchange(
        [ffn_bf.at[pl.ds(k * unit_ffn, unit_ffn), :] for k in range(3)],
        functools.partial(place_rows, ffn_shard, unit_ffn),
        homes.ffn_targets(),
        scratch[8:10],
    )
    documents.finish()
    place_tables(docs_full, freq_ref, cos_ref, sin_ref, start_ref)
    if aligned:
        attn_line.relay(1)
    h_gather.pass_on()
    if aligned:
        attn_line.relay()
    ffn_spread.arrive()
    line = LineGather(ffn_col, ffn_shard, layers, 3, scratch[10:15])
    h_gather.finish()
    dy_gather = Gather(dy_ref, dy_full, chips, scratch[15:20])
    if aligned:
        attn_line.finish()
        w_ref = attn_col
    else:
        w_ref = attn_ref
    scale = HEAD_SIZE**-0.5
    for slot in range(2 * heads + 2):
        pad_ref[slot * LANES : slot * LANES + HEAD_SIZE, :] = w_ref[
            slot * HEAD_SIZE : (slot + 1) * HEAD_SIZE, :
        ]
        pad_ref[slot * LANES + HEAD_SIZE : (slot + 1) * LANES, :] = jnp.zeros(
            (LANES - HEAD_SIZE, w_ref.shape[1]), BF
        )
    width = (heads + 2) * LANES

    @pl.loop(0, seq // TILE)
    def project(i):
        at = pl.ds(pl.multiple_of(i * TILE, TILE), TILE)
        low = lax.broadcasted_iota(jnp.int32, (TILE, LANES), 1) < HEAD_SIZE // 2
        projected = product_transposed(h_ref[at, :], pad_ref[0:width, :])
        cosine, sine = cos_ref[at, :], sin_ref[at, :]
        for head in range(heads + 1):
            u = projected[:, head * LANES : (head + 1) * LANES]
            r = (u * cosine + turned(u, low) * sine).astype(BF)
            if head < heads:
                q_ref[at, head * LANES : (head + 1) * LANES] = r
            else:
                k_ref[at, :] = r
        v_ref[at, :] = projected[:, (heads + 1) * LANES :].astype(BF)

    for i in range(seq // TILE):
        rows = slice(i * TILE, (i + 1) * TILE)
        for head in range(heads):
            lanes = slice(head * LANES, (head + 1) * LANES)
            q = q_ref[rows, lanes]
            out = jnp.zeros((TILE, LANES), F32)
            total = jnp.zeros((TILE, 1), F32)
            for j in range(i + 1):
                keys = slice(j * TILE, (j + 1) * TILE)
                s = product_transposed(q, k_ref[keys, :]) * scale
                e = jnp.where(allowed_tile(start_ref, i * TILE, j * TILE), jnp.exp(s), 0.0)
                total = total + jnp.sum(e, axis=1, keepdims=True)
                out = out + plain_times(e.astype(BF), v_ref[keys, :])
            att_ref[rows, lanes] = (out / total).astype(BF)
            log_ref[rows, lanes] = jnp.broadcast_to(jnp.log(total), (TILE, LANES))

    @pl.loop(0, seq // TILE)
    def project_out(i):
        at = pl.ds(pl.multiple_of(i * TILE, TILE), TILE)
        part_ref[at, :] = plain_times(att_ref[at, :], pad_ref[width:, :]).astype(BF)

    reduce = Reduce(part_ref, chips, own_rows, scratch[20:22], scratch[22:26])
    line.relay(1)
    reduce.exchange()
    line.relay(1)
    dy_gather.pass_on()
    line.relay(1)
    reduce.arrive()

    @pl.loop(0, own_rows // CHUNK)
    def finish(k):
        at = chunk_rows(k)
        middle = x_ref[at, :].astype(F32) + reduce.total(k)
        middle_ref[at, :] = middle
        hidden_two[at, :] = (middle * rms_scale(middle) * (1.0 + gains_ref[1:2, :])).astype(BF)

    gather = Gather(hidden_two, h2_full, chips, scratch[26:31])
    line.relay(1)
    gather.pass_on()
    line.relay()
    gather.finish()
    dy_gather.finish()
    reduce.drain()
    line.finish()
    ffn_spread.drain()
    if aligned:
        attn_spread.drain()


def forward_step(x_own, gains, docs, dy_own, attn, ffn_weights, attn_total, heads, columns, layers, aligned):
    rows, width = x_own.shape
    seq = rows * columns
    chips = columns // 2
    ffn_rows = ffn_weights.shape[0]
    place = np.arange(LANES)
    frequency = np.where(
        place < HEAD_SIZE, ROPE_THETA ** (-2.0 * (place % (HEAD_SIZE // 2)) / HEAD_SIZE), 0.0
    ).astype(np.float32)[None, :]
    attn_scratch = []
    if aligned:
        attn_scratch = [
            pltpu.VMEM(attn.shape, BF),
            pltpu.VMEM(attn.shape, BF),
            pltpu.VMEM((layers * attn.shape[0], width), BF),
            *Exchange.scratch(),
            *LineGather.scratch(layers, 1),
        ]
    return pl.pallas_call(
        functools.partial(
            forward_kernel, columns, layers, heads, Homes(layers, columns, attn_total), aligned
        ),
        out_shape=(
            jax.ShapeDtypeStruct((seq, heads * LANES), BF),
            jax.ShapeDtypeStruct((seq, LANES), BF),
            jax.ShapeDtypeStruct((seq, LANES), BF),
            jax.ShapeDtypeStruct((seq, heads * LANES), BF),
            jax.ShapeDtypeStruct((seq, heads * LANES), F32),
            jax.ShapeDtypeStruct(((2 * heads + 2) * LANES, width), BF),
            jax.ShapeDtypeStruct((rows, width), F32),
            jax.ShapeDtypeStruct((seq, LANES), F32),
            jax.ShapeDtypeStruct((seq, LANES), F32),
            jax.ShapeDtypeStruct((seq, LANES), jnp.int32),
            jax.ShapeDtypeStruct((seq, width), BF),
            jax.ShapeDtypeStruct((seq, width), BF),
            jax.ShapeDtypeStruct((seq, width), BF),
            jax.ShapeDtypeStruct((layers * ffn_rows, width), BF),
        ),
        in_specs=vmem_specs(7),
        out_specs=tuple(vmem_specs(11) + [pl.BlockSpec(memory_space=pl.ANY)] * 3),
        scratch_shapes=[
            pltpu.VMEM((seq, width), BF),
            pltpu.VMEM((rows, width), BF),
            pltpu.VMEM((rows, width), BF),
            pltpu.VMEM((columns, rows), jnp.int32),
            pltpu.VMEM((ffn_rows, width), BF),
            pltpu.VMEM((ffn_rows, width), BF),
            *attn_scratch,
            *Docs.scratch(columns),
            *Gather.scratch(chips),
            *Exchange.scratch(),
            *LineGather.scratch(layers, 3),
            *Gather.scratch(chips),
            *Reduce.buffers(chips, rows, width),
            *Reduce.semaphores(chips),
            *Gather.scratch(chips),
        ],
        compiler_params=comm_params(3),
        name="forward_step",
        cost_estimate=pl.CostEstimate(flops=6_000_000_000, bytes_accessed=250_000_000, transcendentals=2_000_000),
    )(x_own, gains, docs, jnp.asarray(frequency), dy_own, attn, ffn_weights)


class Load:
    def __init__(self, source, target, sems, blocks=1):
        size = source.shape[0] // blocks
        self.copies = []
        for k in range(blocks):
            at = pl.ds(k * size, size)
            copy = pltpu.make_async_copy(source.at[at, :], target.at[at, :], sems.at[k])
            copy.start()
            self.copies.append(copy)
        self.next = 0

    def wait(self, count=None):
        stop = len(self.copies) if count is None else self.next + count
        for copy in self.copies[self.next : stop]:
            copy.wait()
        self.next = stop


def columns_of(width, most=512):
    return most, width // most


def backward_kernel(columns, layers, heads, sharers, factor, *refs):
    (h2_hbm, dy_hbm, w_hbm, h_hbm, pad_hbm), refs = refs[:5], refs[5:]
    (cos_hbm, sin_hbm, start_hbm, q_hbm, k_hbm, v_hbm, att_hbm, log_hbm), refs = refs[:8], refs[8:]
    (middle_ref, dy_ref, gain_ref), refs = refs[:3], refs[3:]
    (block_out_ref, grad_ref, sums_ref, ffn_sum, term_in, in_part), refs = refs[:6], refs[6:]
    (x_ref, y_ref, w_ref, pad_ref, cos_ref, sin_ref, start_ref), refs = refs[:7], refs[7:]
    (q_ref, k_ref, v_ref, att_ref, log_ref), refs = refs[:5], refs[5:]
    (act_ref, gg_ref, gu_ref, act_t, gg_t, gu_t, term, part_ref), refs = refs[:8], refs[8:]
    (gm_full, grad_bf, dk_ref, dv_ref, out_ref, out_t), refs = refs[:6], refs[6:]
    ga_ref, shared_ref = gg_ref.at[:, 0 : heads * LANES], act_ref.at[:, 0 : 2 * LANES]
    load_sems, store_sem, shared_send, shared_recv, *scratch = refs
    seq, own_rows, chips = gm_full.shape[0], middle_ref.shape[0], columns // 2
    hidden = w_ref.shape[0] // 3
    tiles = seq // TILE
    block, blocks = columns_of(w_ref.shape[1])
    w_load = Load(w_hbm, w_ref, load_sems.at[pl.ds(0, 3)], 3)
    h2_load = Load(h2_hbm, x_ref, load_sems.at[pl.ds(3, 1)])
    dy_load = Load(dy_hbm, y_ref, load_sems.at[pl.ds(4, 1)])
    later = [
        Load(source, target, load_sems.at[pl.ds(5 + k, 1)])
        for k, (source, target) in enumerate(
            (
                (pad_hbm, pad_ref),
                (cos_hbm, cos_ref),
                (sin_hbm, sin_ref),
                (start_hbm, start_ref),
                (q_hbm, q_ref),
                (k_hbm, k_ref),
                (v_hbm, v_ref),
                (att_hbm, att_ref),
                (log_hbm, log_ref),
            )
        )
    ]
    greet(columns, layers)
    w_gate, w_up, w_down = (pl.ds(k * hidden, hidden) for k in range(3))

    w_load.wait()
    h2_load.wait()
    dy_load.wait()

    @pl.loop(0, tiles)
    def feed_forward(i):
        at = pl.ds(pl.multiple_of(i * TILE, TILE), TILE)
        gate = product_transposed(x_ref[at, :], w_ref[w_gate, :])
        up = product_transposed(x_ref[at, :], w_ref[w_up, :])
        grad_act = product_transposed(y_ref[at, :], w_ref[w_down, :])
        sigmoid = 1.0 / (1.0 + jnp.exp(-gate))
        swish = gate * sigmoid
        act_ref[at, :] = (swish * up).astype(BF)
        gg_ref[at, :] = (grad_act * up * sigmoid * (1.0 + gate * (1.0 - sigmoid))).astype(BF)
        gu_ref[at, :] = (grad_act * swish).astype(BF)
        act_t[:, at] = jnp.transpose(act_ref[at, :])
        gg_t[:, at] = jnp.transpose(gg_ref[at, :])
        gu_t[:, at] = jnp.transpose(gu_ref[at, :])

    @pl.loop(0, blocks)
    def weight_gradients(j):
        at = pl.ds(pl.multiple_of(j * block, block), block)
        for rows, left, right in ((w_gate, gg_t, x_ref), (w_up, gu_t, x_ref), (w_down, act_t, y_ref)):
            term[rows, at] = (plain_times(left[...], right[:, at]) * factor).astype(BF)

    line = LineReduce(term, layers, 3, scratch[0:6])
    h_load = Load(h_hbm, x_ref, load_sems.at[pl.ds(14, 1)])

    @pl.loop(0, tiles)
    def back_part(i):
        at = pl.ds(pl.multiple_of(i * TILE, TILE), TILE)
        part_ref[at, :] = (
            plain_times(gg_ref[at, :], w_ref[w_gate, :]) + plain_times(gu_ref[at, :], w_ref[w_up, :])
        ).astype(BF)

    back = Reduce(part_ref, chips, own_rows, scratch[6:8], scratch[8:12])
    sums_ref[...] = jnp.zeros_like(sums_ref)

    @pl.loop(0, tiles)
    def out_part(i):
        at = pl.ds(pl.multiple_of(i * TILE, TILE), TILE)
        y_ref[at, :] = plain_times(act_ref[at, :], w_ref[w_down, :]).astype(BF)

    back.exchange()
    line.relay(2)
    back.arrive()
    back.drain()

    @pl.loop(0, own_rows // CHUNK)
    def turn(k):
        at = chunk_rows(k)
        grad_hidden = back.total(k)
        middle = middle_ref[at, :]
        scale = rms_scale(middle)
        normed = middle * scale
        sums_ref[0:1, :] += jnp.sum(grad_hidden * normed, axis=0, keepdims=True)
        grad = dy_ref[at, :].astype(F32) + norm_backward(grad_hidden, normed, scale, gain_ref[...])
        grad_ref[at, :] = grad
        grad_bf[at, :] = grad.astype(BF)

    gather = Gather(grad_bf, gm_full, chips, scratch[12:17])
    line.relay(1)
    gather.pass_on()
    line.relay(2)
    gather.finish()
    out = Reduce(y_ref, chips, own_rows, scratch[6:8], scratch[17:21])
    for load in later:
        load.wait()

    scale = HEAD_SIZE**-0.5
    width = (heads + 2) * LANES

    @pl.loop(0, tiles)
    def attended_gradient(i):
        at = pl.ds(pl.multiple_of(i * TILE, TILE), TILE)
        ga_ref[at, :] = product_transposed(gm_full[at, :], pad_ref[width:, :]).astype(BF)

    out.exchange()
    dk_ref[...] = jnp.zeros_like(dk_ref)
    dv_ref[...] = jnp.zeros_like(dv_ref)
    low = lax.broadcasted_iota(jnp.int32, (TILE, LANES), 1) < HEAD_SIZE // 2

    def turn_back(u, rows):
        return (u * cos_ref[rows, :] - turned(u, low) * sin_ref[rows, :]).astype(BF)

    for i in range(tiles):
        rows = slice(i * TILE, (i + 1) * TILE)
        for head in range(heads):
            lanes = slice(head * LANES, (head + 1) * LANES)
            q = q_ref[rows, lanes]
            ga = ga_ref[rows, lanes]
            delta = jnp.sum(ga.astype(F32) * att_ref[rows, lanes].astype(F32), axis=1, keepdims=True)
            logs = log_ref[rows, head * LANES : head * LANES + 1]
            dq = jnp.zeros((TILE, LANES), F32)
            for j in range(i + 1):
                keys = slice(j * TILE, (j + 1) * TILE)
                s = product_transposed(q, k_ref[keys, :]) * scale
                p = jnp.where(allowed_tile(start_ref, i * TILE, j * TILE), jnp.exp(s - logs), 0.0)
                dp = product_transposed(ga, v_ref[keys, :])
                ds = (p * (dp - delta) * scale).astype(BF)
                dq = dq + plain_times(ds, k_ref[keys, :])
                dk_ref[keys, :] += transposed_times(ds, q)
                dv_ref[keys, :] += transposed_times(p.astype(BF), ga)
            out_ref[rows, lanes] = turn_back(dq, rows)
        if i == tiles // 2:
            line.relay(1)
    line.relay(1)
    for i in range(tiles):
        rows = slice(i * TILE, (i + 1) * TILE)
        out_ref[rows, heads * LANES : (heads + 1) * LANES] = turn_back(dk_ref[rows, :], rows)
        out_ref[rows, (heads + 1) * LANES :] = dv_ref[rows, :].astype(BF)
    if sharers > 1:
        me = lax.axis_index("context")
        both = pl.ds(heads * LANES, 2 * LANES)
        copy = send(
            out_ref.at[:, both], shared_ref, shared_send, shared_recv, {"context": sibling_of(me)}
        )
        copy.wait()
        lane = lax.broadcasted_iota(jnp.int32, (TILE, 2 * LANES), 1) % LANES
        kept = lane // (HEAD_SIZE // sharers) == lax.rem(me, 2)
        for i in range(tiles):
            rows = slice(i * TILE, (i + 1) * TILE)
            value = out_ref[rows, both].astype(F32) + shared_ref[rows, :].astype(F32)
            out_ref[rows, both] = jnp.where(kept, value, 0.0).astype(BF)
    for i in range(tiles):
        rows = slice(i * TILE, (i + 1) * TILE)
        out_t[0:width, rows] = jnp.transpose(out_ref[rows, :])
        out_t[width:, rows] = jnp.transpose(att_ref[rows, :])

    @pl.loop(0, tiles)
    def input_part(i):
        at = pl.ds(pl.multiple_of(i * TILE, TILE), TILE)
        part_ref[at, :] = plain_times(out_ref[at, :], pad_ref[0:width, :]).astype(BF)

    store = pltpu.make_async_copy(part_ref, in_part, store_sem)
    store.start()
    h_load.wait()

    @pl.loop(0, blocks)
    def attention_gradients(j):
        at = pl.ds(pl.multiple_of(j * block, block), block)
        inner = (plain_times(out_t[0:width, :], x_ref[:, at]) * factor).astype(BF)
        outer = (plain_times(out_t[width:, :], gm_full[:, at]) * factor).astype(BF)
        for value, first, count in ((inner, 0, heads + 2), (outer, heads + 2, heads)):
            for k in range(count):
                if sharers > 1:
                    term_in[pl.ds((first + k) * LANES, LANES), at] = value[k * LANES : (k + 1) * LANES, :]
                else:
                    term_in[pl.ds((first + k) * HEAD_SIZE, HEAD_SIZE), at] = value[
                        k * LANES : k * LANES + HEAD_SIZE, :
                    ]

    out.arrive()

    @pl.loop(0, own_rows // CHUNK)
    def finish_out(k):
        at = chunk_rows(k)
        block_out_ref[at, :] = middle_ref[at, :] + out.total(k)

    line.finish(ffn_sum)
    store.wait()
    line.drain()
    out.drain()


def backward_step(
    h2_full, dy_full, ffn_col, h_full, padded, tables, saved, middle, dy_own, gain_row, heads, columns, layers, sharers
):
    seq, width = h2_full.shape
    rows = seq // columns
    chips = columns // 2
    hidden = ffn_col.shape[0] // 3
    ffn_rows = ffn_col.shape[0] // layers
    each = HEAD_SIZE if sharers == 1 else LANES
    loaded = [ffn_col, padded, *tables, *saved]
    return pl.pallas_call(
        functools.partial(
            backward_kernel, columns, layers, heads, sharers, float(seq * layers) ** (-0.5)
        ),
        out_shape=(
            jax.ShapeDtypeStruct((rows, width), F32),
            jax.ShapeDtypeStruct((rows, width), F32),
            jax.ShapeDtypeStruct((8, width), F32),
            jax.ShapeDtypeStruct((ffn_rows, width), BF),
            jax.ShapeDtypeStruct(((2 * heads + 2) * each, width), BF),
            jax.ShapeDtypeStruct((seq, width), BF),
        ),
        in_specs=[pl.BlockSpec(memory_space=pl.ANY)] * 13 + vmem_specs(3),
        out_specs=tuple(vmem_specs(5) + [pl.BlockSpec(memory_space=pl.ANY)]),
        scratch_shapes=[
            pltpu.VMEM((seq, width), BF),
            pltpu.VMEM((seq, width), BF),
            *[pltpu.VMEM(array.shape, array.dtype) for array in loaded],
            *[pltpu.VMEM((seq, hidden), BF)] * 3,
            *[pltpu.VMEM((hidden, seq), BF)] * 3,
            pltpu.VMEM(ffn_col.shape, BF),
            pltpu.VMEM((seq, width), BF),
            pltpu.VMEM((seq, width), BF),
            pltpu.VMEM((rows, width), BF),
            pltpu.VMEM((seq, LANES), F32),
            pltpu.VMEM((seq, LANES), F32),
            pltpu.VMEM((seq, (heads + 2) * LANES), BF),
            pltpu.VMEM(((2 * heads + 2) * LANES, seq), BF),
            pltpu.SemaphoreType.DMA((15,)),
            pltpu.SemaphoreType.DMA,
            pltpu.SemaphoreType.DMA,
            pltpu.SemaphoreType.DMA,
            *LineReduce.scratch(layers, 3, ffn_rows, width),
            *Reduce.buffers(chips, rows, width),
            *Reduce.semaphores(chips),
            *Gather.scratch(chips),
            *Reduce.semaphores(chips),
        ],
        compiler_params=comm_params(4),
        name="backward_step",
        cost_estimate=pl.CostEstimate(flops=28_000_000_000, bytes_accessed=150_000_000, transcendentals=4_000_000),
    )(h2_full, dy_full, ffn_col, h_full, padded, *tables, *saved, middle, dy_own, gain_row)


def update_rows(g_ref, p_ref, m_ref, grad_ref, new_p_ref, new_m_ref):
    gradient = g_ref[...].astype(F32)
    grad_ref[...] = gradient
    parameter = p_ref[...]
    first_moment = BETA_ONE * m_ref[0] + (1.0 - BETA_ONE) * gradient
    second_moment = BETA_TWO * m_ref[1] + (1.0 - BETA_TWO) * gradient * gradient
    new_m_ref[0] = first_moment
    new_m_ref[1] = second_moment
    below = jnp.sqrt(second_moment * (1.0 / (1.0 - BETA_TWO**STEP))) + ADAM_EPS
    step = first_moment * (LEARN_RATE / (1.0 - BETA_ONE**STEP)) / below
    new_p_ref[...] = parameter * (1.0 - LEARN_RATE * WEIGHT_DECAY) - step


def update_kernel(steps, *refs):
    first = pl.program_id(0) < steps

    @pl.when(first)
    def one():
        update_rows(*refs[0:3], *refs[6:9])

    @pl.when(jnp.logical_not(first))
    def other():
        update_rows(*refs[3:6], *refs[9:12])


def update_all(first, second):
    specs, shapes = [], []
    blocks = []
    for gradient, parameter, _ in (first, second):
        rows = parameter.shape[0]
        whole = [n for n in (48, 32) if rows % n == 0]
        blocks.append(whole[0] if whole else rows)
    steps = first[1].shape[0] // blocks[0]
    rest = second[1].shape[0] // blocks[1]
    for block, place, (_, parameter, _) in (
        (blocks[0], lambda i: jnp.minimum(i, steps - 1), first),
        (blocks[1], lambda i: jnp.maximum(i - steps, 0), second),
    ):
        rows, width = parameter.shape
        flat = pl.BlockSpec((block, width), lambda i, place=place: (place(i), 0))
        pair = pl.BlockSpec((2, block, width), lambda i, place=place: (0, place(i), 0))
        specs.append([flat, flat, pair])
        shapes += [
            jax.ShapeDtypeStruct((rows, width), F32),
            jax.ShapeDtypeStruct((rows, width), F32),
            jax.ShapeDtypeStruct((2, rows, width), F32),
        ]
    out = pl.pallas_call(
        functools.partial(update_kernel, steps),
        grid=(steps + rest,),
        out_shape=tuple(shapes),
        in_specs=specs[0] + specs[1],
        out_specs=tuple(specs[0] + specs[1]),
        compiler_params=pltpu.CompilerParams(vmem_limit_bytes=VMEM_LIMIT),
        name="update_all",
        cost_estimate=pl.CostEstimate(flops=20_000_000, bytes_accessed=25_000_000, transcendentals=1_000_000),
    )(*first, *second)
    return out[:3], out[3:]


def unpadded(rows, count):
    return jnp.concatenate([rows[k * LANES : k * LANES + HEAD_SIZE] for k in range(count)])


def on_device(
    block_input,
    cotangent,
    documents,
    attn_weights,
    ffn_weights,
    norm_gains,
    attn_moments,
    ffn_moments,
    gain_moments,
):
    layers, columns = lax.axis_size("fsdp"), lax.axis_size("context")
    rows, width = block_input.shape[1:]
    seq = rows * columns
    heads = QUERY_HEADS // columns
    sharers = max(1, columns // KEY_VALUE_HEADS)
    share = KEY_VALUE_HEADS * HEAD_SIZE // columns
    grad_factor = float(rows * layers * columns) ** (-0.5)
    attn_plan, ffn_plan = unit_plans(layers, columns, attn_weights.shape[0] * layers * columns)
    core = lax.rem(lax.axis_index("context"), 2)
    swap = [(c, c + 1 - 2 * (c % 2)) for c in range(columns)]

    x_own, dy_own = block_input[0], cotangent[0]
    attn_total = attn_weights.shape[0] * layers * columns
    aligned = attn_weights.shape[0] % (3 * CHUNK) == 0
    attn_source = attn_weights
    if not aligned:
        attn_col = lax.all_gather(
            attn_plan.spread(attn_weights.astype(BF)), "fsdp", axis=0, tiled=True
        )
        if sharers > 1:
            query_rows = heads * HEAD_SIZE
            own_part = attn_col[query_rows : query_rows + 2 * share]
            other = lax.ppermute(own_part, "context", swap)

            def whole_head(first):
                mine, theirs = own_part[first : first + share], other[first : first + share]
                return jnp.where(
                    core == 0, jnp.concatenate([mine, theirs]), jnp.concatenate([theirs, mine])
                )

            attn_col = jnp.concatenate(
                [
                    attn_col[:query_rows],
                    whole_head(0),
                    whole_head(share),
                    attn_col[query_rows + 2 * share :],
                ]
            )
        attn_source = attn_col
    *saved, padded, middle, cosine, sine, starts, h_full, h2_full, dy_full, ffn_col = forward_step(
        x_own, norm_gains, documents, dy_own, attn_source, ffn_weights, attn_total, heads, columns, layers, aligned
    )
    tables = (cosine, sine, starts)

    block_out, grad_middle, sums, ffn_sum, attn_term, in_part = backward_step(
        h2_full,
        dy_full,
        ffn_col,
        h_full,
        padded,
        tables,
        saved,
        middle,
        dy_own,
        norm_gains[1:2],
        heads,
        columns,
        layers,
        sharers,
    )
    if sharers > 1:
        own_rows = [
            lax.dynamic_slice_in_dim(attn_term, (heads + k) * LANES + core * share, share, 0)
            for k in range(2)
        ]
        attn_term = jnp.concatenate(
            [
                unpadded(attn_term, heads),
                *own_rows,
                unpadded(attn_term[(heads + 2) * LANES :], heads),
            ]
        )
    last_args = (in_part, x_own, grad_middle, norm_gains[0:1], sums, columns, layers)
    if aligned:
        grad_input, gain_sums, attn_shard, ffn_shard = last_step(*last_args, (attn_term, ffn_sum))
    else:
        attn_sum = lax.psum_scatter(attn_term, "fsdp", scatter_dimension=0, tiled=True)
        grad_input, gain_sums = last_step(*last_args)
        ffn_shard = ffn_plan.collect(ffn_sum)
        attn_shard = attn_plan.collect(attn_sum)

    column_count = width // (layers * columns)
    first_column = lax.axis_index(EVERY) * column_count
    gain_shard = lax.dynamic_slice_in_dim(gain_sums[:2], first_column, column_count, 1) * grad_factor
    own_gains = lax.dynamic_slice_in_dim(norm_gains, first_column, column_count, 1)
    (ffn_shard, new_ffn, ffn_states), (attn_shard, new_attn, attn_states) = update_all(
        (ffn_shard, ffn_weights, ffn_moments), (attn_shard, attn_weights, attn_moments)
    )
    new_gains, gain_states = adamw_update(own_gains, gain_shard, gain_moments, 0.0)
    return (
        block_out[None],
        grad_input[None],
        attn_shard,
        ffn_shard,
        gain_shard,
        new_attn,
        new_ffn,
        new_gains,
        attn_states,
        ffn_states,
        jnp.stack(gain_states),
    )


def solution(mesh):
    placed = (
        P("fsdp", "context", None),
        P("fsdp", "context", None),
        P("fsdp", "context"),
        P(EVERY, None),
        P(EVERY, None),
        P(),
        P(None, EVERY, None),
        P(None, EVERY, None),
        P(None, None, EVERY),
    )
    return jax.shard_map(
        on_device,
        mesh=mesh,
        in_specs=placed,
        out_specs=(
            P("fsdp", "context", None),
            P("fsdp", "context", None),
            P(EVERY, None),
            P(EVERY, None),
            P(None, EVERY),
            P(EVERY, None),
            P(EVERY, None),
            P(None, EVERY),
            P(None, EVERY, None),
            P(None, EVERY, None),
            P(None, None, EVERY),
        ),
        check_vma=False,
    )
```

```python
import functools

import jax
import jax.numpy as jnp
import numpy as np
from jax import lax
from jax.experimental import pallas as pl
from jax.experimental.pallas import tpu as pltpu
from jax.sharding import PartitionSpec as P

QUERY_HEADS = 16
KEY_VALUE_HEADS = 8
HEAD_SIZE = 96
STEP = 3

NORM_EPS = 1e-05
ROPE_THETA = 100000.0
BETA_ONE = 0.9
BETA_TWO = 0.95
ADAM_EPS = 1e-08
LEARN_RATE = 0.02
WEIGHT_DECAY = 0.1

LANES = 128
TILE = 256
CHUNK = 16
VMEM_LIMIT = 67_000_000
EVERY = ("fsdp", "context")
BF = jnp.bfloat16
F32 = jnp.float32
ID_TYPE = pl.DeviceIdType.MESH


def product_transposed(left_matrix, right_matrix):
    return lax.dot_general(
        left_matrix, right_matrix, (((1,), (1,)), ((), ())), preferred_element_type=F32
    )


def transposed_times(left_matrix, right_matrix):
    return lax.dot_general(
        left_matrix, right_matrix, (((0,), (0,)), ((), ())), preferred_element_type=F32
    )


def plain_times(left_matrix, right_matrix):
    return jnp.dot(left_matrix, right_matrix, preferred_element_type=F32)


def rms_scale(tensor_in):
    return lax.rsqrt(jnp.mean(tensor_in * tensor_in, axis=-1, keepdims=True) + NORM_EPS)


def norm_backward(grad_in, normed, norm_scale, gain_row):
    scaled = grad_in * (1.0 + gain_row)
    return norm_scale * (scaled - normed * jnp.mean(scaled * normed, axis=-1, keepdims=True))


def adamw_update(parameter, gradient, moments, decay_rate):
    first_moment = BETA_ONE * moments[0] + (1.0 - BETA_ONE) * gradient
    second_moment = BETA_TWO * moments[1] + (1.0 - BETA_TWO) * gradient * gradient
    first_hat = first_moment / (1.0 - BETA_ONE**STEP)
    second_hat = second_moment / (1.0 - BETA_TWO**STEP)
    updated = parameter - LEARN_RATE * (
        first_hat / (jnp.sqrt(second_hat) + ADAM_EPS) + decay_rate * parameter
    )
    return (updated, (first_moment, second_moment))


class UnitPlan:
    def __init__(self, homes, devices):
        waiting = [[] for _ in range(devices)]
        for unit, (device, place) in enumerate(homes):
            waiting[unit // 3].append((unit % 3, device, place))
        self.rounds = []
        for _ in range(3):
            taken = [None] * devices

            def settle(source, seen):
                for piece, device, place in waiting[source]:
                    if device in seen:
                        continue
                    seen.add(device)
                    if taken[device] is None or settle(taken[device][0], seen):
                        taken[device] = (source, piece, place)
                        return True
                return False

            for source in range(devices):
                if not settle(source, set()):
                    raise ValueError("no matching")
            pairs, pieces, places = [], [0] * devices, [0] * devices
            for device, (source, piece, place) in enumerate(taken):
                pairs.append((source, device))
                pieces[source] = piece
                places[device] = place
                waiting[source].remove((piece, device, place))
            self.rounds.append((pairs, np.array(pieces), np.array(places)))

    def _reorder(self, got, columns):
        order = np.argsort(np.stack(columns, axis=1), axis=1).astype(np.int32)
        mine = jnp.asarray(order)[lax.axis_index(EVERY)]
        stacked = jnp.stack(got)
        return jnp.concatenate(
            [lax.dynamic_index_in_dim(stacked, mine[k], 0, keepdims=False) for k in range(3)]
        )

    def spread(self, rows):
        pieces = rows.reshape(3, rows.shape[0] // 3, rows.shape[1])
        me = lax.axis_index(EVERY)
        got = []
        for pairs, piece, _ in self.rounds:
            unit = lax.dynamic_index_in_dim(
                pieces, jnp.asarray(piece, jnp.int32)[me], 0, keepdims=False
            )
            got.append(lax.ppermute(unit, EVERY, pairs))
        return self._reorder(got, [place for _, _, place in self.rounds])

    def collect(self, rows):
        places_of = rows.reshape(3, rows.shape[0] // 3, rows.shape[1])
        me = lax.axis_index(EVERY)
        got = []
        for pairs, _, place in self.rounds:
            unit = lax.dynamic_index_in_dim(
                places_of, jnp.asarray(place, jnp.int32)[me], 0, keepdims=False
            )
            got.append(lax.ppermute(unit, EVERY, [(b, a) for a, b in pairs]))
        return self._reorder(got, [piece for _, piece, _ in self.rounds])


def unit_plans(layers, columns, attn_rows):
    devices = layers * columns

    def home(column, position):
        return ((position // 3) * columns + column, position % 3)

    homes = []
    for unit in range(3 * devices):
        matrix, rest = divmod(unit, devices)
        stretch, column = divmod(rest, columns)
        homes.append(home(column, matrix * layers + stretch))
    ffn_plan = UnitPlan(homes, devices)
    unit_rows = attn_rows // (3 * devices)
    query_units = QUERY_HEADS * HEAD_SIZE // columns // unit_rows
    share_units = KEY_VALUE_HEADS * HEAD_SIZE // columns // unit_rows
    homes = []
    position = 0
    for count in (query_units, share_units, share_units, query_units):
        for column in range(columns):
            for k in range(count):
                homes.append(home(column, position + k))
        position += count
    return UnitPlan(homes, devices), ffn_plan


class Homes:
    def __init__(self, layers, columns, attn_rows):
        devices = layers * columns
        unit_rows = attn_rows // (3 * devices)
        self.layers, self.columns = layers, columns
        self.counts = [
            QUERY_HEADS * HEAD_SIZE // columns // unit_rows,
            KEY_VALUE_HEADS * HEAD_SIZE // columns // unit_rows,
        ]
        query, share = self.counts
        self.first = [0, query, query + share, query + 2 * share]
        self.sizes = [query, share, share, query]

    def _spot(self, column, position):
        return position // 3, column, position % 3

    def _column(self, group):
        half = self.columns // 2
        return group % half * 2 + group // half

    def _group(self, column):
        return column % 2 * (self.columns // 2) + column // 2

    def attn_targets(self):
        device = lax.axis_index("fsdp") * self.columns + lax.axis_index("context")
        found = []
        for piece in range(3):
            unit = device * 3 + piece
            column, position = 0, 0
            for first, size in zip(self.first, self.sizes):
                inside = unit - first * self.columns
                begun = inside >= 0
                column = jnp.where(begun, self._column(inside // size), column)
                position = jnp.where(begun, first + inside % size, position)
            found.append(self._spot(column, position))
        return found

    def attn_owners(self):
        group = self._group(lax.axis_index("context"))
        found = []
        for place in range(3):
            position = lax.axis_index("fsdp") * 3 + place
            unit = 0
            for first, size in zip(self.first, self.sizes):
                inside = position - first
                unit = jnp.where(inside >= 0, first * self.columns + group * size + inside, unit)
            device = unit // 3
            found.append((device // self.columns, device % self.columns, unit % 3))
        return found

    def ffn_targets(self):
        layer, column = lax.axis_index("fsdp"), lax.axis_index("context")
        return [
            (layer, (3 * column + piece) % self.columns, (3 * column + piece) // self.columns)
            for piece in range(3)
        ]

    def ffn_owners(self):
        layer, column = lax.axis_index("fsdp"), lax.axis_index("context")
        return [
            (layer, (place * self.columns + column) // 3, (place * self.columns + column) % 3)
            for place in range(3)
        ]


def partner(me, step, chips):
    return lax.rem(me // 2 + step, chips) * 2 + lax.rem(me, 2)


def sibling_of(me):
    return me + 1 - 2 * lax.rem(me, 2)


def rows_at(index, rows):
    return pl.ds(pl.multiple_of(index * rows, rows), rows)


def greet(columns, layers=1, others=()):
    barrier = pltpu.get_barrier_semaphore()
    me = lax.axis_index("context")
    awaited = columns - 1 + layers - 1
    for layer, column in others:
        apart = (layer != lax.axis_index("fsdp")) | (column != me)
        awaited = awaited + jnp.where(apart, 1, 0)

        @pl.when(apart)
        def there():
            pl.semaphore_signal(
                barrier, inc=1, device_id={"fsdp": layer, "context": column}, device_id_type=ID_TYPE
            )

    for step in range(1, columns):
        pl.semaphore_signal(
            barrier, inc=1, device_id={"context": lax.rem(me + step, columns)}, device_id_type=ID_TYPE
        )
    if layers > 1:
        layer = lax.axis_index("fsdp")
        for step in range(1, layers):
            pl.semaphore_signal(
                barrier, inc=1, device_id={"fsdp": lax.rem(layer + step, layers)}, device_id_type=ID_TYPE
            )
    pl.semaphore_wait(barrier, awaited)


def send(source, target, send_sem, recv_sem, device):
    copy = pltpu.make_async_remote_copy(
        src_ref=source,
        dst_ref=target,
        send_sem=send_sem,
        recv_sem=recv_sem,
        device_id=device,
        device_id_type=ID_TYPE,
    )
    copy.start()
    return copy


def remote(source, target, send_sem, recv_sem, device):
    return pltpu.make_async_remote_copy(
        src_ref=source,
        dst_ref=target,
        send_sem=send_sem,
        recv_sem=recv_sem,
        device_id=device,
        device_id_type=ID_TYPE,
    )


class Exchange:
    @staticmethod
    def scratch():
        return [pltpu.SemaphoreType.DMA((3,)), pltpu.SemaphoreType.DMA((3,))]

    def __init__(self, sources, targets, homes, sems):
        send_sem, recv_sem = sems
        self.parts = []
        for i, (layer, column, place) in enumerate(homes):
            itself = (layer == lax.axis_index("fsdp")) & (column == lax.axis_index("context"))
            target = targets(layer, place)
            copy = functools.partial(
                remote,
                sources[i],
                target,
                send_sem.at[i],
                recv_sem.at[place],
                {"fsdp": layer, "context": column},
            )
            stay = functools.partial(pltpu.make_async_copy, sources[i], target, recv_sem.at[place])

            @pl.when(itself)
            def here():
                stay().start()

            @pl.when(jnp.logical_not(itself))
            def there():
                copy().start()

            self.parts.append((itself, copy))
        self.landing = [
            functools.partial(pltpu.make_async_copy, sources[k], sources[k], recv_sem.at[k])
            for k in range(3)
        ]

    def arrive(self):
        for landed in self.landing:
            landed().wait()

    def drain(self):
        for itself, copy in self.parts:

            @pl.when(jnp.logical_not(itself))
            def sent():
                copy().wait_send()


class LineGather:
    @staticmethod
    def scratch(layers, pieces):
        return [*[pltpu.SemaphoreType.DMA(((layers - 1) * pieces,))] * 4, pltpu.SemaphoreType.DMA]

    def __init__(self, full, own, layers, pieces, sems):
        self.full, self.own, self.layers, self.pieces = full, own, layers, pieces
        *self.sems, local_sem = sems
        self.rows = own.shape[0]
        self.size = self.rows // pieces
        self.count = (layers - 1) * pieces
        self.local = pltpu.make_async_copy(
            own, full.at[rows_at(lax.axis_index("fsdp"), self.rows), :], local_sem
        )
        for m in range(pieces):
            self._send(m)
        self.local.start()
        self.next = pieces

    def _block(self, shard, piece):
        first = pl.multiple_of(shard * self.rows + piece * self.size, self.size)
        return self.full.at[pl.ds(first, self.size), :]

    def _moves(self, m):
        k, piece = divmod(m, self.pieces)
        layer = lax.axis_index("fsdp")
        up_send, up_recv, down_send, down_recv = self.sems
        top = self.layers - 1
        for first, last, other, shard, send_sem, recv_sem in (
            (layer - k >= 0, layer < top, layer + 1, layer - k, up_send, up_recv),
            (layer + k <= top, layer > 0, layer - 1, layer + k, down_send, down_recv),
        ):
            block = self._block(shard, piece)
            source = self.own.at[pl.ds(piece * self.size, self.size), :] if k == 0 else block
            yield first & last, functools.partial(
                remote, source, block, send_sem.at[m], recv_sem.at[m], {"fsdp": other}
            )

    def _send(self, m):
        for go, copy in self._moves(m):

            @pl.when(go)
            def start():
                copy().start()

    def _land(self, m):
        k, piece = divmod(m, self.pieces)
        layer = lax.axis_index("fsdp")
        _, up_recv, _, down_recv = self.sems
        for there, shard, recv_sem in (
            (layer - 1 - k >= 0, layer - 1 - k, up_recv),
            (layer + 1 + k <= self.layers - 1, layer + 1 + k, down_recv),
        ):
            block = self._block(shard, piece)
            copy = functools.partial(pltpu.make_async_copy, block, block, recv_sem.at[m])

            @pl.when(there)
            def landed():
                copy().wait()

    def relay(self, count=None):
        stop = self.count if count is None else min(self.count, self.next + count)
        for m in range(self.next, stop):
            self._land(m - self.pieces)
            self._send(m)
        self.next = stop

    def finish(self):
        self.relay()
        for m in range(self.count - self.pieces, self.count):
            self._land(m)
        for m in range(self.count):
            for go, copy in self._moves(m):

                @pl.when(go)
                def sent():
                    copy().wait_send()

        self.local.wait()


class LineReduce:
    @staticmethod
    def scratch(layers, pieces, rows, width):
        count = (layers - 1) * pieces
        return [
            pltpu.VMEM((count, rows // pieces, width), BF),
            pltpu.VMEM((count, rows // pieces, width), BF),
            *[pltpu.SemaphoreType.DMA((count,))] * 4,
        ]

    def __init__(self, term, layers, pieces, scratch):
        self.term, self.layers, self.pieces = term, layers, pieces
        self.rows = term.shape[0] // layers
        self.size = self.rows // pieces
        self.up_in, self.down_in, *self.sems = scratch
        self.count = (layers - 1) * pieces
        self.slots = self.count + layers - 1
        self.next = 1
        layer = lax.axis_index("fsdp")
        top = layers - 1

        @pl.when(layer == 0)
        def bottom():
            for m in range(self.count):
                self._up(m, self._block(top - m // pieces, m % pieces)).start()

        @pl.when(layer == top)
        def ceiling():
            for m in range(self.count):
                self._down(m, self._block(m // pieces, m % pieces)).start()

    def _block(self, target, piece):
        return self.term.at[pl.ds(target * self.rows + piece * self.size, self.size), :]

    def _up(self, m, source):
        up_send, up_recv, _, _ = self.sems
        other = {"fsdp": lax.axis_index("fsdp") + 1}
        return remote(source, self.up_in.at[m], up_send.at[m], up_recv.at[m], other)

    def _down(self, m, source):
        _, _, down_send, down_recv = self.sems
        other = {"fsdp": lax.axis_index("fsdp") - 1}
        return remote(source, self.down_in.at[m], down_send.at[m], down_recv.at[m], other)

    def _add(self, sums, m, target):
        first = pl.multiple_of(target * self.rows + m % self.pieces * self.size, CHUNK)

        @pl.loop(0, self.size // CHUNK)
        def add(c):
            at = chunk_rows(c)
            of_term = pl.ds(pl.multiple_of(first + c * CHUNK, CHUNK), CHUNK)
            sums[m, at, :] = (
                sums[m, at, :].astype(F32) + self.term[of_term, :].astype(F32)
            ).astype(BF)

    def _slot(self, slot):
        layer = lax.axis_index("fsdp")
        top = self.layers - 1
        _, up_recv, _, down_recv = self.sems
        m = slot - layer
        target = top - m // self.pieces

        @pl.when((layer > 0) & (m >= 0) & (m < self.count) & (layer <= target))
        def from_below():
            pltpu.make_async_copy(self.up_in.at[m], self.up_in.at[m], up_recv.at[m]).wait()

            @pl.when(layer < target)
            def pass_up():
                self._add(self.up_in, m, target)
                self._up(m, self.up_in.at[m]).start()

        n = slot - (top - layer)
        goal = n // self.pieces

        @pl.when((layer < top) & (n >= 0) & (n < self.count) & (layer >= goal))
        def from_above():
            pltpu.make_async_copy(self.down_in.at[n], self.down_in.at[n], down_recv.at[n]).wait()

            @pl.when(layer > goal)
            def pass_down():
                self._add(self.down_in, n, goal)
                self._down(n, self.down_in.at[n]).start()

    def relay(self, count=None):
        stop = self.slots if count is None else min(self.slots, self.next + count)
        if stop > self.next:

            @pl.loop(self.next, stop)
            def slots(slot):
                self._slot(slot)

        self.next = stop

    def finish(self, total):
        self.relay()
        layer = lax.axis_index("fsdp")
        top = self.layers - 1
        for own in range(self.layers):

            @pl.when(layer == own)
            def here():
                for piece in range(self.pieces):

                    @pl.loop(0, self.size // CHUNK)
                    def add(c):
                        start = pl.multiple_of(c * CHUNK, CHUNK)
                        at = pl.ds(start, CHUNK)
                        value = self.term[
                            pl.ds(own * self.rows + piece * self.size + start, CHUNK), :
                        ].astype(F32)
                        if own > 0:
                            m = (top - own) * self.pieces + piece
                            value = value + self.up_in[m, at, :].astype(F32)
                        if own < top:
                            m = own * self.pieces + piece
                            value = value + self.down_in[m, at, :].astype(F32)
                        total[pl.ds(piece * self.size + start, CHUNK), :] = value.astype(BF)

    def drain(self):
        layer = lax.axis_index("fsdp")
        top = self.layers - 1
        for m in range(self.count):
            k = m // self.pieces

            @pl.when(layer < top - k)
            def up():
                self._up(m, self.up_in.at[m]).wait_send()

            @pl.when(layer > k)
            def down():
                self._down(m, self.down_in.at[m]).wait_send()


class Gather:
    @staticmethod
    def scratch(chips):
        return [
            pltpu.SemaphoreType.DMA((chips,)),
            pltpu.SemaphoreType.DMA((chips,)),
            pltpu.SemaphoreType.DMA((chips,)),
            pltpu.SemaphoreType.DMA((chips,)),
            pltpu.SemaphoreType.DMA,
        ]

    def __init__(self, block, full, chips, sems):
        own_send, own_recv, self.on_send, self.on_recv, local_sem = sems
        me = lax.axis_index("context")
        rows = block.shape[0]
        self.block, self.full, self.chips, self.me, self.rows = block, full, chips, me, rows
        mine = full.at[rows_at(me, rows), :]
        self.own = [
            send(block, mine, own_send.at[step], own_recv.at[step], {"context": partner(me, step, chips)})
            for step in range(1, chips)
        ]
        self.own.append(
            send(block, mine, own_send.at[0], own_recv.at[0], {"context": sibling_of(me)})
        )
        self.local = pltpu.make_async_copy(block, mine, local_sem)
        self.local.start()

        self.passed = []

    def pass_on(self):
        for step in range(1, self.chips):
            self.own[step - 1].wait_recv()
            source = partner(self.me, self.chips - step, self.chips)
            there = self.full.at[rows_at(source, self.rows), :]
            self.passed.append(
                send(there, there, self.on_send.at[step], self.on_recv.at[step], {"context": sibling_of(self.me)})
            )

    def finish(self):
        if not self.passed:
            self.pass_on()
        self.own[-1].wait_recv()
        for copy in self.passed:
            copy.wait_recv()
        for copy in self.own + self.passed:
            copy.wait_send()
        self.local.wait()


class Reduce:
    @staticmethod
    def buffers(chips, rows, width):
        return [pltpu.VMEM((chips * rows, width), BF), pltpu.VMEM(((chips - 1) * rows, width), BF)]

    @staticmethod
    def semaphores(chips):
        return [pltpu.SemaphoreType.DMA((chips,))] * 4

    def __init__(self, part, chips, rows, buffers, semaphores):
        self.near, self.far = buffers
        near_send, near_recv, self.far_send, self.far_recv = semaphores
        me = lax.axis_index("context")
        self.part, self.chips, self.rows, self.me = part, chips, rows, me
        self.near_copies = {}
        for step in [*range(1, chips), 0]:
            block = partner(sibling_of(me), step, chips)
            self.near_copies[step] = send(
                part.at[rows_at(block, rows), :],
                self.near.at[pl.ds(step * rows, rows), :],
                near_send.at[step],
                near_recv.at[step],
                {"context": sibling_of(me)},
            )
        self.far_copies = []

    def exchange(self):
        for step in range(1, self.chips):
            self.near_copies[step].wait_recv()
            target = partner(self.me, step, self.chips)
            first = pl.multiple_of(target * self.rows, self.rows)

            @pl.loop(0, self.rows // CHUNK)
            def add(k):
                at = chunk_rows(step * (self.rows // CHUNK) + k)
                from_part = pl.ds(pl.multiple_of(first + k * CHUNK, CHUNK), CHUNK)
                self.near[at, :] = (
                    self.part[from_part, :].astype(F32) + self.near[at, :].astype(F32)
                ).astype(BF)

            self.far_copies.append(
                send(
                    self.near.at[pl.ds(step * self.rows, self.rows), :],
                    self.far.at[pl.ds((step - 1) * self.rows, self.rows), :],
                    self.far_send.at[step],
                    self.far_recv.at[step],
                    {"context": target},
                )
            )

    def arrive(self):
        self.near_copies[0].wait_recv()
        for copy in self.far_copies:
            copy.wait_recv()

    def total(self, k):
        at = chunk_rows(k)
        first = pl.multiple_of(self.me * self.rows, self.rows)
        value = self.part[pl.ds(pl.multiple_of(first + k * CHUNK, CHUNK), CHUNK), :].astype(F32)
        value = value + self.near[at, :].astype(F32)
        for step in range(1, self.chips):
            there = chunk_rows((step - 1) * (self.rows // CHUNK) + k)
            value = value + self.far[there, :].astype(F32)
        return value

    def drain(self):
        for copy in list(self.near_copies.values()) + self.far_copies:
            copy.wait_send()


def chunk_rows(k):
    return pl.ds(pl.multiple_of(k * CHUNK, CHUNK), CHUNK)


def vmem_specs(count):
    return [pl.BlockSpec(memory_space=pltpu.VMEM)] * count


def comm_params(collective_id):
    return pltpu.CompilerParams(
        collective_id=collective_id, has_side_effects=True, vmem_limit_bytes=VMEM_LIMIT
    )


def place_rows(ref, unit, layer, place):
    return ref.at[rows_at(place, unit), :]


class Docs:
    @staticmethod
    def scratch(columns):
        return [
            pltpu.SemaphoreType.DMA((columns,)),
            pltpu.SemaphoreType.DMA((columns,)),
            pltpu.SemaphoreType.DMA,
        ]

    def __init__(self, docs, docs_full, columns, sems):
        docs_send, docs_recv, docs_local = sems
        me = lax.axis_index("context")
        mine = docs_full.at[pl.ds(me, 1), :]
        self.copies = [
            send(docs, mine, docs_send.at[step], docs_recv.at[step], {"context": lax.rem(me + step, columns)})
            for step in range(1, columns)
        ]
        self.local = pltpu.make_async_copy(docs, mine, docs_local)
        self.local.start()

    def finish(self):
        for copy in self.copies:
            copy.wait_recv()
        for copy in self.copies:
            copy.wait_send()
        self.local.wait()


class GainSums:
    @staticmethod
    def scratch(columns, layers, width):
        return [
            pltpu.VMEM((8, width), F32),
            pltpu.VMEM((columns, 8, width), F32),
            pltpu.VMEM((8, width), F32),
            pltpu.VMEM((layers, 8, width), F32),
            pltpu.SemaphoreType.DMA((columns,)),
            pltpu.SemaphoreType.DMA((columns,)),
            pltpu.SemaphoreType.DMA((layers,)),
            pltpu.SemaphoreType.DMA((layers,)),
        ]

    def __init__(self, columns, layers, scratch):
        self.columns, self.layers = columns, layers
        self.own, self.plane_slots, self.plane, self.line_slots, *self.sems = scratch
        self.own[...] = jnp.zeros_like(self.own)

    def start(self):
        me = lax.axis_index("context")
        plane_send, plane_recv, _, _ = self.sems
        self.in_plane = [
            send(
                self.own,
                self.plane_slots.at[step],
                plane_send.at[step],
                plane_recv.at[step],
                {"context": lax.rem(me + step, self.columns)},
            )
            for step in range(1, self.columns)
        ]

    def along(self):
        layer = lax.axis_index("fsdp")
        _, _, line_send, line_recv = self.sems
        total = self.own[...]
        for step, copy in enumerate(self.in_plane):
            copy.wait_recv()
            total = total + self.plane_slots[step + 1]
        self.plane[...] = total
        self.in_line = [
            send(
                self.plane,
                self.line_slots.at[step],
                line_send.at[step],
                line_recv.at[step],
                {"fsdp": lax.rem(layer + step, self.layers)},
            )
            for step in range(1, self.layers)
        ]

    def finish(self, result):
        total = self.plane[...]
        for step, copy in enumerate(self.in_line):
            copy.wait_recv()
            total = total + self.line_slots[step + 1]
        result[...] = total
        for copy in self.in_plane + self.in_line:
            copy.wait_send()


def input_gradient(reduce, gains, x_ref, grad_ref, gain_row, result):
    @pl.loop(0, x_ref.shape[0] // CHUNK)
    def finish(k):
        at = chunk_rows(k)
        grad_hidden = reduce.total(k)
        residual = x_ref[at, :].astype(F32)
        scale = rms_scale(residual)
        normed = residual * scale
        gains.own[0:1, :] += jnp.sum(grad_hidden * normed, axis=0, keepdims=True)
        result[at, :] = grad_ref[at, :] + norm_backward(grad_hidden, normed, scale, gain_row)


def last_kernel(columns, layers, part_in, x_ref, grad_ref, gain_ref, sums_ref, input_grad_ref, gains_ref, *scratch):
    rows, chips = x_ref.shape[0], columns // 2
    greet(columns, layers)
    reduce = Reduce(part_in, chips, rows, scratch[0:2], scratch[2:6])
    gains = GainSums(columns, layers, scratch[6:])
    gains.own[1:2, :] = sums_ref[0:1, :]
    reduce.exchange()
    reduce.arrive()
    input_gradient(reduce, gains, x_ref, grad_ref, gain_ref[...], input_grad_ref)
    gains.start()
    gains.along()
    gains.finish(gains_ref)
    reduce.drain()


def last_step(part_in, x_own, grad_middle, gain_row, sums, columns, layers):
    rows, width = x_own.shape
    chips = columns // 2
    return pl.pallas_call(
        functools.partial(last_kernel, columns, layers),
        out_shape=(
            jax.ShapeDtypeStruct((rows, width), F32),
            jax.ShapeDtypeStruct((8, width), F32),
        ),
        in_specs=vmem_specs(5),
        out_specs=tuple(vmem_specs(2)),
        scratch_shapes=[
            *Reduce.buffers(chips, rows, width),
            *Reduce.semaphores(chips),
            *GainSums.scratch(columns, layers, width),
        ],
        compiler_params=comm_params(5),
        name="last_step",
        cost_estimate=pl.CostEstimate(flops=0, bytes_accessed=150_000_000, transcendentals=0),
    )(part_in, x_own, grad_middle, gain_row, sums)


def turned(heads, low):
    return jnp.where(low, pltpu.roll(heads, LANES - HEAD_SIZE // 2, 1), pltpu.roll(heads, HEAD_SIZE // 2, 1))


def allowed_tile(start_ref, row_first, col_first):
    rows = row_first + lax.broadcasted_iota(jnp.int32, (TILE, TILE), 0)
    cols = col_first + lax.broadcasted_iota(jnp.int32, (TILE, TILE), 1)
    starts = jnp.broadcast_to(start_ref[row_first : row_first + TILE, 0:1], (TILE, TILE))
    return (cols <= rows) & (cols >= starts)


def place_tables(docs_ref, freq_ref, cos_ref, sin_ref, start_ref):
    blocks = docs_ref.shape[0]

    @pl.loop(0, blocks)
    def one_block(r):
        at = pl.ds(pl.multiple_of(r * LANES, LANES), LANES)
        mine = jnp.transpose(
            jnp.broadcast_to(docs_ref[pl.ds(r, 1), :].astype(F32), (LANES, LANES))
        )
        earlier = jnp.zeros((LANES, LANES), F32)
        for other in range(blocks):
            theirs = docs_ref[other : other + 1, :].astype(F32)
            earlier = earlier + jnp.where(theirs < mine, 1.0, 0.0)
        starts = jnp.broadcast_to(jnp.sum(earlier, axis=1, keepdims=True), (LANES, LANES))
        start_ref[at, :] = starts.astype(jnp.int32)
        token = r * LANES + lax.broadcasted_iota(jnp.int32, (LANES, LANES), 0)
        angles = (token.astype(F32) - starts) * freq_ref[...]
        lane = lax.broadcasted_iota(jnp.int32, (LANES, LANES), 1)
        sine = jnp.sin(angles)
        cos_ref[at, :] = jnp.where(lane < HEAD_SIZE, jnp.cos(angles), 0.0)
        sin_ref[at, :] = jnp.where(
            lane < HEAD_SIZE // 2, -sine, jnp.where(lane < HEAD_SIZE, sine, 0.0)
        )


def forward_kernel(columns, layers, heads, homes, aligned, *refs):
    (x_ref, gains_ref, docs_ref, freq_ref, dy_ref, attn_ref, ffn_ref), refs = refs[:7], refs[7:]
    (q_ref, k_ref, v_ref, att_ref, log_ref, pad_ref, middle_ref), refs = refs[:7], refs[7:]
    (cos_ref, sin_ref, start_ref, h_ref), refs = refs[:4], refs[4:]
    (h2_full, dy_full, ffn_col), refs = refs[:3], refs[3:]
    (part_ref, hidden, hidden_two, docs_full, ffn_bf, ffn_shard), refs = refs[:6], refs[6:]
    if aligned:
        (attn_bf, attn_shard, attn_col, *attn_scratch), refs = refs[:10], refs[10:]
    scratch = refs
    seq, own_rows, chips = h_ref.shape[0], x_ref.shape[0], columns // 2
    ffn_rows = ffn_ref.shape[0]
    if aligned:
        attn_rows = attn_ref.shape[0]

        @pl.loop(0, attn_rows // CHUNK)
        def cast_attn(k):
            attn_bf[chunk_rows(k), :] = attn_ref[chunk_rows(k), :].astype(BF)

        targets = homes.attn_targets()
        greet(columns, layers, [spot[:2] for spot in targets + homes.attn_owners()])
        unit = attn_rows // 3
        attn_spread = Exchange(
            [attn_bf.at[pl.ds(k * unit, unit), :] for k in range(3)],
            functools.partial(place_rows, attn_shard, unit),
            targets,
            attn_scratch[0:2],
        )
    else:
        greet(columns, layers)
    documents = Docs(docs_ref, docs_full, columns, scratch[0:3])

    @pl.loop(0, own_rows // CHUNK)
    def norm(k):
        residual = x_ref[chunk_rows(k), :].astype(F32)
        gain = 1.0 + gains_ref[0:1, :]
        hidden[chunk_rows(k), :] = (residual * rms_scale(residual) * gain).astype(BF)

    h_gather = Gather(hidden, h_ref, chips, scratch[3:8])

    @pl.loop(0, ffn_rows // CHUNK)
    def cast_ffn(k):
        ffn_bf[chunk_rows(k), :] = ffn_ref[chunk_rows(k), :].astype(BF)

    unit_ffn = ffn_rows // 3
    if aligned:
        attn_spread.arrive()
        attn_line = LineGather(attn_col, attn_shard, layers, 1, attn_scratch[2:7])
    ffn_spread = Exchange(
        [ffn_bf.at[pl.ds(k * unit_ffn, unit_ffn), :] for k in range(3)],
        functools.partial(place_rows, ffn_shard, unit_ffn),
        homes.ffn_targets(),
        scratch[8:10],
    )
    documents.finish()
    place_tables(docs_full, freq_ref, cos_ref, sin_ref, start_ref)
    if aligned:
        attn_line.relay(1)
    h_gather.pass_on()
    if aligned:
        attn_line.relay()
    ffn_spread.arrive()
    line = LineGather(ffn_col, ffn_shard, layers, 3, scratch[10:15])
    h_gather.finish()
    dy_gather = Gather(dy_ref, dy_full, chips, scratch[15:20])
    if aligned:
        attn_line.finish()
        w_ref = attn_col
    else:
        w_ref = attn_ref
    scale = HEAD_SIZE**-0.5
    for slot in range(2 * heads + 2):
        pad_ref[slot * LANES : slot * LANES + HEAD_SIZE, :] = w_ref[
            slot * HEAD_SIZE : (slot + 1) * HEAD_SIZE, :
        ]
        pad_ref[slot * LANES + HEAD_SIZE : (slot + 1) * LANES, :] = jnp.zeros(
            (LANES - HEAD_SIZE, w_ref.shape[1]), BF
        )
    width = (heads + 2) * LANES

    @pl.loop(0, seq // TILE)
    def project(i):
        at = pl.ds(pl.multiple_of(i * TILE, TILE), TILE)
        low = lax.broadcasted_iota(jnp.int32, (TILE, LANES), 1) < HEAD_SIZE // 2
        projected = product_transposed(h_ref[at, :], pad_ref[0:width, :])
        cosine, sine = cos_ref[at, :], sin_ref[at, :]
        for head in range(heads + 1):
            u = projected[:, head * LANES : (head + 1) * LANES]
            r = (u * cosine + turned(u, low) * sine).astype(BF)
            if head < heads:
                q_ref[at, head * LANES : (head + 1) * LANES] = r
            else:
                k_ref[at, :] = r
        v_ref[at, :] = projected[:, (heads + 1) * LANES :].astype(BF)

    for i in range(seq // TILE):
        rows = slice(i * TILE, (i + 1) * TILE)
        for head in range(heads):
            lanes = slice(head * LANES, (head + 1) * LANES)
            q = q_ref[rows, lanes]
            out = jnp.zeros((TILE, LANES), F32)
            total = jnp.zeros((TILE, 1), F32)
            for j in range(i + 1):
                keys = slice(j * TILE, (j + 1) * TILE)
                s = product_transposed(q, k_ref[keys, :]) * scale
                e = jnp.where(allowed_tile(start_ref, i * TILE, j * TILE), jnp.exp(s), 0.0)
                total = total + jnp.sum(e, axis=1, keepdims=True)
                out = out + plain_times(e.astype(BF), v_ref[keys, :])
            att_ref[rows, lanes] = (out / total).astype(BF)
            log_ref[rows, lanes] = jnp.broadcast_to(jnp.log(total), (TILE, LANES))

    @pl.loop(0, seq // TILE)
    def project_out(i):
        at = pl.ds(pl.multiple_of(i * TILE, TILE), TILE)
        part_ref[at, :] = plain_times(att_ref[at, :], pad_ref[width:, :]).astype(BF)

    reduce = Reduce(part_ref, chips, own_rows, scratch[20:22], scratch[22:26])
    line.relay(1)
    reduce.exchange()
    line.relay(1)
    dy_gather.pass_on()
    line.relay(1)
    reduce.arrive()

    @pl.loop(0, own_rows // CHUNK)
    def finish(k):
        at = chunk_rows(k)
        middle = x_ref[at, :].astype(F32) + reduce.total(k)
        middle_ref[at, :] = middle
        hidden_two[at, :] = (middle * rms_scale(middle) * (1.0 + gains_ref[1:2, :])).astype(BF)

    gather = Gather(hidden_two, h2_full, chips, scratch[26:31])
    line.relay(1)
    gather.pass_on()
    line.relay()
    gather.finish()
    dy_gather.finish()
    reduce.drain()
    line.finish()
    ffn_spread.drain()
    if aligned:
        attn_spread.drain()


def forward_step(x_own, gains, docs, dy_own, attn, ffn_weights, attn_total, heads, columns, layers, aligned):
    rows, width = x_own.shape
    seq = rows * columns
    chips = columns // 2
    ffn_rows = ffn_weights.shape[0]
    place = np.arange(LANES)
    frequency = np.where(
        place < HEAD_SIZE, ROPE_THETA ** (-2.0 * (place % (HEAD_SIZE // 2)) / HEAD_SIZE), 0.0
    ).astype(np.float32)[None, :]
    attn_scratch = []
    if aligned:
        attn_scratch = [
            pltpu.VMEM(attn.shape, BF),
            pltpu.VMEM(attn.shape, BF),
            pltpu.VMEM((layers * attn.shape[0], width), BF),
            *Exchange.scratch(),
            *LineGather.scratch(layers, 1),
        ]
    return pl.pallas_call(
        functools.partial(
            forward_kernel, columns, layers, heads, Homes(layers, columns, attn_total), aligned
        ),
        out_shape=(
            jax.ShapeDtypeStruct((seq, heads * LANES), BF),
            jax.ShapeDtypeStruct((seq, LANES), BF),
            jax.ShapeDtypeStruct((seq, LANES), BF),
            jax.ShapeDtypeStruct((seq, heads * LANES), BF),
            jax.ShapeDtypeStruct((seq, heads * LANES), F32),
            jax.ShapeDtypeStruct(((2 * heads + 2) * LANES, width), BF),
            jax.ShapeDtypeStruct((rows, width), F32),
            jax.ShapeDtypeStruct((seq, LANES), F32),
            jax.ShapeDtypeStruct((seq, LANES), F32),
            jax.ShapeDtypeStruct((seq, LANES), jnp.int32),
            jax.ShapeDtypeStruct((seq, width), BF),
            jax.ShapeDtypeStruct((seq, width), BF),
            jax.ShapeDtypeStruct((seq, width), BF),
            jax.ShapeDtypeStruct((layers * ffn_rows, width), BF),
        ),
        in_specs=vmem_specs(7),
        out_specs=tuple(vmem_specs(11) + [pl.BlockSpec(memory_space=pl.ANY)] * 3),
        scratch_shapes=[
            pltpu.VMEM((seq, width), BF),
            pltpu.VMEM((rows, width), BF),
            pltpu.VMEM((rows, width), BF),
            pltpu.VMEM((columns, rows), jnp.int32),
            pltpu.VMEM((ffn_rows, width), BF),
            pltpu.VMEM((ffn_rows, width), BF),
            *attn_scratch,
            *Docs.scratch(columns),
            *Gather.scratch(chips),
            *Exchange.scratch(),
            *LineGather.scratch(layers, 3),
            *Gather.scratch(chips),
            *Reduce.buffers(chips, rows, width),
            *Reduce.semaphores(chips),
            *Gather.scratch(chips),
        ],
        compiler_params=comm_params(3),
        name="forward_step",
        cost_estimate=pl.CostEstimate(flops=6_000_000_000, bytes_accessed=250_000_000, transcendentals=2_000_000),
    )(x_own, gains, docs, jnp.asarray(frequency), dy_own, attn, ffn_weights)


class Load:
    def __init__(self, source, target, sems, blocks=1):
        size = source.shape[0] // blocks
        self.copies = []
        for k in range(blocks):
            at = pl.ds(k * size, size)
            copy = pltpu.make_async_copy(source.at[at, :], target.at[at, :], sems.at[k])
            copy.start()
            self.copies.append(copy)
        self.next = 0

    def wait(self, count=None):
        stop = len(self.copies) if count is None else self.next + count
        for copy in self.copies[self.next : stop]:
            copy.wait()
        self.next = stop


def columns_of(width, most=512):
    return most, width // most


def backward_kernel(columns, layers, heads, sharers, factor, homes, *refs):
    (h2_hbm, dy_hbm, w_hbm, h_hbm, pad_hbm), refs = refs[:5], refs[5:]
    (cos_hbm, sin_hbm, start_hbm, q_hbm, k_hbm, v_hbm, att_hbm, log_hbm), refs = refs[:8], refs[8:]
    (middle_ref, dy_ref, gains_in, x_own), refs = refs[:4], refs[4:]
    if homes is None:
        (block_out_ref, grad_ref, sums_ref, ffn_sum, term_in, in_part), refs = refs[:6], refs[6:]
    else:
        (block_out_ref, input_grad_ref, gains_ref, attn_back, ffn_back), refs = refs[:5], refs[5:]
        (grad_ref, sums_ref, ffn_sum, term_in, attn_done), refs = refs[:5], refs[5:]
        last, refs = refs[:20], refs[20:]
    (x_ref, y_ref, w_ref, pad_ref, cos_ref, sin_ref, start_ref), refs = refs[:7], refs[7:]
    (q_ref, k_ref, v_ref, att_ref, log_ref), refs = refs[:5], refs[5:]
    (act_ref, gg_ref, gu_ref, act_t, gg_t, gu_t, term, part_ref), refs = refs[:8], refs[8:]
    (gm_full, grad_bf, dk_ref, dv_ref, out_ref, out_t), refs = refs[:6], refs[6:]
    ga_ref, shared_ref = gg_ref.at[:, 0 : heads * LANES], act_ref.at[:, 0 : 2 * LANES]
    load_sems, store_sem, shared_send, shared_recv, *scratch = refs
    seq, own_rows, chips = gm_full.shape[0], middle_ref.shape[0], columns // 2
    hidden = w_ref.shape[0] // 3
    tiles = seq // TILE
    block, blocks = columns_of(w_ref.shape[1])
    w_load = Load(w_hbm, w_ref, load_sems.at[pl.ds(0, 3)], 3)
    h2_load = Load(h2_hbm, x_ref, load_sems.at[pl.ds(3, 1)])
    dy_load = Load(dy_hbm, y_ref, load_sems.at[pl.ds(4, 1)])
    later = [
        Load(source, target, load_sems.at[pl.ds(5 + k, 1)])
        for k, (source, target) in enumerate(
            (
                (pad_hbm, pad_ref),
                (cos_hbm, cos_ref),
                (sin_hbm, sin_ref),
                (start_hbm, start_ref),
                (q_hbm, q_ref),
                (k_hbm, k_ref),
                (v_hbm, v_ref),
                (att_hbm, att_ref),
                (log_hbm, log_ref),
            )
        )
    ]
    if homes is None:
        greet(columns, layers)
    else:
        attn_owners = homes.attn_owners()
        greet(columns, layers, [spot[:2] for spot in homes.attn_targets() + attn_owners])
    w_gate, w_up, w_down = (pl.ds(k * hidden, hidden) for k in range(3))

    w_load.wait()
    h2_load.wait()
    dy_load.wait()

    @pl.loop(0, tiles)
    def feed_forward(i):
        at = pl.ds(pl.multiple_of(i * TILE, TILE), TILE)
        gate = product_transposed(x_ref[at, :], w_ref[w_gate, :])
        up = product_transposed(x_ref[at, :], w_ref[w_up, :])
        grad_act = product_transposed(y_ref[at, :], w_ref[w_down, :])
        sigmoid = 1.0 / (1.0 + jnp.exp(-gate))
        swish = gate * sigmoid
        act_ref[at, :] = (swish * up).astype(BF)
        gg_ref[at, :] = (grad_act * up * sigmoid * (1.0 + gate * (1.0 - sigmoid))).astype(BF)
        gu_ref[at, :] = (grad_act * swish).astype(BF)
        act_t[:, at] = jnp.transpose(act_ref[at, :])
        gg_t[:, at] = jnp.transpose(gg_ref[at, :])
        gu_t[:, at] = jnp.transpose(gu_ref[at, :])

    @pl.loop(0, blocks)
    def weight_gradients(j):
        at = pl.ds(pl.multiple_of(j * block, block), block)
        for rows, left, right in ((w_gate, gg_t, x_ref), (w_up, gu_t, x_ref), (w_down, act_t, y_ref)):
            term[rows, at] = (plain_times(left[...], right[:, at]) * factor).astype(BF)

    line = LineReduce(term, layers, 3, scratch[0:6])
    h_load = Load(h_hbm, x_ref, load_sems.at[pl.ds(14, 1)])

    @pl.loop(0, tiles)
    def back_part(i):
        at = pl.ds(pl.multiple_of(i * TILE, TILE), TILE)
        part_ref[at, :] = (
            plain_times(gg_ref[at, :], w_ref[w_gate, :]) + plain_times(gu_ref[at, :], w_ref[w_up, :])
        ).astype(BF)

    back = Reduce(part_ref, chips, own_rows, scratch[6:8], scratch[8:12])
    sums_ref[...] = jnp.zeros_like(sums_ref)

    @pl.loop(0, tiles)
    def out_part(i):
        at = pl.ds(pl.multiple_of(i * TILE, TILE), TILE)
        y_ref[at, :] = plain_times(act_ref[at, :], w_ref[w_down, :]).astype(BF)

    back.exchange()
    line.relay(2)
    back.arrive()
    back.drain()

    @pl.loop(0, own_rows // CHUNK)
    def turn(k):
        at = chunk_rows(k)
        grad_hidden = back.total(k)
        middle = middle_ref[at, :]
        scale = rms_scale(middle)
        normed = middle * scale
        sums_ref[0:1, :] += jnp.sum(grad_hidden * normed, axis=0, keepdims=True)
        grad = dy_ref[at, :].astype(F32) + norm_backward(grad_hidden, normed, scale, gains_in[1:2, :])
        grad_ref[at, :] = grad
        grad_bf[at, :] = grad.astype(BF)

    gather = Gather(grad_bf, gm_full, chips, scratch[12:17])
    line.relay(1)
    gather.pass_on()
    line.relay(2)
    gather.finish()
    out = Reduce(y_ref, chips, own_rows, scratch[6:8], scratch[17:21])
    for load in later:
        load.wait()

    scale = HEAD_SIZE**-0.5
    width = (heads + 2) * LANES

    @pl.loop(0, tiles)
    def attended_gradient(i):
        at = pl.ds(pl.multiple_of(i * TILE, TILE), TILE)
        ga_ref[at, :] = product_transposed(gm_full[at, :], pad_ref[width:, :]).astype(BF)

    out.exchange()
    dk_ref[...] = jnp.zeros_like(dk_ref)
    dv_ref[...] = jnp.zeros_like(dv_ref)
    low = lax.broadcasted_iota(jnp.int32, (TILE, LANES), 1) < HEAD_SIZE // 2

    def turn_back(u, rows):
        return (u * cos_ref[rows, :] - turned(u, low) * sin_ref[rows, :]).astype(BF)

    for i in range(tiles):
        rows = slice(i * TILE, (i + 1) * TILE)
        for head in range(heads):
            lanes = slice(head * LANES, (head + 1) * LANES)
            q = q_ref[rows, lanes]
            ga = ga_ref[rows, lanes]
            delta = jnp.sum(ga.astype(F32) * att_ref[rows, lanes].astype(F32), axis=1, keepdims=True)
            logs = log_ref[rows, head * LANES : head * LANES + 1]
            dq = jnp.zeros((TILE, LANES), F32)
            for j in range(i + 1):
                keys = slice(j * TILE, (j + 1) * TILE)
                s = product_transposed(q, k_ref[keys, :]) * scale
                p = jnp.where(allowed_tile(start_ref, i * TILE, j * TILE), jnp.exp(s - logs), 0.0)
                dp = product_transposed(ga, v_ref[keys, :])
                ds = (p * (dp - delta) * scale).astype(BF)
                dq = dq + plain_times(ds, k_ref[keys, :])
                dk_ref[keys, :] += transposed_times(ds, q)
                dv_ref[keys, :] += transposed_times(p.astype(BF), ga)
            out_ref[rows, lanes] = turn_back(dq, rows)
        if i == tiles // 2:
            line.relay(1)
    line.relay(1)
    for i in range(tiles):
        rows = slice(i * TILE, (i + 1) * TILE)
        out_ref[rows, heads * LANES : (heads + 1) * LANES] = turn_back(dk_ref[rows, :], rows)
        out_ref[rows, (heads + 1) * LANES :] = dv_ref[rows, :].astype(BF)
    if sharers > 1:
        me = lax.axis_index("context")
        both = pl.ds(heads * LANES, 2 * LANES)
        copy = send(
            out_ref.at[:, both], shared_ref, shared_send, shared_recv, {"context": sibling_of(me)}
        )
        copy.wait()
        lane = lax.broadcasted_iota(jnp.int32, (TILE, 2 * LANES), 1) % LANES
        kept = lane // (HEAD_SIZE // sharers) == lax.rem(me, 2)
        for i in range(tiles):
            rows = slice(i * TILE, (i + 1) * TILE)
            value = out_ref[rows, both].astype(F32) + shared_ref[rows, :].astype(F32)
            out_ref[rows, both] = jnp.where(kept, value, 0.0).astype(BF)
    for i in range(tiles):
        rows = slice(i * TILE, (i + 1) * TILE)
        out_t[0:width, rows] = jnp.transpose(out_ref[rows, :])
        out_t[width:, rows] = jnp.transpose(att_ref[rows, :])

    @pl.loop(0, tiles)
    def input_part(i):
        at = pl.ds(pl.multiple_of(i * TILE, TILE), TILE)
        part_ref[at, :] = plain_times(out_ref[at, :], pad_ref[0:width, :]).astype(BF)

    if homes is None:
        store = pltpu.make_async_copy(part_ref, in_part, store_sem)
        store.start()
    else:
        near_rows = chips * own_rows
        room = (w_ref.at[pl.ds(0, near_rows), :], w_ref.at[pl.ds(near_rows, near_rows - own_rows), :])
        first = Reduce(part_ref, chips, own_rows, room, last[0:4])
    h_load.wait()

    @pl.loop(0, blocks)
    def attention_gradients(j):
        at = pl.ds(pl.multiple_of(j * block, block), block)
        inner = (plain_times(out_t[0:width, :], x_ref[:, at]) * factor).astype(BF)
        outer = (plain_times(out_t[width:, :], gm_full[:, at]) * factor).astype(BF)
        for value, first, count in ((inner, 0, heads + 2), (outer, heads + 2, heads)):
            for k in range(count):
                if sharers > 1:
                    term_in[pl.ds((first + k) * LANES, LANES), at] = value[k * LANES : (k + 1) * LANES, :]
                else:
                    term_in[pl.ds((first + k) * HEAD_SIZE, HEAD_SIZE), at] = value[
                        k * LANES : k * LANES + HEAD_SIZE, :
                    ]

    if homes is not None:
        attn_line = LineReduce(term_in, layers, 3, last[4:10])
        first.exchange()
    out.arrive()

    @pl.loop(0, own_rows // CHUNK)
    def finish_out(k):
        at = chunk_rows(k)
        block_out_ref[at, :] = middle_ref[at, :] + out.total(k)

    line.finish(ffn_sum)
    if homes is None:
        store.wait()
    else:
        unit_ffn, unit = ffn_sum.shape[0] // 3, attn_done.shape[0] // 3
        ffn_owned = Exchange(
            [ffn_sum.at[pl.ds(k * unit_ffn, unit_ffn), :] for k in range(3)],
            functools.partial(place_rows, ffn_back, unit_ffn),
            homes.ffn_owners(),
            last[10:12],
        )
        gains = GainSums(columns, layers, last[12:20])
        gains.own[1:2, :] = sums_ref[0:1, :]
        attn_line.relay(3)
        first.arrive()
        input_gradient(first, gains, x_own, grad_ref, gains_in[0:1, :], input_grad_ref)
        gains.start()
        attn_line.relay(4)
        gains.along()
        attn_line.finish(attn_done)
        attn_owned = Exchange(
            [attn_done.at[pl.ds(k * unit, unit), :] for k in range(3)],
            functools.partial(place_rows, attn_back, unit),
            attn_owners,
            scratch[21:23],
        )
        gains.finish(gains_ref)
        ffn_owned.arrive()
        attn_owned.arrive()
        ffn_owned.drain()
        attn_owned.drain()
        attn_line.drain()
        first.drain()
    line.drain()
    out.drain()


def backward_step(
    h2_full, dy_full, ffn_col, h_full, padded, tables, saved, middle, dy_own, gains, x_own, heads, columns, layers, sharers, joined
):
    seq, width = h2_full.shape
    rows = seq // columns
    chips = columns // 2
    hidden = ffn_col.shape[0] // 3
    ffn_rows = ffn_col.shape[0] // layers
    each = HEAD_SIZE if sharers == 1 else LANES
    term_rows = (2 * heads + 2) * each
    attn_rows = term_rows // layers
    loaded = [ffn_col, padded, *tables, *saved]
    own = jax.ShapeDtypeStruct((rows, width), F32)
    eight = jax.ShapeDtypeStruct((8, width), F32)
    anywhere = pl.BlockSpec(memory_space=pl.ANY)
    homes, last = None, []
    if joined:
        homes = Homes(layers, columns, attn_rows * layers * columns)
        shapes = (
            own,
            own,
            eight,
            jax.ShapeDtypeStruct((attn_rows, width), BF),
            jax.ShapeDtypeStruct((ffn_rows, width), BF),
        )
        specs = (*vmem_specs(3), anywhere, anywhere)
        last = [
            pltpu.VMEM((rows, width), F32),
            pltpu.VMEM((8, width), F32),
            pltpu.VMEM((ffn_rows, width), BF),
            pltpu.VMEM((term_rows, width), BF),
            pltpu.VMEM((attn_rows, width), BF),
            *Reduce.semaphores(chips),
            *LineReduce.scratch(layers, 3, attn_rows, width),
            *Exchange.scratch(),
            *GainSums.scratch(columns, layers, width),
        ]
    else:
        shapes = (
            own,
            own,
            eight,
            jax.ShapeDtypeStruct((ffn_rows, width), BF),
            jax.ShapeDtypeStruct((term_rows, width), BF),
            jax.ShapeDtypeStruct((seq, width), BF),
        )
        specs = (*vmem_specs(5), anywhere)
    return pl.pallas_call(
        functools.partial(
            backward_kernel, columns, layers, heads, sharers, float(seq * layers) ** (-0.5), homes
        ),
        out_shape=shapes,
        in_specs=[anywhere] * 13 + vmem_specs(3) + (vmem_specs(1) if joined else [anywhere]),
        out_specs=specs,
        scratch_shapes=[
            *last,
            pltpu.VMEM((seq, width), BF),
            pltpu.VMEM((seq, width), BF),
            *[pltpu.VMEM(array.shape, array.dtype) for array in loaded],
            *[pltpu.VMEM((seq, hidden), BF)] * 3,
            *[pltpu.VMEM((hidden, seq), BF)] * 3,
            pltpu.VMEM(ffn_col.shape, BF),
            pltpu.VMEM((seq, width), BF),
            pltpu.VMEM((seq, width), BF),
            pltpu.VMEM((rows, width), BF),
            pltpu.VMEM((seq, LANES), F32),
            pltpu.VMEM((seq, LANES), F32),
            pltpu.VMEM((seq, (heads + 2) * LANES), BF),
            pltpu.VMEM(((2 * heads + 2) * LANES, seq), BF),
            pltpu.SemaphoreType.DMA((15,)),
            pltpu.SemaphoreType.DMA,
            pltpu.SemaphoreType.DMA,
            pltpu.SemaphoreType.DMA,
            *LineReduce.scratch(layers, 3, ffn_rows, width),
            *Reduce.buffers(chips, rows, width),
            *Reduce.semaphores(chips),
            *Gather.scratch(chips),
            *Reduce.semaphores(chips),
            *Exchange.scratch(),
        ],
        compiler_params=comm_params(4),
        name="backward_step",
        cost_estimate=pl.CostEstimate(flops=28_000_000_000, bytes_accessed=250_000_000, transcendentals=4_000_000),
    )(h2_full, dy_full, ffn_col, h_full, padded, *tables, *saved, middle, dy_own, gains, x_own)


def update_kernel(counts, *refs):
    sources, targets, held = refs[:8], refs[8:16], refs[16:26]
    in_sems, out_sems, pass_in, pass_out = refs[26:]
    pieces, leaving = [], []
    for k in range(2):
        size = sources[3 * k].shape[0] // counts[k]
        for n in range(counts[k]):
            pieces.append((k, pl.ds(n * size, size), size))

    def ends(k, at):
        g, p, m = sources[3 * k : 3 * k + 3]
        g_held, p_held, m_held, grad_held = held[4 * k : 4 * k + 4]
        grad_out, p_out, m_out = targets[3 * k : 3 * k + 3]
        incoming = (
            (g.at[at, :], g_held.at[at, :]),
            (p.at[at, :], p_held.at[at, :]),
            (m.at[:, at, :], m_held.at[:, at, :]),
        )
        outgoing = (
            (grad_held.at[at, :], grad_out.at[at, :]),
            (p_held.at[at, :], p_out.at[at, :]),
            (m_held.at[:, at, :], m_out.at[:, at, :]),
        )
        return incoming, outgoing

    arriving = []
    for n, (k, at, _) in enumerate(pieces):
        copies = [
            pltpu.make_async_copy(source, target, in_sems.at[n, j])
            for j, (source, target) in enumerate(ends(k, at)[0])
        ]
        for copy in copies:
            copy.start()
        arriving.append(copies)
    passing = [
        pltpu.make_async_copy(sources[6 + k], held[8 + k], pass_in.at[k]) for k in range(2)
    ]
    for copy in passing:
        copy.start()
    for n, (k, at, size) in enumerate(pieces):
        for copy in arriving[n]:
            copy.wait()
        g_held, p_held, m_held, grad_held = held[4 * k : 4 * k + 4]
        part = CHUNK if size % CHUNK == 0 else size

        @pl.loop(0, size // part)
        def rows(c):
            here = pl.ds(pl.multiple_of(at.start + c * part, part), part)
            gradient = g_held[here, :].astype(F32)
            grad_held[here, :] = gradient
            parameter = p_held[here, :]
            first_moment = BETA_ONE * m_held[0, here, :] + (1.0 - BETA_ONE) * gradient
            second_moment = BETA_TWO * m_held[1, here, :] + (1.0 - BETA_TWO) * gradient * gradient
            m_held[0, here, :] = first_moment
            m_held[1, here, :] = second_moment
            below = jnp.sqrt(second_moment * (1.0 / (1.0 - BETA_TWO**STEP))) + ADAM_EPS
            step = first_moment * (LEARN_RATE / (1.0 - BETA_ONE**STEP)) / below
            p_held[here, :] = parameter * (1.0 - LEARN_RATE * WEIGHT_DECAY) - step

        for j, (source, target) in enumerate(ends(k, at)[1]):
            copy = pltpu.make_async_copy(source, target, out_sems.at[n, j])
            copy.start()
            leaving.append(copy)
    for k in range(2):
        passing[k].wait()
        copy = pltpu.make_async_copy(held[8 + k], targets[6 + k], pass_out.at[k])
        copy.start()
        leaving.append(copy)
    for copy in leaving:
        copy.wait()


def update_all(first, second, passed):
    shapes, held, counts = [], [], []
    for gradient, parameter, moments in (first, second):
        rows = parameter.shape[0]
        counts.append(rows // 48 if rows % 48 == 0 else 1)
        flat = jax.ShapeDtypeStruct(parameter.shape, F32)
        shapes += [flat, flat, jax.ShapeDtypeStruct(moments.shape, F32)]
        held += [
            pltpu.VMEM(gradient.shape, BF),
            pltpu.VMEM(parameter.shape, F32),
            pltpu.VMEM(moments.shape, F32),
            pltpu.VMEM(parameter.shape, F32),
        ]
    shapes += [jax.ShapeDtypeStruct(array.shape, array.dtype) for array in passed]
    held += [pltpu.VMEM(array.shape, array.dtype) for array in passed]
    out = pl.pallas_call(
        functools.partial(update_kernel, counts),
        out_shape=tuple(shapes),
        in_specs=[pl.BlockSpec(memory_space=pl.ANY)] * 8,
        out_specs=tuple([pl.BlockSpec(memory_space=pl.ANY)] * 8),
        scratch_shapes=[
            *held,
            pltpu.SemaphoreType.DMA((sum(counts), 3)),
            pltpu.SemaphoreType.DMA((sum(counts), 3)),
            pltpu.SemaphoreType.DMA((2,)),
            pltpu.SemaphoreType.DMA((2,)),
        ],
        compiler_params=pltpu.CompilerParams(vmem_limit_bytes=VMEM_LIMIT),
        name="update_all",
        cost_estimate=pl.CostEstimate(flops=20_000_000, bytes_accessed=25_000_000, transcendentals=1_000_000),
    )(*first, *second, *passed)
    return out[:3], out[3:6], out[6:]


def unpadded(rows, count):
    return jnp.concatenate([rows[k * LANES : k * LANES + HEAD_SIZE] for k in range(count)])


def on_device(
    block_input,
    cotangent,
    documents,
    attn_weights,
    ffn_weights,
    norm_gains,
    attn_moments,
    ffn_moments,
    gain_moments,
):
    layers, columns = lax.axis_size("fsdp"), lax.axis_size("context")
    rows, width = block_input.shape[1:]
    seq = rows * columns
    heads = QUERY_HEADS // columns
    sharers = max(1, columns // KEY_VALUE_HEADS)
    share = KEY_VALUE_HEADS * HEAD_SIZE // columns
    grad_factor = float(rows * layers * columns) ** (-0.5)
    attn_plan, ffn_plan = unit_plans(layers, columns, attn_weights.shape[0] * layers * columns)
    core = lax.rem(lax.axis_index("context"), 2)
    swap = [(c, c + 1 - 2 * (c % 2)) for c in range(columns)]

    x_own, dy_own = block_input[0], cotangent[0]
    attn_total = attn_weights.shape[0] * layers * columns
    aligned = attn_weights.shape[0] % (3 * CHUNK) == 0
    attn_source = attn_weights
    if not aligned:
        attn_col = lax.all_gather(
            attn_plan.spread(attn_weights.astype(BF)), "fsdp", axis=0, tiled=True
        )
        if sharers > 1:
            query_rows = heads * HEAD_SIZE
            own_part = attn_col[query_rows : query_rows + 2 * share]
            other = lax.ppermute(own_part, "context", swap)

            def whole_head(first):
                mine, theirs = own_part[first : first + share], other[first : first + share]
                return jnp.where(
                    core == 0, jnp.concatenate([mine, theirs]), jnp.concatenate([theirs, mine])
                )

            attn_col = jnp.concatenate(
                [
                    attn_col[:query_rows],
                    whole_head(0),
                    whole_head(share),
                    attn_col[query_rows + 2 * share :],
                ]
            )
        attn_source = attn_col
    *saved, padded, middle, cosine, sine, starts, h_full, h2_full, dy_full, ffn_col = forward_step(
        x_own, norm_gains, documents, dy_own, attn_source, ffn_weights, attn_total, heads, columns, layers, aligned
    )
    tables = (cosine, sine, starts)

    sums_of = backward_step(
        h2_full,
        dy_full,
        ffn_col,
        h_full,
        padded,
        tables,
        saved,
        middle,
        dy_own,
        norm_gains,
        x_own,
        heads,
        columns,
        layers,
        sharers,
        aligned,
    )
    if aligned:
        block_out, grad_input, gain_sums, attn_shard, ffn_shard = sums_of
    else:
        block_out, grad_middle, sums, ffn_sum, attn_term, in_part = sums_of
        if sharers > 1:
            own_rows = [
                lax.dynamic_slice_in_dim(attn_term, (heads + k) * LANES + core * share, share, 0)
                for k in range(2)
            ]
            attn_term = jnp.concatenate(
                [
                    unpadded(attn_term, heads),
                    *own_rows,
                    unpadded(attn_term[(heads + 2) * LANES :], heads),
                ]
            )
        attn_sum = lax.psum_scatter(attn_term, "fsdp", scatter_dimension=0, tiled=True)
        grad_input, gain_sums = last_step(
            in_part, x_own, grad_middle, norm_gains[0:1], sums, columns, layers
        )
        ffn_shard = ffn_plan.collect(ffn_sum)
        attn_shard = attn_plan.collect(attn_sum)

    column_count = width // (layers * columns)
    first_column = lax.axis_index(EVERY) * column_count
    gain_shard = lax.dynamic_slice_in_dim(gain_sums[:2], first_column, column_count, 1) * grad_factor
    own_gains = lax.dynamic_slice_in_dim(norm_gains, first_column, column_count, 1)
    ffn_new, attn_new, (block_out, grad_input) = update_all(
        (ffn_shard, ffn_weights, ffn_moments),
        (attn_shard, attn_weights, attn_moments),
        (block_out, grad_input),
    )
    ffn_shard, new_ffn, ffn_states = ffn_new
    attn_shard, new_attn, attn_states = attn_new
    new_gains, gain_states = adamw_update(own_gains, gain_shard, gain_moments, 0.0)
    return (
        block_out[None],
        grad_input[None],
        attn_shard,
        ffn_shard,
        gain_shard,
        new_attn,
        new_ffn,
        new_gains,
        attn_states,
        ffn_states,
        jnp.stack(gain_states),
    )


def solution(mesh):
    placed = (
        P("fsdp", "context", None),
        P("fsdp", "context", None),
        P("fsdp", "context"),
        P(EVERY, None),
        P(EVERY, None),
        P(),
        P(None, EVERY, None),
        P(None, EVERY, None),
        P(None, None, EVERY),
    )
    return jax.shard_map(
        on_device,
        mesh=mesh,
        in_specs=placed,
        out_specs=(
            P("fsdp", "context", None),
            P("fsdp", "context", None),
            P(EVERY, None),
            P(EVERY, None),
            P(None, EVERY),
            P(EVERY, None),
            P(EVERY, None),
            P(None, EVERY),
            P(None, EVERY, None),
            P(None, EVERY, None),
            P(None, None, EVERY),
        ),
        check_vma=False,
    )
```
